32 devices in a mesh: dp: 4 (over z), sp: 8 (over y, x, core).
Axes of the slice: x: 2, y: 2, z: 4, core: 2. Of those that a mesh axis runs over, the one named last changes fastest.
Arguments:
- x_prompt: bfloat16 [48, 1024, 2048], P('dp', 'sp'), parts along dimension 0
- ln_attn_w: float32 [2048], replicated
- ln_attn_b: float32 [2048], replicated
- ln_mlp_w: float32 [2048], replicated
- ln_mlp_b: float32 [2048], replicated
- w_qkv: bfloat16 [2048, 16, 3, 128], replicated
- w_out: bfloat16 [2048, 2048], replicated
- w_up: bfloat16 [2048, 8192], replicated
- w_down: bfloat16 [8192, 2048], replicated
Outputs:
- output 1: bfloat16 [48, 1024, 2048], P('dp', 'sp'), parts along dimension 0
- output 2: bfloat16 [48, 16, 1024, 128], P('dp', 'sp'), parts along dimension 0
- output 3: bfloat16 [48, 16, 1024, 128], P('dp', 'sp'), parts along dimension 0
There are 4 independent parts. The reference program is written for one: setup_inputs(seed, part) draws one part's arguments, and reference() takes and returns one part's arrays. A program takes and returns all parts, laid end to end along the dimension named above; an argument that names none is the same for every part.
All inputs are finite; a program needn't handle non-finite values.
Results may differ from the reference program's by a relative error of at most 0.0040455.
Values are sent between devices in bfloat16 or wider.
A program may use at most 1 GiB of HBM per device.

```python
import math
import jax
import jax.numpy as jnp
from jax import lax

MODEL_DIM = 2048
NUM_HEADS = 16
KV_GROUPS = 16
HEAD_DIM = 128
FFN_DIM = 8192
BATCH_PART = 12
SEQ_DEV = 128
SEQ_SHARDS = 8

GROUP_SIZE = NUM_HEADS // KV_GROUPS
SEQ_LEN = SEQ_SHARDS * SEQ_DEV
HALF_DIM = HEAD_DIM // 2
LN_EPS = 1e-5
ROPE_BASE = 10000.0


def setup_inputs(seed: int = 0, part: int = 0) -> dict:
    key_list = jax.random.split(jax.random.key(seed), 9)
    x_key = jax.random.fold_in(key_list[0], part)
    x_prompt = jax.random.normal(x_key, (BATCH_PART, SEQ_LEN, MODEL_DIM), jnp.float32)
    ln_attn_w = 1.0 + 0.25 * jax.random.normal(key_list[1], (MODEL_DIM,), jnp.float32)
    ln_attn_b = 0.1 * jax.random.normal(key_list[2], (MODEL_DIM,), jnp.float32)
    ln_mlp_w = 1.0 + 0.25 * jax.random.normal(key_list[3], (MODEL_DIM,), jnp.float32)
    ln_mlp_b = 0.2 * jax.random.normal(key_list[4], (MODEL_DIM,), jnp.float32)
    w_qkv = jax.random.normal(key_list[5], (MODEL_DIM, KV_GROUPS, GROUP_SIZE + 2, HEAD_DIM), jnp.float32) * MODEL_DIM ** -0.5
    out_gain = math.sqrt(SEQ_LEN / (2.0 * math.log(SEQ_LEN)))
    w_out = jax.random.normal(key_list[6], (NUM_HEADS * HEAD_DIM, MODEL_DIM), jnp.float32) * ((NUM_HEADS * HEAD_DIM) ** -0.5 * out_gain)
    w_up = jax.random.normal(key_list[7], (MODEL_DIM, FFN_DIM), jnp.float32) * MODEL_DIM ** -0.5
    w_down = jax.random.normal(key_list[8], (FFN_DIM, MODEL_DIM), jnp.float32) * FFN_DIM ** -0.5
    return {"x_prompt": x_prompt.astype(jnp.bfloat16), "ln_attn_w": ln_attn_w, "ln_attn_b": ln_attn_b, "ln_mlp_w": ln_mlp_w, "ln_mlp_b": ln_mlp_b, "w_qkv": w_qkv.astype(jnp.bfloat16), "w_out": w_out.astype(jnp.bfloat16), "w_up": w_up.astype(jnp.bfloat16), "w_down": w_down.astype(jnp.bfloat16)}


def layer_norm(x_rows, ln_gain, ln_bias):
    x_f32 = x_rows.astype(jnp.float32)
    row_mean = jnp.mean(x_f32, axis=-1, keepdims=True)
    row_var = jnp.mean(jnp.square(x_f32 - row_mean), axis=-1, keepdims=True)
    return ((x_f32 - row_mean) * lax.rsqrt(row_var + LN_EPS) * ln_gain + ln_bias).astype(jnp.bfloat16)


def rotary(t_in, cos_t, sin_t):
    t_f32 = t_in.astype(jnp.float32)
    low_half = t_f32[..., :HALF_DIM]
    high_half = t_f32[..., HALF_DIM:]
    return jnp.concatenate([low_half * cos_t - high_half * sin_t, high_half * cos_t + low_half * sin_t], axis=-1).astype(jnp.bfloat16)


def reference(x_prompt, ln_attn_w, ln_attn_b, ln_mlp_w, ln_mlp_b, w_qkv, w_out, w_up, w_down):
    positions = jnp.arange(SEQ_LEN)
    inv_freq = ROPE_BASE ** (-2.0 * jnp.arange(HALF_DIM, dtype=jnp.float32) / HEAD_DIM)
    angles = positions.astype(jnp.float32)[:, None] * inv_freq[None, :]
    cos_t = jnp.cos(angles)
    sin_t = jnp.sin(angles)
    w_qkv_flat = w_qkv.reshape(MODEL_DIM, KV_GROUPS * (GROUP_SIZE + 2) * HEAD_DIM)

    def one_seq(x_seq):
        h_attn = layer_norm(x_seq, ln_attn_w, ln_attn_b)
        h_mlp = layer_norm(x_seq, ln_mlp_w, ln_mlp_b)
        qkv_all = jnp.dot(h_attn, w_qkv_flat, preferred_element_type=jnp.float32).astype(jnp.bfloat16)
        qkv_all = qkv_all.reshape(SEQ_LEN, KV_GROUPS, GROUP_SIZE + 2, HEAD_DIM)
        q_rot = rotary(qkv_all[:, :, :GROUP_SIZE], cos_t[:, None, None], sin_t[:, None, None])
        k_rot = rotary(qkv_all[:, :, GROUP_SIZE], cos_t[:, None], sin_t[:, None])
        v_seq = qkv_all[:, :, GROUP_SIZE + 1]
        key_f = k_rot.astype(jnp.float32)
        val_f = v_seq.astype(jnp.float32)
        q_blocks = q_rot.reshape(SEQ_SHARDS, SEQ_DEV, KV_GROUPS, GROUP_SIZE, HEAD_DIM)

        def one_block(blk_args):
            q_blk, blk_start = blk_args
            scores = jnp.einsum("skgh,tkh->kgst", q_blk.astype(jnp.float32), key_f) * HEAD_DIM ** -0.5
            q_pos = blk_start + jnp.arange(SEQ_DEV)
            allowed = positions[None, :] <= q_pos[:, None]
            scores = jnp.where(allowed, scores, -1e30)
            attn_prob = jax.nn.softmax(scores, axis=-1).astype(jnp.bfloat16).astype(jnp.float32)
            return jnp.einsum("kgst,tkh->skgh", attn_prob, val_f).astype(jnp.bfloat16)

        context = lax.map(one_block, (q_blocks, jnp.arange(SEQ_SHARDS) * SEQ_DEV))
        ctx_flat = context.reshape(SEQ_LEN, NUM_HEADS * HEAD_DIM)
        attn_out = jnp.dot(ctx_flat, w_out, preferred_element_type=jnp.float32)
        hidden = jax.nn.gelu(jnp.dot(h_mlp, w_up, preferred_element_type=jnp.float32), approximate=False).astype(jnp.bfloat16)
        mlp_out = jnp.dot(hidden, w_down, preferred_element_type=jnp.float32)
        y_seq = (x_seq.astype(jnp.float32) + attn_out + mlp_out).astype(jnp.bfloat16)
        return y_seq, k_rot.transpose(1, 0, 2), v_seq.transpose(1, 0, 2)

    y_out, k_cache, v_cache = lax.map(one_seq, x_prompt)
    return y_out, k_cache, v_cache
```

```python
import functools

import jax
import jax.numpy as jnp
from jax import lax
from jax.experimental import pallas as pl
from jax.experimental.pallas import tpu as pltpu
from jax.sharding import PartitionSpec as P

LN_EPS = 1e-5
ROPE_BASE = 10000.0
LOG2E = 1.4426950408889634
N_CHUNKS = 4
UP_TILE = 512
QKV_TILE = 1024
Q_TILE = 256
F32 = jnp.float32
BF16 = jnp.bfloat16


def rope_tables(positions, head_dim):
    half_dim = head_dim // 2
    inv_freq = ROPE_BASE ** (-2.0 * jnp.arange(half_dim, dtype=F32) / head_dim)
    angles = positions.astype(F32)[:, None] * inv_freq[None, :]
    cos_t, sin_t = jnp.cos(angles), jnp.sin(angles)
    return jnp.concatenate([cos_t, cos_t], -1), jnp.concatenate([-sin_t, sin_t], -1)


def causal_head(q, k, v, write):
    seq, head_dim = q.shape
    scale = LOG2E * head_dim**-0.5
    rows = lax.broadcasted_iota(jnp.int32, (Q_TILE, Q_TILE), 0)
    cols = lax.broadcasted_iota(jnp.int32, (Q_TILE, Q_TILE), 1)
    for i in range(seq // Q_TILE):
        lo, hi = i * Q_TILE, (i + 1) * Q_TILE
        q_i = q[lo:hi]
        dims = (((1,), (1,)), ((), ()))
        diag = lax.dot_general(q_i, k[lo:hi], dims, preferred_element_type=F32)
        diag = jnp.where(cols <= rows, diag, -1e30)
        top = jnp.max(diag, axis=-1, keepdims=True)
        if lo:
            past = lax.dot_general(q_i, k[:lo], dims, preferred_element_type=F32)
            top = jnp.maximum(top, jnp.max(past, axis=-1, keepdims=True))
        diag = jnp.exp2((diag - top) * scale)
        total = jnp.sum(diag, axis=-1, keepdims=True)
        if lo:
            past = jnp.exp2((past - top) * scale)
            total = total + jnp.sum(past, axis=-1, keepdims=True)
        inv = 1.0 / total
        out = jnp.dot((diag * inv).astype(BF16), v[lo:hi], preferred_element_type=F32)
        if lo:
            out = out + jnp.dot((past * inv).astype(BF16), v[:lo], preferred_element_type=F32)
        write(i, out.astype(BF16))


def layer_kernel(
    n,
    x_hbm,
    cos_ref,
    sin_ref,
    ln_aw,
    ln_ab,
    ln_mw,
    ln_mb,
    w_qkv,
    w_up,
    w_down,
    resid_hbm,
    recv,
    ctx_recv,
    send,
    ctx_send,
    x_buf,
    h_attn,
    h_mlp,
    acc,
    qkv_acc,
    own,
    own_ctx,
    x_sem,
    own_sem,
    out_sem,
    send_sem,
    recv_sem,
    ctx_send_sem,
    ctx_recv_sem,
):
    me = lax.axis_index("sp")
    n_batch, _, heads, seq_dev, head_dim = send.shape[1:]
    width = x_hbm.shape[1]
    nb = n_batch // N_CHUNKS
    rows = nb * seq_dev
    ffn = w_up.shape[1]
    dests = QKV_TILE // (heads * head_dim)

    def peer(step):
        return lax.bitwise_xor(me, step)

    def put(chunk, to, frm):
        bs = pl.ds(chunk * nb, nb)
        return pltpu.make_async_remote_copy(
            src_ref=send.at[:, bs, to],
            dst_ref=recv.at[:, bs, :, frm],
            send_sem=send_sem.at[chunk, to],
            recv_sem=recv_sem.at[chunk, frm],
            device_id={"sp": to},
            device_id_type=pl.DeviceIdType.MESH,
        )

    def put_ctx(chunk, to, frm):
        bs = pl.ds(chunk * nb, nb)
        return pltpu.make_async_remote_copy(
            src_ref=ctx_send.at[bs, to],
            dst_ref=ctx_recv.at[bs, frm],
            send_sem=ctx_send_sem.at[chunk, to],
            recv_sem=ctx_recv_sem.at[chunk, frm],
            device_id={"sp": to},
            device_id_type=pl.DeviceIdType.MESH,
        )

    def put_own(chunk):
        return pltpu.make_async_copy(own, recv.at[:, pl.ds(chunk * nb, nb), :, me], own_sem.at[0])

    def put_own_ctx(chunk):
        return pltpu.make_async_copy(own_ctx, ctx_recv.at[pl.ds(chunk * nb, nb), me], own_sem.at[1])

    def get_x(chunk):
        return pltpu.make_async_copy(x_hbm.at[pl.ds(chunk * rows, rows)], x_buf, x_sem)

    get_x(0).start()
    barrier = pltpu.get_barrier_semaphore()
    for step in range(1, n):
        pl.semaphore_signal(barrier, inc=1, device_id={"sp": peer(step)}, device_id_type=pl.DeviceIdType.MESH)
    pl.semaphore_wait(barrier, n - 1)

    @pl.loop(0, N_CHUNKS)
    def _(chunk):
        get_x(chunk).wait()

        @pl.loop(0, rows // 16)
        def _(i):
            r = pl.ds(pl.multiple_of(i * 16, 16), 16)
            g = pl.ds(pl.multiple_of(chunk * rows + i * 16, 16), 16)
            xf = x_buf[r, :].astype(F32)
            mean = jnp.sum(xf, axis=-1, keepdims=True) * (1.0 / width)
            dev = xf - mean
            var = jnp.sum(dev * dev, axis=-1, keepdims=True) * (1.0 / width)
            unit = dev * lax.rsqrt(var + LN_EPS)
            h_attn[r, :] = (unit * ln_aw[...] + ln_ab[...]).astype(BF16)
            h_mlp[g, :] = (unit * ln_mw[...] + ln_mb[...]).astype(BF16)
            acc[g, :] = xf

        @pl.when(chunk + 1 < N_CHUNKS)
        def _():
            get_x(chunk + 1).start()

        @pl.when(chunk > 0)
        def _():
            put_own(chunk - 1).wait()

        def qkv_body(w_ref, o_ref):
            kind, part = pl.program_id(0), pl.program_id(1)
            qkv_acc[...] = jnp.dot(h_attn[...], w_ref[...], preferred_element_type=F32)

            @pl.when(kind < 2)
            def _():
                for d in range(dests * heads):
                    for b in range(nb):
                        u = qkv_acc[b * seq_dev : (b + 1) * seq_dev, d * head_dim : (d + 1) * head_dim]
                        u = u.astype(BF16).astype(F32)
                        u = u * cos_ref[...] + pltpu.roll(u, head_dim // 2, 1) * sin_ref[...]
                        o_ref[0, b, d // heads, d % heads] = u.astype(BF16)

            @pl.when(kind == 2)
            def _():
                for d in range(dests * heads):
                    for b in range(nb):
                        u = qkv_acc[b * seq_dev : (b + 1) * seq_dev, d * head_dim : (d + 1) * head_dim]
                        o_ref[0, b, d // heads, d % heads] = u.astype(BF16)

            @pl.when(me // dests == part)
            def _():
                own[kind] = o_ref[0, :, lax.rem(me, dests)]

        parts = n // dests
        pltpu.emit_pipeline(
            qkv_body,
            grid=(3, parts),
            in_specs=[pl.BlockSpec((width, QKV_TILE), lambda t, p: (0, t * parts + p))],
            out_specs=[
                pl.BlockSpec((1, nb, dests, heads, seq_dev, head_dim), lambda t, p: (t, chunk, p, 0, 0, 0))
            ],
        )(w_qkv, send)
        for step in range(1, n):
            put(chunk, peer(step), me).start()
        put_own(chunk).start()

    @pl.loop(0, N_CHUNKS)
    def _(chunk):
        def mlp_body(up_ref, down_ref):
            blocks = n_batch * seq_dev // 512
            for r in range(blocks):
                rs = pl.ds(r * 512, 512)
                up = jnp.dot(h_mlp[rs, :], up_ref[...], preferred_element_type=F32)
                hid = (0.5 * up * (1.0 + lax.erf(up * 0.5**0.5))).astype(BF16)
                acc[rs, :] += jnp.dot(hid, down_ref[...], preferred_element_type=F32)

        steps = ffn // UP_TILE // N_CHUNKS
        pltpu.emit_pipeline(
            mlp_body,
            grid=(steps,),
            in_specs=[
                pl.BlockSpec((width, UP_TILE), lambda f: (0, chunk * steps + f)),
                pl.BlockSpec((UP_TILE, width), lambda f: (chunk * steps + f, 0)),
            ],
        )(w_up, w_down)

        @pl.when(chunk == N_CHUNKS - 1)
        def _():
            pltpu.make_async_copy(acc, resid_hbm, out_sem).start()

        @pl.when(chunk == 0)
        def _():
            put_own(N_CHUNKS - 1).wait()

        for step in range(1, n):
            put(chunk, me, peer(step)).wait_recv()

        @pl.when(chunk > 0)
        def _():
            put_own_ctx(chunk - 1).wait()

        def attn_body(q_ref, k_ref, v_ref, o_ref):
            b, h = pl.program_id(0), pl.program_id(1)
            flat = lambda ref: ref[...].reshape(n * seq_dev, head_dim)
            per = Q_TILE // seq_dev

            def write(i, out):
                o_ref[0, i * per : (i + 1) * per, 0] = out.reshape(per, seq_dev, head_dim)

            causal_head(flat(q_ref), flat(k_ref), flat(v_ref), write)
            own_ctx[b, h] = o_ref[0, me, 0]

        spec = lambda t: pl.BlockSpec(
            (1, 1, 1, n, seq_dev, head_dim), lambda b, h: (t, chunk * nb + b, h, 0, 0, 0)
        )
        pltpu.emit_pipeline(
            attn_body,
            grid=(nb, heads),
            in_specs=[spec(0), spec(1), spec(2)],
            out_specs=[
                pl.BlockSpec((1, n, 1, seq_dev, head_dim), lambda b, h: (chunk * nb + b, 0, h, 0, 0))
            ],
        )(recv, recv, recv, ctx_send)
        for step in range(1, n):
            put_ctx(chunk, peer(step), me).start()
        put_own_ctx(chunk).start()

    put_own_ctx(N_CHUNKS - 1).wait()
    pltpu.make_async_copy(acc, resid_hbm, out_sem).wait()

    @pl.loop(0, N_CHUNKS)
    def _(chunk):
        for step in range(1, n):
            put(chunk, peer(step), me).wait_send()
            put_ctx(chunk, peer(step), me).wait_send()
            put_ctx(chunk, me, peer(step)).wait_recv()


def out_kernel(ctx_ref, w_ref, resid_ref, k_in, v_in, y_ref, k_out, v_out, rows_ref):
    nb, n, heads, seq_dev, head_dim = ctx_ref.shape
    for b in range(nb):
        for s in range(n):
            for h in range(heads):
                col = (s * heads + h) * head_dim
                rows_ref[b * seq_dev : (b + 1) * seq_dev, col : col + head_dim] = ctx_ref[b, s, h]
    attn = jnp.dot(rows_ref[...], w_ref[...], preferred_element_type=F32)
    y_ref[...] = (resid_ref[...] + attn).astype(BF16)
    k_out[...] = k_in[0]
    v_out[...] = v_in[0]


def solution(mesh):
    n = mesh.shape["sp"]

    def local_layer(x_blk, ln_attn_w, ln_attn_b, ln_mlp_w, ln_mlp_b, w_qkv, w_out, w_up, w_down):
        n_batch, seq_dev, width = x_blk.shape
        groups, head_dim = w_qkv.shape[1], w_qkv.shape[3]
        heads = groups // n
        nb = n_batch // N_CHUNKS
        rows = n_batch * seq_dev
        ffn = w_up.shape[1]
        q_pos = lax.axis_index("sp") * seq_dev + jnp.arange(seq_dev)
        cos_t, sin_t = rope_tables(q_pos, head_dim)
        w_cols = w_qkv.transpose(0, 2, 1, 3).reshape(width, -1)
        row = lambda p: p.reshape(1, width)
        anywhere = pl.BlockSpec(memory_space=pl.ANY)
        vmem = pl.BlockSpec(memory_space=pltpu.VMEM)
        flops = 2 * rows * width * (3 * width + 2 * ffn) + 2 * rows * n * seq_dev * width * 2
        resid, recv, ctx_recv, _, _ = pl.pallas_call(
            functools.partial(layer_kernel, n),
            out_shape=[
                jax.ShapeDtypeStruct((rows, width), F32),
                jax.ShapeDtypeStruct((3, n_batch, heads, n, seq_dev, head_dim), BF16),
                jax.ShapeDtypeStruct((n_batch, n, heads, seq_dev, head_dim), BF16),
                jax.ShapeDtypeStruct((3, n_batch, n, heads, seq_dev, head_dim), BF16),
                jax.ShapeDtypeStruct((n_batch, n, heads, seq_dev, head_dim), BF16),
            ],
            in_specs=[anywhere] + [vmem] * 6 + [anywhere] * 3,
            out_specs=[anywhere] * 5,
            scratch_shapes=[
                pltpu.VMEM((nb * seq_dev, width), BF16),
                pltpu.VMEM((nb * seq_dev, width), BF16),
                pltpu.VMEM((rows, width), BF16),
                pltpu.VMEM((rows, width), F32),
                pltpu.VMEM((nb * seq_dev, QKV_TILE), F32),
                pltpu.VMEM((3, nb, heads, seq_dev, head_dim), BF16),
                pltpu.VMEM((nb, heads, seq_dev, head_dim), BF16),
                pltpu.SemaphoreType.DMA,
                pltpu.SemaphoreType.DMA((2,)),
                pltpu.SemaphoreType.DMA,
                pltpu.SemaphoreType.DMA((N_CHUNKS, n)),
                pltpu.SemaphoreType.DMA((N_CHUNKS, n)),
                pltpu.SemaphoreType.DMA((N_CHUNKS, n)),
                pltpu.SemaphoreType.DMA((N_CHUNKS, n)),
            ],
            compiler_params=pltpu.CompilerParams(
                collective_id=0, has_side_effects=True, vmem_limit_bytes=60 * 2**20
            ),
            cost_estimate=pl.CostEstimate(flops=flops, bytes_accessed=3 * 10**8, transcendentals=10**7),
            name="layer",
        )(
            x_blk.reshape(rows, width),
            cos_t,
            sin_t,
            row(ln_attn_w),
            row(ln_attn_b),
            row(ln_mlp_w),
            row(ln_mlp_b),
            w_cols,
            w_up,
            w_down,
        )
        cache = jax.ShapeDtypeStruct((n_batch, heads, n, seq_dev, head_dim), BF16)
        block = nb * seq_dev
        cache_block = (nb, heads, n, seq_dev, head_dim)
        y_out, k_cache, v_cache = pl.pallas_call(
            out_kernel,
            grid=(N_CHUNKS,),
            out_shape=[jax.ShapeDtypeStruct((rows, width), BF16), cache, cache],
            in_specs=[
                pl.BlockSpec((nb, n, heads, seq_dev, head_dim), lambda i: (i, 0, 0, 0, 0)),
                pl.BlockSpec((width, width), lambda i: (0, 0)),
                pl.BlockSpec((block, width), lambda i: (i, 0)),
                pl.BlockSpec((1, *cache_block), lambda i: (1, i, 0, 0, 0, 0)),
                pl.BlockSpec((1, *cache_block), lambda i: (2, i, 0, 0, 0, 0)),
            ],
            out_specs=[
                pl.BlockSpec((block, width), lambda i: (i, 0)),
                pl.BlockSpec(cache_block, lambda i: (i, 0, 0, 0, 0)),
                pl.BlockSpec(cache_block, lambda i: (i, 0, 0, 0, 0)),
            ],
            scratch_shapes=[pltpu.VMEM((block, width), BF16)],
            compiler_params=pltpu.CompilerParams(vmem_limit_bytes=60 * 2**20),
            cost_estimate=pl.CostEstimate(
                flops=2 * rows * width * width, bytes_accessed=6 * 10**7, transcendentals=0
            ),
            name="out",
        )(ctx_recv, w_out, resid, recv, recv)
        shape = (n_batch, heads, n * seq_dev, head_dim)
        return y_out.reshape(x_blk.shape), k_cache.reshape(shape), v_cache.reshape(shape)

    act_spec, cache_spec = P("dp", "sp", None), P("dp", "sp", None, None)
    return jax.shard_map(
        local_layer,
        mesh=mesh,
        in_specs=(act_spec,) + (P(),) * 8,
        out_specs=(act_spec, cache_spec, cache_spec),
        check_vma=False,
    )
```

```python
import functools

import jax
import jax.numpy as jnp
from jax import lax
from jax.experimental import pallas as pl
from jax.experimental.pallas import tpu as pltpu
from jax.sharding import PartitionSpec as P

LN_EPS = 1e-5
ROPE_BASE = 10000.0
LOG2E = 1.4426950408889634
N_CHUNKS = 4
UP_TILE = 512
QKV_HEADS = 8
Q_TILE = 256
F32 = jnp.float32
BF16 = jnp.bfloat16


def rope_tables(positions, head_dim):
    half_dim = head_dim // 2
    inv_freq = ROPE_BASE ** (-2.0 * jnp.arange(half_dim, dtype=F32) / head_dim)
    angles = positions.astype(F32)[:, None] * inv_freq[None, :]
    cos_t, sin_t = jnp.cos(angles), jnp.sin(angles)
    return jnp.concatenate([cos_t, cos_t], -1), jnp.concatenate([-sin_t, sin_t], -1)


def causal_head(q, k, v, write):
    seq, head_dim = q.shape
    scale = LOG2E * head_dim**-0.5
    rows = lax.broadcasted_iota(jnp.int32, (Q_TILE, Q_TILE), 0)
    cols = lax.broadcasted_iota(jnp.int32, (Q_TILE, Q_TILE), 1)
    for i in range(seq // Q_TILE):
        lo, hi = i * Q_TILE, (i + 1) * Q_TILE
        q_i = q[lo:hi]
        dims = (((1,), (1,)), ((), ()))
        diag = lax.dot_general(q_i, k[lo:hi], dims, preferred_element_type=F32)
        diag = jnp.where(cols <= rows, diag, -1e30)
        top = jnp.max(diag, axis=-1, keepdims=True)
        if lo:
            past = lax.dot_general(q_i, k[:lo], dims, preferred_element_type=F32)
            top = jnp.maximum(top, jnp.max(past, axis=-1, keepdims=True))
        diag = jnp.exp2((diag - top) * scale)
        total = jnp.sum(diag, axis=-1, keepdims=True)
        if lo:
            past = jnp.exp2((past - top) * scale)
            total = total + jnp.sum(past, axis=-1, keepdims=True)
        inv = 1.0 / total
        out = jnp.dot((diag * inv).astype(BF16), v[lo:hi], preferred_element_type=F32)
        if lo:
            out = out + jnp.dot((past * inv).astype(BF16), v[:lo], preferred_element_type=F32)
        write(i, out.astype(BF16))


def layer_kernel(
    n,
    x_hbm,
    cos_ref,
    sin_ref,
    ln_aw,
    ln_ab,
    ln_mw,
    ln_mb,
    w_qkv,
    w_up,
    w_down,
    resid_hbm,
    recv,
    ctx_recv,
    send,
    ctx_send,
    h_mlp,
    acc,
    own_ctx,
    x_sem,
    w_sem,
    bounce_sem,
    own_sem,
    out_sem,
    send_sem,
    recv_sem,
    ctx_send_sem,
    ctx_recv_sem,
):
    me = lax.axis_index("sp")
    n_batch, _, heads, seq_dev, head_dim = send.shape[1:]
    width = x_hbm.shape[1]
    nb = n_batch // N_CHUNKS
    rows = nb * seq_dev
    ffn = w_up.shape[1]
    dests = QKV_HEADS // heads
    parts = n // dests
    blocks = 3 * parts

    def peer(step):
        return lax.bitwise_xor(me, step)

    def put(chunk, kind, to, frm):
        bs = pl.ds(chunk * nb, nb)
        return pltpu.make_async_remote_copy(
            src_ref=send.at[kind, bs, to],
            dst_ref=recv.at[kind, bs, :, frm],
            send_sem=send_sem.at[chunk, kind, to],
            recv_sem=recv_sem.at[chunk, kind, frm],
            device_id={"sp": to},
            device_id_type=pl.DeviceIdType.MESH,
        )

    def put_ctx(chunk, to, frm):
        bs = pl.ds(chunk * nb, nb)
        return pltpu.make_async_remote_copy(
            src_ref=ctx_send.at[bs, to],
            dst_ref=ctx_recv.at[bs, frm],
            send_sem=ctx_send_sem.at[chunk, to],
            recv_sem=ctx_recv_sem.at[chunk, frm],
            device_id={"sp": to},
            device_id_type=pl.DeviceIdType.MESH,
        )

    def put_own_ctx(chunk):
        return pltpu.make_async_copy(own_ctx, ctx_recv.at[pl.ds(chunk * nb, nb), me], own_sem.at[3])

    def qkv_phase(x_buf, h_attn, w_nat, w_cols, qkv_acc, out_buf, own):
        def get_x(chunk):
            return pltpu.make_async_copy(x_hbm.at[pl.ds(chunk * rows, rows)], x_buf, x_sem)

        def get_w(block):
            slot = lax.rem(block, 2)
            src = w_qkv.at[:, block // parts, pl.ds(lax.rem(block, parts) * QKV_HEADS, QKV_HEADS)]
            return pltpu.make_async_copy(src, w_nat.at[slot], w_sem.at[slot])

        def bounce(step):
            slot, block = lax.rem(step, 2), lax.rem(step, blocks)
            dst = send.at[
                block // parts, pl.ds(step // blocks * nb, nb), pl.ds(lax.rem(block, parts) * dests, dests)
            ]
            return pltpu.make_async_copy(out_buf.at[slot], dst, bounce_sem.at[slot])

        def put_own(chunk, kind):
            dst = recv.at[kind, pl.ds(chunk * nb, nb), :, me]
            return pltpu.make_async_copy(own.at[kind], dst, own_sem.at[kind])

        def send_block(step):
            bounce(step).wait()
            block = lax.rem(step, blocks)
            for d in range(dests):
                to = lax.rem(block, parts) * dests + lax.rem(me + d, dests)

                @pl.when(to != me)
                def _():
                    put(step // blocks, block // parts, to, me).start()

        get_x(0).start()
        get_w(0).start()
        barrier = pltpu.get_barrier_semaphore()
        for step in range(1, n):
            pl.semaphore_signal(
                barrier, inc=1, device_id={"sp": peer(step)}, device_id_type=pl.DeviceIdType.MESH
            )

        @pl.loop(0, N_CHUNKS * blocks)
        def _(step):
            chunk, block = step // blocks, lax.rem(step, blocks)
            kind, part = block // parts, lax.rem(block, parts)
            slot = lax.rem(step, 2)

            @pl.when(block == 0)
            def _():
                get_x(chunk).wait()

                @pl.loop(0, rows // 16)
                def _(i):
                    r = pl.ds(pl.multiple_of(i * 16, 16), 16)
                    g = pl.ds(pl.multiple_of(chunk * rows + i * 16, 16), 16)
                    xf = x_buf[r, :].astype(F32)
                    mean = jnp.sum(xf, axis=-1, keepdims=True) * (1.0 / width)
                    dev = xf - mean
                    var = jnp.sum(dev * dev, axis=-1, keepdims=True) * (1.0 / width)
                    unit = dev * lax.rsqrt(var + LN_EPS)
                    h_attn[r, :] = (unit * ln_aw[...] + ln_ab[...]).astype(BF16)
                    h_mlp[g, :] = (unit * ln_mw[...] + ln_mb[...]).astype(BF16)
                    acc[g, :] = xf

                @pl.when(chunk + 1 < N_CHUNKS)
                def _():
                    get_x(chunk + 1).start()

            @pl.when(chunk == 0)
            def _():
                get_w(block).wait()

                @pl.when(block + 1 < blocks)
                def _():
                    get_w(block + 1).start()

                @pl.loop(0, width // 128)
                def _(i):
                    r = pl.ds(pl.multiple_of(i * 128, 128), 128)
                    by_head = jnp.swapaxes(w_nat[slot, r].astype(F32), 0, 1)
                    for h in range(QKV_HEADS):
                        w_cols[block, r, h * head_dim : (h + 1) * head_dim] = by_head[h].astype(BF16)

            qkv_acc[...] = jnp.dot(h_attn[...], w_cols[block], preferred_element_type=F32)

            def take(b, h):
                u = qkv_acc[b * seq_dev : (b + 1) * seq_dev, h * head_dim : (h + 1) * head_dim]
                return u.astype(BF16)

            @pl.when(kind < 2)
            def _():
                for h in range(QKV_HEADS):
                    for b in range(nb):
                        u = take(b, h).astype(F32)
                        u = u * cos_ref[...] + pltpu.roll(u, head_dim // 2, 1) * sin_ref[...]
                        out_buf[slot, b, h // heads, h % heads] = u.astype(BF16)

            @pl.when(kind == 2)
            def _():
                for h in range(QKV_HEADS):
                    for b in range(nb):
                        out_buf[slot, b, h // heads, h % heads] = take(b, h)

            bounce(step).start()

            @pl.when(me // dests == part)
            def _():
                @pl.when(chunk > 0)
                def _():
                    put_own(chunk - 1, kind).wait()

                own[kind] = out_buf[slot, :, lax.rem(me, dests)]
                put_own(chunk, kind).start()

            @pl.when(step == 0)
            def _():
                pl.semaphore_wait(barrier, n - 1)

            @pl.when(step > 0)
            def _():
                send_block(step - 1)

        send_block(N_CHUNKS * blocks - 1)
        for kind in range(3):
            put_own(N_CHUNKS - 1, kind).wait()

    pl.run_scoped(
        qkv_phase,
        pltpu.VMEM((rows, width), BF16),
        pltpu.VMEM((rows, width), BF16),
        pltpu.VMEM((2, width, QKV_HEADS, head_dim), BF16),
        pltpu.VMEM((blocks, width, QKV_HEADS * head_dim), BF16),
        pltpu.VMEM((rows, QKV_HEADS * head_dim), F32),
        pltpu.VMEM((2, nb, dests, heads, seq_dev, head_dim), BF16),
        pltpu.VMEM((3, nb, heads, seq_dev, head_dim), BF16),
    )

    @pl.loop(0, N_CHUNKS)
    def _(chunk):
        def mlp_body(up_ref, down_ref):
            blocks = n_batch * seq_dev // 512
            for r in range(blocks):
                rs = pl.ds(r * 512, 512)
                up = jnp.dot(h_mlp[rs, :], up_ref[...], preferred_element_type=F32)
                hid = (0.5 * up * (1.0 + lax.erf(up * 0.5**0.5))).astype(BF16)
                acc[rs, :] += jnp.dot(hid, down_ref[...], preferred_element_type=F32)

        steps = ffn // UP_TILE // N_CHUNKS
        pltpu.emit_pipeline(
            mlp_body,
            grid=(steps,),
            in_specs=[
                pl.BlockSpec((width, UP_TILE), lambda f: (0, chunk * steps + f)),
                pl.BlockSpec((UP_TILE, width), lambda f: (chunk * steps + f, 0)),
            ],
        )(w_up, w_down)

        @pl.when(chunk == N_CHUNKS - 1)
        def _():
            pltpu.make_async_copy(acc, resid_hbm, out_sem).start()

        for step in range(1, n):
            for kind in range(3):
                put(chunk, kind, me, peer(step)).wait_recv()

        @pl.when(chunk > 0)
        def _():
            put_own_ctx(chunk - 1).wait()

        def attn_body(q_ref, k_ref, v_ref, o_ref):
            b, h = pl.program_id(0), pl.program_id(1)
            flat = lambda ref: ref[...].reshape(n * seq_dev, head_dim)
            per = Q_TILE // seq_dev

            def write(i, out):
                o_ref[0, i * per : (i + 1) * per, 0] = out.reshape(per, seq_dev, head_dim)

            causal_head(flat(q_ref), flat(k_ref), flat(v_ref), write)
            own_ctx[b, h] = o_ref[0, me, 0]

        spec = lambda t: pl.BlockSpec(
            (1, 1, 1, n, seq_dev, head_dim), lambda b, h: (t, chunk * nb + b, h, 0, 0, 0)
        )
        pltpu.emit_pipeline(
            attn_body,
            grid=(nb, heads),
            in_specs=[spec(0), spec(1), spec(2)],
            out_specs=[
                pl.BlockSpec((1, n, 1, seq_dev, head_dim), lambda b, h: (chunk * nb + b, 0, h, 0, 0))
            ],
        )(recv, recv, recv, ctx_send)
        for step in range(1, n):
            put_ctx(chunk, peer(step), me).start()
        put_own_ctx(chunk).start()

    put_own_ctx(N_CHUNKS - 1).wait()
    pltpu.make_async_copy(acc, resid_hbm, out_sem).wait()

    @pl.loop(0, N_CHUNKS)
    def _(chunk):
        for step in range(1, n):
            for kind in range(3):
                put(chunk, kind, peer(step), me).wait_send()
            put_ctx(chunk, peer(step), me).wait_send()
            put_ctx(chunk, me, peer(step)).wait_recv()


def out_kernel(ctx_ref, w_ref, resid_ref, k_in, v_in, y_ref, k_out, v_out, rows_ref):
    nb, n, heads, seq_dev, head_dim = ctx_ref.shape
    for b in range(nb):
        for s in range(n):
            for h in range(heads):
                col = (s * heads + h) * head_dim
                rows_ref[b * seq_dev : (b + 1) * seq_dev, col : col + head_dim] = ctx_ref[b, s, h]
    attn = jnp.dot(rows_ref[...], w_ref[...], preferred_element_type=F32)
    y_ref[...] = (resid_ref[...] + attn).astype(BF16)
    k_out[...] = k_in[0]
    v_out[...] = v_in[0]


def solution(mesh):
    n = mesh.shape["sp"]

    def local_layer(x_blk, ln_attn_w, ln_attn_b, ln_mlp_w, ln_mlp_b, w_qkv, w_out, w_up, w_down):
        n_batch, seq_dev, width = x_blk.shape
        groups, head_dim = w_qkv.shape[1], w_qkv.shape[3]
        heads = groups // n
        nb = n_batch // N_CHUNKS
        rows = n_batch * seq_dev
        ffn = w_up.shape[1]
        q_pos = lax.axis_index("sp") * seq_dev + jnp.arange(seq_dev)
        cos_t, sin_t = rope_tables(q_pos, head_dim)
        row = lambda p: p.reshape(1, width)
        anywhere = pl.BlockSpec(memory_space=pl.ANY)
        vmem = pl.BlockSpec(memory_space=pltpu.VMEM)
        flops = 2 * rows * width * (3 * width + 2 * ffn) + 2 * rows * n * seq_dev * width * 2
        resid, recv, ctx_recv, _, _ = pl.pallas_call(
            functools.partial(layer_kernel, n),
            out_shape=[
                jax.ShapeDtypeStruct((rows, width), F32),
                jax.ShapeDtypeStruct((3, n_batch, heads, n, seq_dev, head_dim), BF16),
                jax.ShapeDtypeStruct((n_batch, n, heads, seq_dev, head_dim), BF16),
                jax.ShapeDtypeStruct((3, n_batch, n, heads, seq_dev, head_dim), BF16),
                jax.ShapeDtypeStruct((n_batch, n, heads, seq_dev, head_dim), BF16),
            ],
            in_specs=[anywhere] + [vmem] * 6 + [anywhere] * 3,
            out_specs=[anywhere] * 5,
            scratch_shapes=[
                pltpu.VMEM((rows, width), BF16),
                pltpu.VMEM((rows, width), F32),
                pltpu.VMEM((nb, heads, seq_dev, head_dim), BF16),
                pltpu.SemaphoreType.DMA,
                pltpu.SemaphoreType.DMA((2,)),
                pltpu.SemaphoreType.DMA((2,)),
                pltpu.SemaphoreType.DMA((4,)),
                pltpu.SemaphoreType.DMA,
                pltpu.SemaphoreType.DMA((N_CHUNKS, 3, n)),
                pltpu.SemaphoreType.DMA((N_CHUNKS, 3, n)),
                pltpu.SemaphoreType.DMA((N_CHUNKS, n)),
                pltpu.SemaphoreType.DMA((N_CHUNKS, n)),
            ],
            compiler_params=pltpu.CompilerParams(
                collective_id=0, has_side_effects=True, vmem_limit_bytes=63 * 2**20
            ),
            cost_estimate=pl.CostEstimate(flops=flops, bytes_accessed=3 * 10**8, transcendentals=10**7),
            name="layer",
        )(
            x_blk.reshape(rows, width),
            cos_t,
            sin_t,
            row(ln_attn_w),
            row(ln_attn_b),
            row(ln_mlp_w),
            row(ln_mlp_b),
            w_qkv.transpose(0, 2, 1, 3),
            w_up,
            w_down,
        )
        cache = jax.ShapeDtypeStruct((n_batch, heads, n, seq_dev, head_dim), BF16)
        nb = 1
        block = nb * seq_dev
        cache_block = (nb, heads, n, seq_dev, head_dim)
        y_out, k_cache, v_cache = pl.pallas_call(
            out_kernel,
            grid=(n_batch // nb,),
            out_shape=[jax.ShapeDtypeStruct((rows, width), BF16), cache, cache],
            in_specs=[
                pl.BlockSpec((nb, n, heads, seq_dev, head_dim), lambda i: (i, 0, 0, 0, 0)),
                pl.BlockSpec((width, width), lambda i: (0, 0)),
                pl.BlockSpec((block, width), lambda i: (i, 0)),
                pl.BlockSpec((1, *cache_block), lambda i: (1, i, 0, 0, 0, 0)),
                pl.BlockSpec((1, *cache_block), lambda i: (2, i, 0, 0, 0, 0)),
            ],
            out_specs=[
                pl.BlockSpec((block, width), lambda i: (i, 0)),
                pl.BlockSpec(cache_block, lambda i: (i, 0, 0, 0, 0)),
                pl.BlockSpec(cache_block, lambda i: (i, 0, 0, 0, 0)),
            ],
            scratch_shapes=[pltpu.VMEM((block, width), BF16)],
            compiler_params=pltpu.CompilerParams(vmem_limit_bytes=60 * 2**20),
            cost_estimate=pl.CostEstimate(
                flops=2 * rows * width * width, bytes_accessed=6 * 10**7, transcendentals=0
            ),
            name="out",
        )(ctx_recv, w_out, resid, recv, recv)
        shape = (n_batch, heads, n * seq_dev, head_dim)
        return y_out.reshape(x_blk.shape), k_cache.reshape(shape), v_cache.reshape(shape)

    act_spec, cache_spec = P("dp", "sp", None), P("dp", "sp", None, None)
    return jax.shard_map(
        local_layer,
        mesh=mesh,
        in_specs=(act_spec,) + (P(),) * 8,
        out_specs=(act_spec, cache_spec, cache_spec),
        check_vma=False,
    )
```

```python
import functools

import jax
import jax.numpy as jnp
from jax import lax
from jax.experimental import pallas as pl
from jax.experimental.pallas import tpu as pltpu
from jax.sharding import PartitionSpec as P

LN_EPS = 1e-5
ROPE_BASE = 10000.0
LOG2E = 1.4426950408889634
N_CHUNKS = 4
UP_TILE = 512
QKV_HEADS = 8
Q_TILE = 256
F32 = jnp.float32
BF16 = jnp.bfloat16


def rope_tables(positions, head_dim):
    half_dim = head_dim // 2
    inv_freq = ROPE_BASE ** (-2.0 * jnp.arange(half_dim, dtype=F32) / head_dim)
    angles = positions.astype(F32)[:, None] * inv_freq[None, :]
    cos_t, sin_t = jnp.cos(angles), jnp.sin(angles)
    return jnp.concatenate([cos_t, cos_t], -1), jnp.concatenate([-sin_t, sin_t], -1)


def causal_head(q, k, v, write):
    seq, head_dim = q.shape
    scale = LOG2E * head_dim**-0.5
    rows = lax.broadcasted_iota(jnp.int32, (Q_TILE, Q_TILE), 0)
    cols = lax.broadcasted_iota(jnp.int32, (Q_TILE, Q_TILE), 1)
    for i in range(seq // Q_TILE):
        lo, hi = i * Q_TILE, (i + 1) * Q_TILE
        q_i = q[lo:hi]
        dims = (((1,), (1,)), ((), ()))
        diag = lax.dot_general(q_i, k[lo:hi], dims, preferred_element_type=F32)
        diag = jnp.where(cols <= rows, diag, -1e30)
        top = jnp.max(diag, axis=-1, keepdims=True)
        if lo:
            past = lax.dot_general(q_i, k[:lo], dims, preferred_element_type=F32)
            top = jnp.maximum(top, jnp.max(past, axis=-1, keepdims=True))
        diag = jnp.exp2((diag - top) * scale)
        total = jnp.sum(diag, axis=-1, keepdims=True)
        if lo:
            past = jnp.exp2((past - top) * scale)
            total = total + jnp.sum(past, axis=-1, keepdims=True)
        inv = 1.0 / total
        out = jnp.dot((diag * inv).astype(BF16), v[lo:hi], preferred_element_type=F32)
        if lo:
            out = out + jnp.dot((past * inv).astype(BF16), v[:lo], preferred_element_type=F32)
        write(i, out.astype(BF16))


def layer_kernel(
    n,
    x_hbm,
    cos_ref,
    sin_ref,
    ln_aw,
    ln_ab,
    ln_mw,
    ln_mb,
    w_qkv,
    w_out,
    w_up,
    w_down,
    y_hbm,
    recv,
    ctx_recv,
    send,
    ctx_send,
    h_mlp,
    acc,
    own_ctx,
    x_sem,
    w_sem,
    bounce_sem,
    own_sem,
    out_sem,
    send_sem,
    recv_sem,
    ctx_send_sem,
    ctx_recv_sem,
):
    me = lax.axis_index("sp")
    n_batch, _, heads, seq_dev, head_dim = send.shape[1:]
    width = x_hbm.shape[1]
    nb = n_batch // N_CHUNKS
    rows = nb * seq_dev
    ffn = w_up.shape[1]
    dests = QKV_HEADS // heads
    parts = n // dests
    blocks = 3 * parts

    def peer(step):
        return lax.bitwise_xor(me, step)

    def put(chunk, kind, to, frm):
        bs = pl.ds(chunk * nb, nb)
        return pltpu.make_async_remote_copy(
            src_ref=send.at[kind, bs, to],
            dst_ref=recv.at[kind, bs, :, frm],
            send_sem=send_sem.at[chunk, kind, to],
            recv_sem=recv_sem.at[chunk, kind, frm],
            device_id={"sp": to},
            device_id_type=pl.DeviceIdType.MESH,
        )

    def put_ctx(chunk, to, frm):
        bs = pl.ds(chunk * nb, nb)
        return pltpu.make_async_remote_copy(
            src_ref=ctx_send.at[bs, to],
            dst_ref=ctx_recv.at[bs, frm],
            send_sem=ctx_send_sem.at[chunk, to],
            recv_sem=ctx_recv_sem.at[chunk, frm],
            device_id={"sp": to},
            device_id_type=pl.DeviceIdType.MESH,
        )

    def put_own_ctx(chunk):
        return pltpu.make_async_copy(own_ctx, ctx_recv.at[pl.ds(chunk * nb, nb), me], own_sem.at[3])

    def qkv_phase(x_buf, h_attn, w_nat, w_cols, qkv_acc, out_buf, own):
        def get_x(chunk):
            return pltpu.make_async_copy(x_hbm.at[pl.ds(chunk * rows, rows)], x_buf, x_sem)

        def get_w(block):
            slot = lax.rem(block, 2)
            src = w_qkv.at[:, block // parts, pl.ds(lax.rem(block, parts) * QKV_HEADS, QKV_HEADS)]
            return pltpu.make_async_copy(src, w_nat.at[slot], w_sem.at[slot])

        def bounce(step):
            slot, block = lax.rem(step, 2), lax.rem(step, blocks)
            dst = send.at[
                block // parts, pl.ds(step // blocks * nb, nb), pl.ds(lax.rem(block, parts) * dests, dests)
            ]
            return pltpu.make_async_copy(out_buf.at[slot], dst, bounce_sem.at[slot])

        def put_own(chunk, kind):
            dst = recv.at[kind, pl.ds(chunk * nb, nb), :, me]
            return pltpu.make_async_copy(own.at[kind], dst, own_sem.at[kind])

        def send_block(step):
            bounce(step).wait()
            block = lax.rem(step, blocks)
            for d in range(dests):
                to = lax.rem(block, parts) * dests + lax.rem(me + d, dests)

                @pl.when(to != me)
                def _():
                    put(step // blocks, block // parts, to, me).start()

        get_x(0).start()
        get_w(0).start()
        barrier = pltpu.get_barrier_semaphore()
        for step in range(1, n):
            pl.semaphore_signal(
                barrier, inc=1, device_id={"sp": peer(step)}, device_id_type=pl.DeviceIdType.MESH
            )

        @pl.loop(0, N_CHUNKS * blocks)
        def _(step):
            chunk, block = step // blocks, lax.rem(step, blocks)
            kind, part = block // parts, lax.rem(block, parts)
            slot = lax.rem(step, 2)

            @pl.when(block == 0)
            def _():
                get_x(chunk).wait()

                @pl.loop(0, rows // 16)
                def _(i):
                    r = pl.ds(pl.multiple_of(i * 16, 16), 16)
                    g = pl.ds(pl.multiple_of(chunk * rows + i * 16, 16), 16)
                    xf = x_buf[r, :].astype(F32)
                    mean = jnp.sum(xf, axis=-1, keepdims=True) * (1.0 / width)
                    dev = xf - mean
                    var = jnp.sum(dev * dev, axis=-1, keepdims=True) * (1.0 / width)
                    unit = dev * lax.rsqrt(var + LN_EPS)
                    h_attn[r, :] = (unit * ln_aw[...] + ln_ab[...]).astype(BF16)
                    h_mlp[g, :] = (unit * ln_mw[...] + ln_mb[...]).astype(BF16)
                    acc[g, :] = xf

                @pl.when(chunk + 1 < N_CHUNKS)
                def _():
                    get_x(chunk + 1).start()

            @pl.when(chunk == 0)
            def _():
                get_w(block).wait()

                @pl.when(block + 1 < blocks)
                def _():
                    get_w(block + 1).start()

                @pl.loop(0, width // 128)
                def _(i):
                    r = pl.ds(pl.multiple_of(i * 128, 128), 128)
                    by_head = jnp.swapaxes(w_nat[slot, r].astype(F32), 0, 1)
                    for h in range(QKV_HEADS):
                        w_cols[block, r, h * head_dim : (h + 1) * head_dim] = by_head[h].astype(BF16)

            qkv_acc[...] = jnp.dot(h_attn[...], w_cols[block], preferred_element_type=F32)

            def take(b, h):
                u = qkv_acc[b * seq_dev : (b + 1) * seq_dev, h * head_dim : (h + 1) * head_dim]
                return u.astype(BF16)

            @pl.when(kind < 2)
            def _():
                for h in range(QKV_HEADS):
                    for b in range(nb):
                        u = take(b, h).astype(F32)
                        u = u * cos_ref[...] + pltpu.roll(u, head_dim // 2, 1) * sin_ref[...]
                        out_buf[slot, b, h // heads, h % heads] = u.astype(BF16)

            @pl.when(kind == 2)
            def _():
                for h in range(QKV_HEADS):
                    for b in range(nb):
                        out_buf[slot, b, h // heads, h % heads] = take(b, h)

            bounce(step).start()

            @pl.when(me // dests == part)
            def _():
                @pl.when(chunk > 0)
                def _():
                    put_own(chunk - 1, kind).wait()

                own[kind] = out_buf[slot, :, lax.rem(me, dests)]
                put_own(chunk, kind).start()

            @pl.when(step == 0)
            def _():
                pl.semaphore_wait(barrier, n - 1)

            @pl.when(step > 0)
            def _():
                send_block(step - 1)

        send_block(N_CHUNKS * blocks - 1)
        for kind in range(3):
            put_own(N_CHUNKS - 1, kind).wait()

    pl.run_scoped(
        qkv_phase,
        pltpu.VMEM((rows, width), BF16),
        pltpu.VMEM((rows, width), BF16),
        pltpu.VMEM((2, width, QKV_HEADS, head_dim), BF16),
        pltpu.VMEM((blocks, width, QKV_HEADS * head_dim), BF16),
        pltpu.VMEM((rows, QKV_HEADS * head_dim), F32),
        pltpu.VMEM((2, nb, dests, heads, seq_dev, head_dim), BF16),
        pltpu.VMEM((3, nb, heads, seq_dev, head_dim), BF16),
    )

    def rest(w_buf, ctx_buf, ctx_rows, y_buf):
        def get_w_out():
            return pltpu.make_async_copy(w_out, w_buf, w_sem.at[0])

        def put_y(chunk):
            return pltpu.make_async_copy(y_buf, y_hbm.at[pl.ds(chunk * rows, rows)], out_sem)

        get_w_out().start()

        @pl.loop(0, N_CHUNKS)
        def _(chunk):
            def mlp_body(up_ref, down_ref):
                for r in range(n_batch * seq_dev // 512):
                    rs = pl.ds(r * 512, 512)
                    up = jnp.dot(h_mlp[rs, :], up_ref[...], preferred_element_type=F32)
                    hid = (0.5 * up * (1.0 + lax.erf(up * 0.5**0.5))).astype(BF16)
                    acc[rs, :] += jnp.dot(hid, down_ref[...], preferred_element_type=F32)

            steps = ffn // UP_TILE // N_CHUNKS
            pltpu.emit_pipeline(
                mlp_body,
                grid=(steps,),
                in_specs=[
                    pl.BlockSpec((width, UP_TILE), lambda f: (0, chunk * steps + f)),
                    pl.BlockSpec((UP_TILE, width), lambda f: (chunk * steps + f, 0)),
                ],
            )(w_up, w_down)

            for step in range(1, n):
                for kind in range(3):
                    put(chunk, kind, me, peer(step)).wait_recv()

            @pl.when(chunk > 0)
            def _():
                put_own_ctx(chunk - 1).wait()

            def attn_body(q_ref, k_ref, v_ref, o_ref):
                b, h = pl.program_id(0), pl.program_id(1)
                flat = lambda ref: ref[...].reshape(n * seq_dev, head_dim)
                per = Q_TILE // seq_dev

                def write(i, out):
                    o_ref[0, i * per : (i + 1) * per, 0] = out.reshape(per, seq_dev, head_dim)

                causal_head(flat(q_ref), flat(k_ref), flat(v_ref), write)
                own_ctx[b, h] = o_ref[0, me, 0]

            spec = lambda t: pl.BlockSpec(
                (1, 1, 1, n, seq_dev, head_dim), lambda b, h: (t, chunk * nb + b, h, 0, 0, 0)
            )
            pltpu.emit_pipeline(
                attn_body,
                grid=(nb, heads),
                in_specs=[spec(0), spec(1), spec(2)],
                out_specs=[
                    pl.BlockSpec((1, n, 1, seq_dev, head_dim), lambda b, h: (chunk * nb + b, 0, h, 0, 0))
                ],
            )(recv, recv, recv, ctx_send)
            for step in range(1, n):
                put_ctx(chunk, peer(step), me).start()
            put_own_ctx(chunk).start()

        put_own_ctx(N_CHUNKS - 1).wait()
        get_w_out().wait()

        @pl.loop(0, N_CHUNKS)
        def _(chunk):
            for step in range(1, n):
                put_ctx(chunk, me, peer(step)).wait_recv()
            get_ctx = pltpu.make_async_copy(ctx_recv.at[pl.ds(chunk * nb, nb)], ctx_buf, x_sem)
            get_ctx.start()
            get_ctx.wait()
            for b in range(nb):
                for s in range(n):
                    for h in range(heads):
                        col = (s * heads + h) * head_dim
                        ctx_rows[b * seq_dev : (b + 1) * seq_dev, col : col + head_dim] = ctx_buf[b, s, h]

            @pl.when(chunk > 0)
            def _():
                put_y(chunk - 1).wait()

            g = pl.ds(pl.multiple_of(chunk * rows, rows), rows)
            for c in range(0, width, 1024):
                cs = slice(c, c + 1024)
                attn = jnp.dot(ctx_rows[...], w_buf[:, cs], preferred_element_type=F32)
                y_buf[:, cs] = (acc[g, cs] + attn).astype(BF16)
            put_y(chunk).start()

        put_y(N_CHUNKS - 1).wait()

    pl.run_scoped(
        rest,
        pltpu.VMEM((width, width), BF16),
        pltpu.VMEM((nb, n, heads, seq_dev, head_dim), BF16),
        pltpu.VMEM((rows, width), BF16),
        pltpu.VMEM((rows, width), BF16),
    )

    @pl.loop(0, N_CHUNKS)
    def _(chunk):
        for step in range(1, n):
            for kind in range(3):
                put(chunk, kind, peer(step), me).wait_send()
            put_ctx(chunk, peer(step), me).wait_send()


def solution(mesh):
    n = mesh.shape["sp"]

    def local_layer(x_blk, ln_attn_w, ln_attn_b, ln_mlp_w, ln_mlp_b, w_qkv, w_out, w_up, w_down):
        n_batch, seq_dev, width = x_blk.shape
        groups, head_dim = w_qkv.shape[1], w_qkv.shape[3]
        heads = groups // n
        nb = n_batch // N_CHUNKS
        rows = n_batch * seq_dev
        ffn = w_up.shape[1]
        q_pos = lax.axis_index("sp") * seq_dev + jnp.arange(seq_dev)
        cos_t, sin_t = rope_tables(q_pos, head_dim)
        row = lambda p: p.reshape(1, width)
        anywhere = pl.BlockSpec(memory_space=pl.ANY)
        vmem = pl.BlockSpec(memory_space=pltpu.VMEM)
        flops = 2 * rows * width * (3 * width + 2 * ffn) + 2 * rows * n * seq_dev * width * 2
        y_out, recv, _, _, _ = pl.pallas_call(
            functools.partial(layer_kernel, n),
            out_shape=[
                jax.ShapeDtypeStruct((rows, width), BF16),
                jax.ShapeDtypeStruct((3, n_batch, heads, n, seq_dev, head_dim), BF16),
                jax.ShapeDtypeStruct((n_batch, n, heads, seq_dev, head_dim), BF16),
                jax.ShapeDtypeStruct((3, n_batch, n, heads, seq_dev, head_dim), BF16),
                jax.ShapeDtypeStruct((n_batch, n, heads, seq_dev, head_dim), BF16),
            ],
            in_specs=[anywhere] + [vmem] * 6 + [anywhere] * 4,
            out_specs=[anywhere] * 5,
            scratch_shapes=[
                pltpu.VMEM((rows, width), BF16),
                pltpu.VMEM((rows, width), F32),
                pltpu.VMEM((nb, heads, seq_dev, head_dim), BF16),
                pltpu.SemaphoreType.DMA,
                pltpu.SemaphoreType.DMA((2,)),
                pltpu.SemaphoreType.DMA((2,)),
                pltpu.SemaphoreType.DMA((4,)),
                pltpu.SemaphoreType.DMA,
                pltpu.SemaphoreType.DMA((N_CHUNKS, 3, n)),
                pltpu.SemaphoreType.DMA((N_CHUNKS, 3, n)),
                pltpu.SemaphoreType.DMA((N_CHUNKS, n)),
                pltpu.SemaphoreType.DMA((N_CHUNKS, n)),
            ],
            compiler_params=pltpu.CompilerParams(
                collective_id=0, has_side_effects=True, vmem_limit_bytes=63 * 2**20
            ),
            cost_estimate=pl.CostEstimate(flops=flops, bytes_accessed=3 * 10**8, transcendentals=10**7),
            name="layer",
        )(
            x_blk.reshape(rows, width),
            cos_t,
            sin_t,
            row(ln_attn_w),
            row(ln_attn_b),
            row(ln_mlp_w),
            row(ln_mlp_b),
            w_qkv.transpose(0, 2, 1, 3),
            w_out,
            w_up,
            w_down,
        )
        shape = (n_batch, heads, n * seq_dev, head_dim)
        return y_out.reshape(x_blk.shape), recv[1].reshape(shape), recv[2].reshape(shape)

    act_spec, cache_spec = P("dp", "sp", None), P("dp", "sp", None, None)
    return jax.shard_map(
        local_layer,
        mesh=mesh,
        in_specs=(act_spec,) + (P(),) * 8,
        out_specs=(act_spec, cache_spec, cache_spec),
        check_vma=False,
    )
```

```python
import functools

import jax
import jax.numpy as jnp
from jax import lax
from jax.experimental import pallas as pl
from jax.experimental.pallas import tpu as pltpu
from jax.sharding import PartitionSpec as P

LN_EPS = 1e-5
ROPE_BASE = 10000.0
LOG2E = 1.4426950408889634
N_CHUNKS = 4
UP_TILE = 512
QKV_HEADS = 8
Q_TILE = 256
FIRST = 2
RELAYED = 3
F32 = jnp.float32
BF16 = jnp.bfloat16


def rope_tables(positions, head_dim):
    half_dim = head_dim // 2
    inv_freq = ROPE_BASE ** (-2.0 * jnp.arange(half_dim, dtype=F32) / head_dim)
    angles = positions.astype(F32)[:, None] * inv_freq[None, :]
    cos_t, sin_t = jnp.cos(angles), jnp.sin(angles)
    return jnp.concatenate([cos_t, cos_t], -1), jnp.concatenate([-sin_t, sin_t], -1)


def causal_head(q, k, v, write):
    seq, head_dim = k.shape
    scale = LOG2E * head_dim**-0.5
    rows = lax.broadcasted_iota(jnp.int32, (Q_TILE, Q_TILE), 0)
    cols = lax.broadcasted_iota(jnp.int32, (Q_TILE, Q_TILE), 1)
    for i in range(q.shape[0] // Q_TILE):
        q_i = q[i * Q_TILE : (i + 1) * Q_TILE]
        lo = seq - q.shape[0] + i * Q_TILE
        hi = lo + Q_TILE
        dims = (((1,), (1,)), ((), ()))
        diag = lax.dot_general(q_i, k[lo:hi], dims, preferred_element_type=F32)
        diag = jnp.where(cols <= rows, diag, -1e30)
        top = jnp.max(diag, axis=-1, keepdims=True)
        if lo:
            past = lax.dot_general(q_i, k[:lo], dims, preferred_element_type=F32)
            top = jnp.maximum(top, jnp.max(past, axis=-1, keepdims=True))
        diag = jnp.exp2((diag - top) * scale)
        total = jnp.sum(diag, axis=-1, keepdims=True)
        if lo:
            past = jnp.exp2((past - top) * scale)
            total = total + jnp.sum(past, axis=-1, keepdims=True)
        inv = 1.0 / total
        out = jnp.dot((diag * inv).astype(BF16), v[lo:hi], preferred_element_type=F32)
        if lo:
            out = out + jnp.dot((past * inv).astype(BF16), v[:lo], preferred_element_type=F32)
        write(i, out.astype(BF16))


def layer_kernel(
    n,
    x_hbm,
    cos_ref,
    sin_ref,
    ln_aw,
    ln_ab,
    ln_mw,
    ln_mb,
    w_qkv,
    w_out,
    w_up,
    w_down,
    y_hbm,
    recv,
    ctx_recv,
    send,
    ctx_send,
    near,
    ctx_near,
    relay,
    h_mlp,
    acc,
    x_sem,
    w_sem,
    bounce_sem,
    own_sem,
    out_sem,
    send_sem,
    recv_sem,
    ctx_send_sem,
    ctx_recv_sem,
    near_send_sem,
    near_recv_sem,
    ctx_near_send_sem,
    ctx_near_recv_sem,
    relay_recv_sem,
    relay_send_sem,
):
    me = lax.axis_index("sp")
    n_batch, _, heads, seq_dev, head_dim = send.shape[1:]
    width = x_hbm.shape[1]
    nb = n_batch // N_CHUNKS
    rows = nb * seq_dev
    ffn = w_up.shape[1]
    dests = QKV_HEADS // heads
    parts = n // dests
    blocks = 3 * parts

    def peer(step):
        return lax.bitwise_xor(me, step)

    def put(chunk, kind, to, frm):
        bs = pl.ds(chunk * nb, nb)
        return pltpu.make_async_remote_copy(
            src_ref=send.at[kind, bs, to],
            dst_ref=recv.at[kind, bs, :, frm],
            send_sem=send_sem.at[chunk, kind, to],
            recv_sem=recv_sem.at[chunk, kind, frm],
            device_id={"sp": to},
            device_id_type=pl.DeviceIdType.MESH,
        )

    def put_ctx(chunk, to, frm):
        bs = pl.ds(chunk * nb, nb)
        return pltpu.make_async_remote_copy(
            src_ref=ctx_send.at[bs, to],
            dst_ref=ctx_recv.at[bs, frm],
            send_sem=ctx_send_sem.at[chunk, to],
            recv_sem=ctx_recv_sem.at[chunk, frm],
            device_id={"sp": to},
            device_id_type=pl.DeviceIdType.MESH,
        )

    def put_relay(chunk, to, slot):
        bs = pl.ds(chunk * nb, nb)
        return pltpu.make_async_remote_copy(
            src_ref=ctx_send.at[bs, to],
            dst_ref=relay.at[bs, slot],
            send_sem=ctx_send_sem.at[chunk, to],
            recv_sem=relay_recv_sem.at[chunk, slot],
            device_id={"sp": to - FIRST},
            device_id_type=pl.DeviceIdType.MESH,
        )

    def forward(chunk, slot):
        bs = pl.ds(chunk * nb, nb)
        return pltpu.make_async_remote_copy(
            src_ref=relay.at[bs, slot],
            dst_ref=ctx_recv.at[bs, 2 * FIRST + slot],
            send_sem=relay_send_sem.at[chunk, slot],
            recv_sem=ctx_recv_sem.at[chunk, 2 * FIRST + slot],
            device_id={"sp": me + FIRST},
            device_id_type=pl.DeviceIdType.MESH,
        )

    def put_near(chunk, kind):
        bs = pl.ds(chunk * nb, nb)
        return pltpu.make_async_remote_copy(
            src_ref=send.at[kind, bs, pl.ds((1 - me) * dests, dests)],
            dst_ref=near.at[kind, bs],
            send_sem=near_send_sem.at[chunk, kind],
            recv_sem=near_recv_sem.at[chunk, kind],
            device_id={"sp": 1 - me},
            device_id_type=pl.DeviceIdType.MESH,
        )

    def put_ctx_near(chunk):
        bs = pl.ds(chunk * nb, nb)
        return pltpu.make_async_remote_copy(
            src_ref=ctx_near.at[bs, 1 - me],
            dst_ref=ctx_recv.at[bs, pl.ds(me * dests, dests)],
            send_sem=ctx_near_send_sem.at[chunk],
            recv_sem=ctx_near_recv_sem.at[chunk],
            device_id={"sp": 1 - me},
            device_id_type=pl.DeviceIdType.MESH,
        )

    is_first = me < FIRST

    def each_peer(do, lowest=0):
        for other in range(lowest, n):
            pl.when(other != me)(functools.partial(do, other))

    def qkv_phase(x_buf, h_attn, w_nat, w_cols, qkv_acc, out_buf, own):
        def get_x(chunk):
            return pltpu.make_async_copy(x_hbm.at[pl.ds(chunk * rows, rows)], x_buf, x_sem)

        def get_w(block):
            slot = lax.rem(block, 2)
            src = w_qkv.at[:, block // parts, pl.ds(lax.rem(block, parts) * QKV_HEADS, QKV_HEADS)]
            return pltpu.make_async_copy(src, w_nat.at[slot], w_sem.at[slot])

        def bounce(step):
            slot, block = lax.rem(step, 2), lax.rem(step, blocks)
            dst = send.at[
                block // parts, pl.ds(step // blocks * nb, nb), pl.ds(lax.rem(block, parts) * dests, dests)
            ]
            return pltpu.make_async_copy(out_buf.at[slot], dst, bounce_sem.at[slot])

        def put_own(chunk, kind):
            dst = recv.at[kind, pl.ds(chunk * nb, nb), :, me]
            return pltpu.make_async_copy(own.at[kind], dst, own_sem.at[kind])

        def send_block(step):
            bounce(step).wait()
            block = lax.rem(step, blocks)
            for d in range(dests):
                to = lax.rem(block, parts) * dests + lax.rem(me + d, dests)

                @pl.when((to != me) & jnp.logical_not(is_first & (block < parts)))
                def _():
                    put(step // blocks, block // parts, to, me).start()

            @pl.when(is_first & (lax.rem(block, parts) == 1 - me))
            def _():
                put_near(step // blocks, block // parts).start()

        get_x(0).start()
        get_w(0).start()
        barrier = pltpu.get_barrier_semaphore()
        for step in range(1, n):
            pl.semaphore_signal(
                barrier, inc=1, device_id={"sp": peer(step)}, device_id_type=pl.DeviceIdType.MESH
            )

        @pl.loop(0, N_CHUNKS * blocks)
        def _(step):
            chunk, block = step // blocks, lax.rem(step, blocks)
            kind, part = block // parts, lax.rem(block, parts)
            slot = lax.rem(step, 2)

            @pl.when(block == 0)
            def _():
                get_x(chunk).wait()

                @pl.loop(0, rows // 16)
                def _(i):
                    r = pl.ds(pl.multiple_of(i * 16, 16), 16)
                    g = pl.ds(pl.multiple_of(chunk * rows + i * 16, 16), 16)
                    xf = x_buf[r, :].astype(F32)
                    mean = jnp.sum(xf, axis=-1, keepdims=True) * (1.0 / width)
                    dev = xf - mean
                    var = jnp.sum(dev * dev, axis=-1, keepdims=True) * (1.0 / width)
                    unit = dev * lax.rsqrt(var + LN_EPS)
                    h_attn[r, :] = (unit * ln_aw[...] + ln_ab[...]).astype(BF16)
                    h_mlp[g, :] = (unit * ln_mw[...] + ln_mb[...]).astype(BF16)
                    acc[g, :] = xf

                @pl.when(chunk + 1 < N_CHUNKS)
                def _():
                    get_x(chunk + 1).start()

            @pl.when(chunk == 0)
            def _():
                get_w(block).wait()

                @pl.when(block + 1 < blocks)
                def _():
                    get_w(block + 1).start()

                @pl.loop(0, width // 128)
                def _(i):
                    r = pl.ds(pl.multiple_of(i * 128, 128), 128)
                    by_head = jnp.swapaxes(w_nat[slot, r].astype(F32), 0, 1)
                    for h in range(QKV_HEADS):
                        w_cols[block, r, h * head_dim : (h + 1) * head_dim] = by_head[h].astype(BF16)

            qkv_acc[...] = jnp.dot(h_attn[...], w_cols[block], preferred_element_type=F32)

            def take(b, h):
                u = qkv_acc[b * seq_dev : (b + 1) * seq_dev, h * head_dim : (h + 1) * head_dim]
                return u.astype(BF16)

            @pl.when(kind < 2)
            def _():
                for h in range(QKV_HEADS):
                    for b in range(nb):
                        u = take(b, h).astype(F32)
                        u = u * cos_ref[...] + pltpu.roll(u, head_dim // 2, 1) * sin_ref[...]
                        out_buf[slot, b, h // heads, h % heads] = u.astype(BF16)

            @pl.when(kind == 2)
            def _():
                for h in range(QKV_HEADS):
                    for b in range(nb):
                        out_buf[slot, b, h // heads, h % heads] = take(b, h)

            bounce(step).start()

            @pl.when(me // dests == part)
            def _():
                @pl.when(chunk > 0)
                def _():
                    put_own(chunk - 1, kind).wait()

                own[kind] = out_buf[slot, :, lax.rem(me, dests)]
                put_own(chunk, kind).start()

            @pl.when(step == 0)
            def _():
                pl.semaphore_wait(barrier, n - 1)

            @pl.when(step > 0)
            def _():
                send_block(step - 1)

        send_block(N_CHUNKS * blocks - 1)
        for kind in range(3):
            put_own(N_CHUNKS - 1, kind).wait()

    pl.run_scoped(
        qkv_phase,
        pltpu.VMEM((rows, width), BF16),
        pltpu.VMEM((rows, width), BF16),
        pltpu.VMEM((2, width, QKV_HEADS, head_dim), BF16),
        pltpu.VMEM((blocks, width, QKV_HEADS * head_dim), BF16),
        pltpu.VMEM((rows, QKV_HEADS * head_dim), F32),
        pltpu.VMEM((2, nb, dests, heads, seq_dev, head_dim), BF16),
        pltpu.VMEM((3, nb, heads, seq_dev, head_dim), BF16),
    )

    def rest(w_buf, ctx_buf, ctx_rows, y_buf, both, own_ctx, own_near):
        def put_own_ctx(chunk):
            return pltpu.make_async_copy(own_ctx, ctx_recv.at[pl.ds(chunk * nb, nb), me], own_sem.at[3])

        def put_own_near(chunk):
            dst = ctx_recv.at[pl.ds(chunk * nb, nb), pl.ds(me * dests, dests)]
            return pltpu.make_async_copy(own_near, dst, own_sem.at[4])

        def get_w_out():
            return pltpu.make_async_copy(w_out, w_buf, w_sem.at[0])

        def put_y(chunk):
            return pltpu.make_async_copy(y_buf, y_hbm.at[pl.ds(chunk * rows, rows)], out_sem)

        get_w_out().start()

        @pl.loop(0, N_CHUNKS)
        def _(chunk):
            def mlp_body(up_ref, down_ref):
                for r in range(n_batch * seq_dev // 512):
                    rs = pl.ds(r * 512, 512)
                    up = jnp.dot(h_mlp[rs, :], up_ref[...], preferred_element_type=F32)
                    hid = (0.5 * up * (1.0 + lax.erf(up * 0.5**0.5))).astype(BF16)
                    acc[rs, :] += jnp.dot(hid, down_ref[...], preferred_element_type=F32)

            steps = ffn // UP_TILE // N_CHUNKS
            pltpu.emit_pipeline(
                mlp_body,
                grid=(steps,),
                in_specs=[
                    pl.BlockSpec((width, UP_TILE), lambda f: (0, chunk * steps + f)),
                    pl.BlockSpec((UP_TILE, width), lambda f: (chunk * steps + f, 0)),
                ],
            )(w_up, w_down)

            @pl.when(is_first)
            def _():
                for kind in range(3):
                    put_near(chunk, kind).wait_recv()

                @pl.when(chunk > 0)
                def _():
                    put_own_near(chunk - 1).wait()

                def near_body(q_own, k_own, v_own, q_other, k_other, v_other, o_ref):
                    b = pl.program_id(0)
                    for kind, (own, other) in enumerate(
                        ((q_own, q_other), (k_own, k_other), (v_own, v_other))
                    ):
                        both[kind, :, :, me] = own[0, 0]
                        both[kind, :, :, 1 - me] = other[0, 0]
                    for d in range(dests):
                        for h in range(heads):
                            q, k, v = (both[t, d, h].reshape(Q_TILE, head_dim) for t in range(3))

                            def write(i, out):
                                o_ref[0, :, d, h] = out.reshape(FIRST, seq_dev, head_dim)

                            causal_head(q, k, v, write)
                    own_near[b] = o_ref[0, me]

                block = (1, 1, dests, heads, seq_dev, head_dim)
                own_spec = lambda t: pl.BlockSpec(block, lambda b: (t, chunk * nb + b, me, 0, 0, 0))
                other_spec = lambda t: pl.BlockSpec(block, lambda b: (t, chunk * nb + b, 0, 0, 0, 0))
                pltpu.emit_pipeline(
                    near_body,
                    grid=(nb,),
                    in_specs=[own_spec(t) for t in range(3)] + [other_spec(t) for t in range(3)],
                    out_specs=[
                        pl.BlockSpec(
                            (1, FIRST, dests, heads, seq_dev, head_dim),
                            lambda b: (chunk * nb + b, 0, 0, 0, 0, 0),
                        )
                    ],
                )(send, send, send, near, near, near, ctx_near)
                put_ctx_near(chunk).start()
                put_own_near(chunk).start()

            each_peer(lambda other: put(chunk, 0, me, other).wait_recv(), FIRST)
            each_peer(lambda other: put(chunk, 1, me, other).wait_recv())
            each_peer(lambda other: put(chunk, 2, me, other).wait_recv())

            @pl.when((chunk > 0) & jnp.logical_not(is_first))
            def _():
                put_own_ctx(chunk - 1).wait()

            def attn_body(q_ref, k_ref, v_ref, o_ref):
                b, h = pl.program_id(0), pl.program_id(1)
                flat = lambda ref: ref[...].reshape(-1, head_dim)
                per = Q_TILE // seq_dev

                def write(i, out):
                    o_ref[0, i * per : (i + 1) * per, 0] = out.reshape(per, seq_dev, head_dim)

                causal_head(flat(q_ref), flat(k_ref), flat(v_ref), write)

                @pl.when(jnp.logical_not(is_first))
                def _():
                    own_ctx[b, h] = o_ref[0, me - FIRST, 0]

            later = n - FIRST
            spec = lambda count: pl.BlockSpec(
                (1, 1, count, seq_dev, head_dim), lambda b, h: (chunk * nb + b, h, 0, 0, 0)
            )
            pltpu.emit_pipeline(
                attn_body,
                grid=(nb, heads),
                in_specs=[spec(later), spec(n), spec(n)],
                out_specs=[
                    pl.BlockSpec((1, later, 1, seq_dev, head_dim), lambda b, h: (chunk * nb + b, 0, h, 0, 0))
                ],
            )(
                recv.at[0, :, :, pl.ds(FIRST, later)],
                recv.at[1],
                recv.at[2],
                ctx_send.at[:, pl.ds(FIRST, later)],
            )
            relays = (me // FIRST == 2) & (chunk < RELAYED)

            def send_ctx(other):
                if other // FIRST == 1:

                    @pl.when(relays)
                    def _():
                        put_relay(chunk, other, me - 2 * FIRST).start()

                    @pl.when(jnp.logical_not(relays))
                    def _():
                        put_ctx(chunk, other, me).start()

                else:
                    put_ctx(chunk, other, me).start()

            each_peer(send_ctx, FIRST)

            @pl.when(jnp.logical_not(is_first))
            def _():
                put_own_ctx(chunk).start()

        @pl.when(is_first)
        def _():
            put_own_near(N_CHUNKS - 1).wait()

        @pl.when(jnp.logical_not(is_first))
        def _():
            put_own_ctx(N_CHUNKS - 1).wait()

        get_w_out().wait()

        @pl.loop(0, N_CHUNKS)
        def _(chunk):
            @pl.when(is_first)
            def _():
                @pl.when(chunk < RELAYED)
                def _():
                    for slot in range(FIRST):
                        put_relay(chunk, me + FIRST, slot).wait_recv()
                        forward(chunk, slot).start()

                put_ctx_near(chunk).wait_recv()

            @pl.when(jnp.logical_not(is_first))
            def _():
                each_peer(lambda other: put_ctx(chunk, me, other).wait_recv())

            get_ctx = pltpu.make_async_copy(ctx_recv.at[pl.ds(chunk * nb, nb)], ctx_buf, x_sem)
            get_ctx.start()
            get_ctx.wait()
            for b in range(nb):
                for s in range(n):
                    for h in range(heads):
                        col = (s * heads + h) * head_dim
                        ctx_rows[b * seq_dev : (b + 1) * seq_dev, col : col + head_dim] = ctx_buf[b, s, h]

            @pl.when(chunk > 0)
            def _():
                put_y(chunk - 1).wait()

            g = pl.ds(pl.multiple_of(chunk * rows, rows), rows)
            for c in range(0, width, 1024):
                cs = slice(c, c + 1024)
                attn = jnp.dot(ctx_rows[...], w_buf[:, cs], preferred_element_type=F32)
                y_buf[:, cs] = (acc[g, cs] + attn).astype(BF16)
            put_y(chunk).start()

        put_y(N_CHUNKS - 1).wait()

    pl.run_scoped(
        rest,
        pltpu.VMEM((width, width), BF16),
        pltpu.VMEM((nb, n, heads, seq_dev, head_dim), BF16),
        pltpu.VMEM((rows, width), BF16),
        pltpu.VMEM((rows, width), BF16),
        pltpu.VMEM((3, dests, heads, FIRST, seq_dev, head_dim), BF16),
        pltpu.VMEM((nb, heads, seq_dev, head_dim), BF16),
        pltpu.VMEM((nb, dests, heads, seq_dev, head_dim), BF16),
    )

    @pl.loop(0, N_CHUNKS)
    def _(chunk):
        def sent(other):
            put(chunk, 1, other, me).wait_send()
            put(chunk, 2, other, me).wait_send()

        each_peer(sent)
        each_peer(lambda other: put_ctx(chunk, other, me).wait_send(), FIRST)

        @pl.when(is_first)
        def _():
            for kind in range(3):
                put_near(chunk, kind).wait_send()
            put_ctx_near(chunk).wait_send()

            @pl.when(chunk < RELAYED)
            def _():
                for slot in range(FIRST):
                    forward(chunk, slot).wait_send()

        @pl.when(jnp.logical_not(is_first))
        def _():
            each_peer(lambda other: put(chunk, 0, other, me).wait_send())


def solution(mesh):
    n = mesh.shape["sp"]

    def local_layer(x_blk, ln_attn_w, ln_attn_b, ln_mlp_w, ln_mlp_b, w_qkv, w_out, w_up, w_down):
        n_batch, seq_dev, width = x_blk.shape
        groups, head_dim = w_qkv.shape[1], w_qkv.shape[3]
        heads = groups // n
        nb = n_batch // N_CHUNKS
        rows = n_batch * seq_dev
        dests = QKV_HEADS // heads
        ffn = w_up.shape[1]
        q_pos = lax.axis_index("sp") * seq_dev + jnp.arange(seq_dev)
        cos_t, sin_t = rope_tables(q_pos, head_dim)
        row = lambda p: p.reshape(1, width)
        anywhere = pl.BlockSpec(memory_space=pl.ANY)
        vmem = pl.BlockSpec(memory_space=pltpu.VMEM)
        flops = 2 * rows * width * (3 * width + 2 * ffn) + 2 * rows * n * seq_dev * width * 2
        y_out, recv, *_ = pl.pallas_call(
            functools.partial(layer_kernel, n),
            out_shape=[
                jax.ShapeDtypeStruct((rows, width), BF16),
                jax.ShapeDtypeStruct((3, n_batch, heads, n, seq_dev, head_dim), BF16),
                jax.ShapeDtypeStruct((n_batch, n, heads, seq_dev, head_dim), BF16),
                jax.ShapeDtypeStruct((3, n_batch, n, heads, seq_dev, head_dim), BF16),
                jax.ShapeDtypeStruct((n_batch, n, heads, seq_dev, head_dim), BF16),
                jax.ShapeDtypeStruct((3, n_batch, dests, heads, seq_dev, head_dim), BF16),
                jax.ShapeDtypeStruct((n_batch, FIRST, dests, heads, seq_dev, head_dim), BF16),
                jax.ShapeDtypeStruct((n_batch, FIRST, heads, seq_dev, head_dim), BF16),
            ],
            in_specs=[anywhere] + [vmem] * 6 + [anywhere] * 4,
            out_specs=[anywhere] * 8,
            scratch_shapes=[
                pltpu.VMEM((rows, width), BF16),
                pltpu.VMEM((rows, width), F32),
                pltpu.SemaphoreType.DMA,
                pltpu.SemaphoreType.DMA((2,)),
                pltpu.SemaphoreType.DMA((2,)),
                pltpu.SemaphoreType.DMA((5,)),
                pltpu.SemaphoreType.DMA,
                pltpu.SemaphoreType.DMA((N_CHUNKS, 3, n)),
                pltpu.SemaphoreType.DMA((N_CHUNKS, 3, n)),
                pltpu.SemaphoreType.DMA((N_CHUNKS, n)),
                pltpu.SemaphoreType.DMA((N_CHUNKS, n)),
                pltpu.SemaphoreType.DMA((N_CHUNKS, 3)),
                pltpu.SemaphoreType.DMA((N_CHUNKS, 3)),
                pltpu.SemaphoreType.DMA((N_CHUNKS,)),
                pltpu.SemaphoreType.DMA((N_CHUNKS,)),
                pltpu.SemaphoreType.DMA((N_CHUNKS, FIRST)),
                pltpu.SemaphoreType.DMA((N_CHUNKS, FIRST)),
            ],
            compiler_params=pltpu.CompilerParams(
                collective_id=0, has_side_effects=True, vmem_limit_bytes=63 * 2**20
            ),
            cost_estimate=pl.CostEstimate(flops=flops, bytes_accessed=3 * 10**8, transcendentals=10**7),
            name="layer",
        )(
            x_blk.reshape(rows, width),
            cos_t,
            sin_t,
            row(ln_attn_w),
            row(ln_attn_b),
            row(ln_mlp_w),
            row(ln_mlp_b),
            w_qkv.transpose(0, 2, 1, 3),
            w_out,
            w_up,
            w_down,
        )
        shape = (n_batch, heads, n * seq_dev, head_dim)
        return y_out.reshape(x_blk.shape), recv[1].reshape(shape), recv[2].reshape(shape)

    act_spec, cache_spec = P("dp", "sp", None), P("dp", "sp", None, None)
    return jax.shard_map(
        local_layer,
        mesh=mesh,
        in_specs=(act_spec,) + (P(),) * 8,
        out_specs=(act_spec, cache_spec, cache_spec),
        check_vma=False,
    )
```

```python
import functools

import jax
import jax.numpy as jnp
from jax import lax
from jax.experimental import pallas as pl
from jax.experimental.pallas import tpu as pltpu
from jax.sharding import PartitionSpec as P

LN_EPS = 1e-5
ROPE_BASE = 10000.0
LOG2E = 1.4426950408889634
N_CHUNKS = 4
UP_TILE = 512
QKV_HEADS = 8
Q_TILE = 256
FIRST = 2
RELAYED = 3
F32 = jnp.float32
BF16 = jnp.bfloat16


def rope_tables(positions, head_dim):
    half_dim = head_dim // 2
    inv_freq = ROPE_BASE ** (-2.0 * jnp.arange(half_dim, dtype=F32) / head_dim)
    angles = positions.astype(F32)[:, None] * inv_freq[None, :]
    cos_t, sin_t = jnp.cos(angles), jnp.sin(angles)
    return jnp.concatenate([cos_t, cos_t], -1), jnp.concatenate([-sin_t, sin_t], -1)


def causal_head(q, k, v, write):
    seq, head_dim = k.shape
    scale = LOG2E * head_dim**-0.5
    keys = lax.broadcasted_iota(jnp.int32, (Q_TILE, Q_TILE), 0)
    queries = lax.broadcasted_iota(jnp.int32, (Q_TILE, Q_TILE), 1)
    for i in range(q.shape[0] // Q_TILE):
        lo = seq - q.shape[0] + i * Q_TILE
        hi = lo + Q_TILE
        q_i = q[i * Q_TILE : (i + 1) * Q_TILE]
        scores = lax.dot_general(k[:hi], q_i, (((1,), (1,)), ((), ())), preferred_element_type=F32)
        diag = jnp.where(keys <= queries, scores[lo:], -1e30)
        scores = jnp.concatenate([scores[:lo], diag], axis=0) if lo else diag
        prob = jnp.exp2((scores - jnp.max(scores, axis=0, keepdims=True)) * scale)
        prob = (prob * (1.0 / jnp.sum(prob, axis=0, keepdims=True))).astype(BF16)
        out = lax.dot_general(prob, v[:hi], (((0,), (0,)), ((), ())), preferred_element_type=F32)
        write(i, out.astype(BF16))


def layer_kernel(
    n,
    x_hbm,
    cos_ref,
    sin_ref,
    ln_aw,
    ln_ab,
    ln_mw,
    ln_mb,
    w_qkv,
    w_out,
    w_up,
    w_down,
    y_hbm,
    recv,
    ctx_recv,
    send,
    ctx_send,
    near,
    ctx_near,
    relay,
    h_mlp,
    acc,
    x_sem,
    w_sem,
    bounce_sem,
    own_sem,
    out_sem,
    up_sem,
    down_sem,
    qkv_sem,
    near_sem,
    send_sem,
    recv_sem,
    ctx_send_sem,
    ctx_recv_sem,
    near_send_sem,
    near_recv_sem,
    ctx_near_send_sem,
    ctx_near_recv_sem,
    relay_recv_sem,
    relay_send_sem,
):
    me = lax.axis_index("sp")
    n_batch, _, heads, seq_dev, head_dim = send.shape[1:]
    width = x_hbm.shape[1]
    nb = n_batch // N_CHUNKS
    rows = nb * seq_dev
    ffn = w_up.shape[1]
    dests = QKV_HEADS // heads
    parts = n // dests
    blocks = 3 * parts

    def peer(step):
        return lax.bitwise_xor(me, step)

    def put(chunk, kind, to, frm):
        bs = pl.ds(chunk * nb, nb)
        return pltpu.make_async_remote_copy(
            src_ref=send.at[kind, bs, to],
            dst_ref=recv.at[kind, bs, :, frm],
            send_sem=send_sem.at[chunk, kind, to],
            recv_sem=recv_sem.at[chunk, kind, frm],
            device_id={"sp": to},
            device_id_type=pl.DeviceIdType.MESH,
        )

    def put_ctx(chunk, to, frm):
        bs = pl.ds(chunk * nb, nb)
        return pltpu.make_async_remote_copy(
            src_ref=ctx_send.at[bs, to],
            dst_ref=ctx_recv.at[bs, frm],
            send_sem=ctx_send_sem.at[chunk, to],
            recv_sem=ctx_recv_sem.at[chunk, frm],
            device_id={"sp": to},
            device_id_type=pl.DeviceIdType.MESH,
        )

    def put_relay(chunk, to, slot):
        bs = pl.ds(chunk * nb, nb)
        return pltpu.make_async_remote_copy(
            src_ref=ctx_send.at[bs, to],
            dst_ref=relay.at[bs, slot],
            send_sem=ctx_send_sem.at[chunk, to],
            recv_sem=relay_recv_sem.at[chunk, slot],
            device_id={"sp": to - FIRST},
            device_id_type=pl.DeviceIdType.MESH,
        )

    def forward(chunk, slot):
        bs = pl.ds(chunk * nb, nb)
        return pltpu.make_async_remote_copy(
            src_ref=relay.at[bs, slot],
            dst_ref=ctx_recv.at[bs, 2 * FIRST + slot],
            send_sem=relay_send_sem.at[chunk, slot],
            recv_sem=ctx_recv_sem.at[chunk, 2 * FIRST + slot],
            device_id={"sp": me + FIRST},
            device_id_type=pl.DeviceIdType.MESH,
        )

    def put_near(chunk, kind):
        bs = pl.ds(chunk * nb, nb)
        return pltpu.make_async_remote_copy(
            src_ref=send.at[kind, bs, pl.ds((1 - me) * dests, dests)],
            dst_ref=near.at[kind, bs],
            send_sem=near_send_sem.at[chunk, kind],
            recv_sem=near_recv_sem.at[chunk, kind],
            device_id={"sp": 1 - me},
            device_id_type=pl.DeviceIdType.MESH,
        )

    def put_ctx_near(chunk):
        bs = pl.ds(chunk * nb, nb)
        return pltpu.make_async_remote_copy(
            src_ref=ctx_near.at[bs, 1 - me],
            dst_ref=ctx_recv.at[bs, pl.ds(me * dests, dests)],
            send_sem=ctx_near_send_sem.at[chunk],
            recv_sem=ctx_near_recv_sem.at[chunk],
            device_id={"sp": 1 - me},
            device_id_type=pl.DeviceIdType.MESH,
        )

    is_first = me < FIRST

    def each_peer(do, lowest=0):
        for other in range(lowest, n):
            pl.when(other != me)(functools.partial(do, other))

    def qkv_phase(x_buf, h_attn, w_nat, w_cols, out_buf, own):
        def get_x(chunk):
            return pltpu.make_async_copy(x_hbm.at[pl.ds(chunk * rows, rows)], x_buf, x_sem)

        def get_w(block):
            slot = lax.rem(block, 2)
            src = w_qkv.at[:, block // parts, pl.ds(lax.rem(block, parts) * QKV_HEADS, QKV_HEADS)]
            return pltpu.make_async_copy(src, w_nat.at[slot], w_sem.at[slot])

        def bounce(step):
            slot, block = lax.rem(step, 2), lax.rem(step, blocks)
            dst = send.at[
                block // parts, pl.ds(step // blocks * nb, nb), pl.ds(lax.rem(block, parts) * dests, dests)
            ]
            return pltpu.make_async_copy(out_buf.at[slot], dst, bounce_sem.at[slot])

        def put_own(chunk, kind):
            dst = recv.at[kind, pl.ds(chunk * nb, nb), :, me]
            return pltpu.make_async_copy(own.at[kind], dst, own_sem.at[kind])

        def send_block(step):
            bounce(step).wait()
            block = lax.rem(step, blocks)
            for d in range(dests):
                to = lax.rem(block, parts) * dests + lax.rem(me + d, dests)

                @pl.when((to != me) & jnp.logical_not(is_first & (block < parts)))
                def _():
                    put(step // blocks, block // parts, to, me).start()

            @pl.when(is_first & (lax.rem(block, parts) == 1 - me))
            def _():
                put_near(step // blocks, block // parts).start()

        get_x(0).start()
        get_w(0).start()
        barrier = pltpu.get_barrier_semaphore()
        for step in range(1, n):
            pl.semaphore_signal(
                barrier, inc=1, device_id={"sp": peer(step)}, device_id_type=pl.DeviceIdType.MESH
            )

        @pl.loop(0, N_CHUNKS * blocks)
        def _(step):
            chunk, block = step // blocks, lax.rem(step, blocks)
            kind, part = block // parts, lax.rem(block, parts)
            slot = lax.rem(step, 2)

            with jax.named_scope("ln"):
                @pl.when(block == 0)
                def _():
                    get_x(chunk).wait()

                    @pl.loop(0, nb)
                    def _(i):
                        r = pl.ds(pl.multiple_of(i * seq_dev, seq_dev), seq_dev)
                        g = pl.ds(pl.multiple_of(chunk * rows + i * seq_dev, seq_dev), seq_dev)
                        xf = x_buf[r, :].astype(F32)
                        mean = jnp.sum(xf, axis=-1, keepdims=True) * (1.0 / width)
                        dev = xf - mean
                        var = jnp.sum(dev * dev, axis=-1, keepdims=True) * (1.0 / width)
                        unit = dev * lax.rsqrt(var + LN_EPS)
                        h_attn[r, :] = (unit * ln_aw[...] + ln_ab[...]).astype(BF16)
                        h_mlp[g, :] = (unit * ln_mw[...] + ln_mb[...]).astype(BF16)
                        acc[g, :] = xf

                    @pl.when(chunk + 1 < N_CHUNKS)
                    def _():
                        get_x(chunk + 1).start()

            with jax.named_scope("relayout"):
                @pl.when(chunk == 0)
                def _():
                    get_w(block).wait()

                    @pl.when(block + 1 < blocks)
                    def _():
                        get_w(block + 1).start()

                    @pl.loop(0, width // 128)
                    def _(i):
                        r = pl.ds(pl.multiple_of(i * 128, 128), 128)
                        by_head = jnp.swapaxes(w_nat[slot, r].astype(F32), 0, 1)
                        for h in range(QKV_HEADS):
                            w_cols[block, r, h * head_dim : (h + 1) * head_dim] = by_head[h].astype(BF16)

            with jax.named_scope("qkv_dot"):
                for d in range(dests):
                    cs = slice(d * heads * head_dim, (d + 1) * heads * head_dim)
                    cols = jnp.dot(h_attn[...], w_cols[block, :, cs], preferred_element_type=F32)
                    for h in range(heads):
                        for b in range(nb):
                            u = cols[b * seq_dev : (b + 1) * seq_dev, h * head_dim : (h + 1) * head_dim]
                            u = u.astype(BF16).astype(F32)
                            turned = u * cos_ref[...] + pltpu.roll(u, head_dim // 2, 1) * sin_ref[...]
                            out_buf[slot, b, d, h] = jnp.where(kind < 2, turned, u).astype(BF16)

            with jax.named_scope("qkv_send"):
                bounce(step).start()

                @pl.when(me // dests == part)
                def _():
                    @pl.when(chunk > 0)
                    def _():
                        put_own(chunk - 1, kind).wait()

                    own[kind] = out_buf[slot, :, lax.rem(me, dests)]
                    put_own(chunk, kind).start()

                @pl.when(step == 0)
                def _():
                    pl.semaphore_wait(barrier, n - 1)

                @pl.when(step > 0)
                def _():
                    send_block(step - 1)

        send_block(N_CHUNKS * blocks - 1)
        for kind in range(3):
            put_own(N_CHUNKS - 1, kind).wait()

    pl.run_scoped(
        qkv_phase,
        pltpu.VMEM((rows, width), BF16),
        pltpu.VMEM((rows, width), BF16),
        pltpu.VMEM((2, width, QKV_HEADS, head_dim), BF16),
        pltpu.VMEM((blocks, width, QKV_HEADS * head_dim), BF16),
        pltpu.VMEM((2, nb, dests, heads, seq_dev, head_dim), BF16),
        pltpu.VMEM((3, nb, heads, seq_dev, head_dim), BF16),
    )

    def rest(up_buf, down_buf, w_buf, qkv_buf, ctx_buf, both, near_buf, ctx_in, ctx_rows, y_buf):
        later = n - FIRST
        steps = ffn // UP_TILE // N_CHUNKS

        def get_up(f):
            cols = pl.ds(pl.multiple_of(f * UP_TILE, UP_TILE), UP_TILE)
            slot = lax.rem(f, 2)
            return pltpu.make_async_copy(w_up.at[:, cols], up_buf.at[slot], up_sem.at[slot])

        def get_down(f):
            cols = pl.ds(pl.multiple_of(f * UP_TILE, UP_TILE), UP_TILE)
            slot = lax.rem(f, 2)
            return pltpu.make_async_copy(w_down.at[cols], down_buf.at[slot], down_sem.at[slot])

        def get_w_out():
            return pltpu.make_async_copy(w_out, w_buf, w_sem.at[0])

        def get_qkv(chunk, kind):
            return pltpu.make_async_copy(recv.at[kind, pl.ds(chunk * nb, nb)], qkv_buf.at[kind], qkv_sem.at[kind])

        def get_own_near(chunk, kind):
            src = send.at[kind, pl.ds(chunk * nb, nb), pl.ds(me * dests, dests)]
            return pltpu.make_async_copy(src, both.at[kind, :, :, :, me], near_sem.at[kind, 0])

        def get_other_near(chunk, kind):
            src = near.at[kind, pl.ds(chunk * nb, nb)]
            return pltpu.make_async_copy(src, both.at[kind, :, :, :, 1 - me], near_sem.at[kind, 1])

        def bounce_ctx(chunk):
            dst = ctx_send.at[pl.ds(chunk * nb, nb), pl.ds(FIRST, later)]
            return pltpu.make_async_copy(ctx_buf, dst, bounce_sem.at[0])

        def bounce_near(chunk):
            return pltpu.make_async_copy(near_buf, ctx_near.at[pl.ds(chunk * nb, nb)], bounce_sem.at[1])

        def put_own_ctx(chunk):
            dst = ctx_recv.at[pl.ds(chunk * nb, nb), me]
            return pltpu.make_async_copy(ctx_buf.at[:, me - FIRST], dst, own_sem.at[3])

        def put_own_near(chunk):
            dst = ctx_recv.at[pl.ds(chunk * nb, nb), pl.ds(me * dests, dests)]
            return pltpu.make_async_copy(near_buf.at[:, me], dst, own_sem.at[4])

        def put_y(chunk):
            return pltpu.make_async_copy(y_buf, y_hbm.at[pl.ds(chunk * rows, rows)], out_sem)

        def send_ctx(chunk):
            bounce_ctx(chunk).wait()
            relays = (me // FIRST == 2) & (chunk < RELAYED)

            def one(other):
                if other // FIRST == 1:

                    @pl.when(relays)
                    def _():
                        put_relay(chunk, other, me - 2 * FIRST).start()

                    @pl.when(jnp.logical_not(relays))
                    def _():
                        put_ctx(chunk, other, me).start()

                else:
                    put_ctx(chunk, other, me).start()

            each_peer(one, FIRST)

            @pl.when(jnp.logical_not(is_first))
            def _():
                put_own_ctx(chunk).wait()

            @pl.when(is_first)
            def _():
                bounce_near(chunk).wait()
                put_ctx_near(chunk).start()
                put_own_near(chunk).wait()

        get_up(0).start()
        get_down(0).start()
        get_w_out().start()

        @pl.loop(0, N_CHUNKS)
        def _(chunk):
            @pl.loop(0, steps)
            def _(j):
                f = chunk * steps + j
                slot = lax.rem(f, 2)

                @pl.when(f + 1 < N_CHUNKS * steps)
                def _():
                    get_up(f + 1).start()
                    get_down(f + 1).start()

                with jax.named_scope("wait_qkv"):
                    @pl.when(j == steps - 1)
                    def _():
                        each_peer(lambda other: put(chunk, 0, me, other).wait_recv(), FIRST)
                        each_peer(lambda other: put(chunk, 1, me, other).wait_recv())
                        each_peer(lambda other: put(chunk, 2, me, other).wait_recv())
                        for kind in range(3):
                            get_qkv(chunk, kind).start()

                        @pl.when(is_first)
                        def _():
                            for kind in range(3):
                                put_near(chunk, kind).wait_recv()
                                get_own_near(chunk, kind).start()
                                get_other_near(chunk, kind).start()

                with jax.named_scope("wait_w"):
                    get_up(f).wait()
                    get_down(f).wait()
                with jax.named_scope("mlp"):
                    for r in range(n_batch * seq_dev // 512):
                        rs = pl.ds(r * 512, 512)
                        up = jnp.dot(h_mlp[rs, :], up_buf[slot], preferred_element_type=F32)
                        hid = (0.5 * up * (1.0 + lax.erf(up * 0.5**0.5))).astype(BF16)
                        acc[rs, :] += jnp.dot(hid, down_buf[slot], preferred_element_type=F32)

                with jax.named_scope("send_ctx"):
                    @pl.when((j == 0) & (chunk > 0))
                    def _():
                        send_ctx(chunk - 1)

            with jax.named_scope("near"):
                @pl.when(is_first)
                def _():
                    for kind in range(3):
                        get_own_near(chunk, kind).wait()
                        get_other_near(chunk, kind).wait()

                    @pl.loop(0, nb)
                    def _(b):
                        for d in range(dests):
                            for h in range(heads):
                                q, k, v = (both[t, b, d, h].reshape(Q_TILE, head_dim) for t in range(3))

                                def write(i, out):
                                    near_buf[b, :, d, h] = out.reshape(FIRST, seq_dev, head_dim)

                                causal_head(q, k, v, write)

                    bounce_near(chunk).start()
                    put_own_near(chunk).start()

            with jax.named_scope("attn"):
                for kind in range(3):
                    get_qkv(chunk, kind).wait()
                for b in range(nb):
                    for h in range(heads):
                        q = qkv_buf[0, b, h, FIRST:].reshape(later * seq_dev, head_dim)
                        k, v = (qkv_buf[t, b, h].reshape(n * seq_dev, head_dim) for t in (1, 2))
                        per = Q_TILE // seq_dev

                        def write(i, out):
                            ctx_buf[b, i * per : (i + 1) * per, h] = out.reshape(per, seq_dev, head_dim)

                        causal_head(q, k, v, write)
            bounce_ctx(chunk).start()

            @pl.when(jnp.logical_not(is_first))
            def _():
                put_own_ctx(chunk).start()

        send_ctx(N_CHUNKS - 1)
        get_w_out().wait()

        @pl.loop(0, N_CHUNKS)
        def _(chunk):
            with jax.named_scope("wait_ctx"):
                @pl.when(is_first)
                def _():
                    @pl.when(chunk < RELAYED)
                    def _():
                        for slot in range(FIRST):
                            put_relay(chunk, me + FIRST, slot).wait_recv()
                            forward(chunk, slot).start()

                    put_ctx_near(chunk).wait_recv()

                @pl.when(jnp.logical_not(is_first))
                def _():
                    each_peer(lambda other: put_ctx(chunk, me, other).wait_recv())

            with jax.named_scope("out_proj"):
                get_ctx = pltpu.make_async_copy(ctx_recv.at[pl.ds(chunk * nb, nb)], ctx_in, x_sem)
                get_ctx.start()
                get_ctx.wait()
                for b in range(nb):
                    for s in range(n):
                        for h in range(heads):
                            col = (s * heads + h) * head_dim
                            ctx_rows[b * seq_dev : (b + 1) * seq_dev, col : col + head_dim] = ctx_in[b, s, h]

                @pl.when(chunk > 0)
                def _():
                    put_y(chunk - 1).wait()

                g = pl.ds(pl.multiple_of(chunk * rows, rows), rows)
                for c in range(0, width, 1024):
                    cs = slice(c, c + 1024)
                    attn = jnp.dot(ctx_rows[...], w_buf[:, cs], preferred_element_type=F32)
                    y_buf[:, cs] = (acc[g, cs] + attn).astype(BF16)
                put_y(chunk).start()

        put_y(N_CHUNKS - 1).wait()

    pl.run_scoped(
        rest,
        pltpu.VMEM((2, width, UP_TILE), BF16),
        pltpu.VMEM((2, UP_TILE, width), BF16),
        pltpu.VMEM((width, width), BF16),
        pltpu.VMEM((3, nb, heads, n, seq_dev, head_dim), BF16),
        pltpu.VMEM((nb, n - FIRST, heads, seq_dev, head_dim), BF16),
        pltpu.VMEM((3, nb, dests, heads, FIRST, seq_dev, head_dim), BF16),
        pltpu.VMEM((nb, FIRST, dests, heads, seq_dev, head_dim), BF16),
        pltpu.VMEM((nb, n, heads, seq_dev, head_dim), BF16),
        pltpu.VMEM((rows, width), BF16),
        pltpu.VMEM((rows, width), BF16),
    )

    @pl.loop(0, N_CHUNKS)
    def _(chunk):
        def sent(other):
            put(chunk, 1, other, me).wait_send()
            put(chunk, 2, other, me).wait_send()

        each_peer(sent)
        each_peer(lambda other: put_ctx(chunk, other, me).wait_send(), FIRST)

        @pl.when(is_first)
        def _():
            for kind in range(3):
                put_near(chunk, kind).wait_send()
            put_ctx_near(chunk).wait_send()

            @pl.when(chunk < RELAYED)
            def _():
                for slot in range(FIRST):
                    forward(chunk, slot).wait_send()

        @pl.when(jnp.logical_not(is_first))
        def _():
            each_peer(lambda other: put(chunk, 0, other, me).wait_send())


def solution(mesh):
    n = mesh.shape["sp"]

    def local_layer(x_blk, ln_attn_w, ln_attn_b, ln_mlp_w, ln_mlp_b, w_qkv, w_out, w_up, w_down):
        n_batch, seq_dev, width = x_blk.shape
        groups, head_dim = w_qkv.shape[1], w_qkv.shape[3]
        heads = groups // n
        nb = n_batch // N_CHUNKS
        rows = n_batch * seq_dev
        dests = QKV_HEADS // heads
        ffn = w_up.shape[1]
        q_pos = lax.axis_index("sp") * seq_dev + jnp.arange(seq_dev)
        cos_t, sin_t = rope_tables(q_pos, head_dim)
        row = lambda p: p.reshape(1, width)
        anywhere = pl.BlockSpec(memory_space=pl.ANY)
        vmem = pl.BlockSpec(memory_space=pltpu.VMEM)
        flops = 2 * rows * width * (3 * width + 2 * ffn) + 2 * rows * n * seq_dev * width * 2
        y_out, recv, *_ = pl.pallas_call(
            functools.partial(layer_kernel, n),
            out_shape=[
                jax.ShapeDtypeStruct((rows, width), BF16),
                jax.ShapeDtypeStruct((3, n_batch, heads, n, seq_dev, head_dim), BF16),
                jax.ShapeDtypeStruct((n_batch, n, heads, seq_dev, head_dim), BF16),
                jax.ShapeDtypeStruct((3, n_batch, n, heads, seq_dev, head_dim), BF16),
                jax.ShapeDtypeStruct((n_batch, n, heads, seq_dev, head_dim), BF16),
                jax.ShapeDtypeStruct((3, n_batch, dests, heads, seq_dev, head_dim), BF16),
                jax.ShapeDtypeStruct((n_batch, FIRST, dests, heads, seq_dev, head_dim), BF16),
                jax.ShapeDtypeStruct((n_batch, FIRST, heads, seq_dev, head_dim), BF16),
            ],
            in_specs=[anywhere] + [vmem] * 6 + [anywhere] * 4,
            out_specs=[anywhere] * 8,
            scratch_shapes=[
                pltpu.VMEM((rows, width), BF16),
                pltpu.VMEM((rows, width), F32),
                pltpu.SemaphoreType.DMA,
                pltpu.SemaphoreType.DMA((2,)),
                pltpu.SemaphoreType.DMA((2,)),
                pltpu.SemaphoreType.DMA((5,)),
                pltpu.SemaphoreType.DMA,
                pltpu.SemaphoreType.DMA((2,)),
                pltpu.SemaphoreType.DMA((2,)),
                pltpu.SemaphoreType.DMA((3,)),
                pltpu.SemaphoreType.DMA((3, 2)),
                pltpu.SemaphoreType.DMA((N_CHUNKS, 3, n)),
                pltpu.SemaphoreType.DMA((N_CHUNKS, 3, n)),
                pltpu.SemaphoreType.DMA((N_CHUNKS, n)),
                pltpu.SemaphoreType.DMA((N_CHUNKS, n)),
                pltpu.SemaphoreType.DMA((N_CHUNKS, 3)),
                pltpu.SemaphoreType.DMA((N_CHUNKS, 3)),
                pltpu.SemaphoreType.DMA((N_CHUNKS,)),
                pltpu.SemaphoreType.DMA((N_CHUNKS,)),
                pltpu.SemaphoreType.DMA((N_CHUNKS, FIRST)),
                pltpu.SemaphoreType.DMA((N_CHUNKS, FIRST)),
            ],
            compiler_params=pltpu.CompilerParams(
                collective_id=0, has_side_effects=True, vmem_limit_bytes=63 * 2**20
            ),
            cost_estimate=pl.CostEstimate(flops=flops, bytes_accessed=3 * 10**8, transcendentals=10**7),
            name="layer",
        )(
            x_blk.reshape(rows, width),
            cos_t,
            sin_t,
            row(ln_attn_w),
            row(ln_attn_b),
            row(ln_mlp_w),
            row(ln_mlp_b),
            w_qkv.transpose(0, 2, 1, 3),
            w_out,
            w_up,
            w_down,
        )
        shape = (n_batch, heads, n * seq_dev, head_dim)
        return y_out.reshape(x_blk.shape), recv[1].reshape(shape), recv[2].reshape(shape)

    act_spec, cache_spec = P("dp", "sp", None), P("dp", "sp", None, None)
    return jax.shard_map(
        local_layer,
        mesh=mesh,
        in_specs=(act_spec,) + (P(),) * 8,
        out_specs=(act_spec, cache_spec, cache_spec),
        check_vma=False,
    )
```

```python
import functools

import jax
import jax.numpy as jnp
import numpy as np
from jax import lax
from jax.experimental import pallas as pl
from jax.experimental.pallas import tpu as pltpu
from jax.sharding import PartitionSpec as P

LN_EPS = 1e-5
ROPE_BASE = 10000.0
LOG2E = 1.4426950408889634
N_CHUNKS = 6
UP_TILE = 512
QKV_HEADS = 8
Q_TILE = 256
FIRST = 2
RELAYED = 4
F32 = jnp.float32
BF16 = jnp.bfloat16


def rope_tables(positions, head_dim):
    half_dim = head_dim // 2
    inv_freq = np.float32(ROPE_BASE) ** (np.float32(-2.0) * np.arange(half_dim, dtype=np.float32) / np.float32(head_dim))
    angles = np.arange(positions, dtype=np.float32)[:, None] * inv_freq[None, :]
    cos_t, sin_t = np.cos(angles.astype(np.float64)), np.sin(angles.astype(np.float64))
    wide = lambda a, b: jnp.asarray(np.concatenate([a, b], -1).astype(np.float32))
    return wide(cos_t, cos_t), wide(-sin_t, sin_t)


def causal_head(q, k, v, write):
    seq, head_dim = k.shape
    scale = LOG2E * head_dim**-0.5
    keys = lax.broadcasted_iota(jnp.int32, (Q_TILE, Q_TILE), 0)
    queries = lax.broadcasted_iota(jnp.int32, (Q_TILE, Q_TILE), 1)
    for i in range(q.shape[0] // Q_TILE):
        lo = seq - q.shape[0] + i * Q_TILE
        hi = lo + Q_TILE
        q_i = q[i * Q_TILE : (i + 1) * Q_TILE]
        scores = lax.dot_general(k[:hi], q_i, (((1,), (1,)), ((), ())), preferred_element_type=F32)
        diag = jnp.where(keys <= queries, scores[lo:], -1e30)
        scores = jnp.concatenate([scores[:lo], diag], axis=0) if lo else diag
        prob = jnp.exp2((scores - jnp.max(scores, axis=0, keepdims=True)) * scale)
        prob = (prob * (1.0 / jnp.sum(prob, axis=0, keepdims=True))).astype(BF16)
        out = lax.dot_general(prob, v[:hi], (((0,), (0,)), ((), ())), preferred_element_type=F32)
        write(i, out.astype(BF16))


def layer_kernel(
    n,
    x_hbm,
    cos_hbm,
    sin_hbm,
    ln_aw,
    ln_ab,
    ln_mw,
    ln_mb,
    w_qkv,
    w_out,
    w_up,
    w_down,
    y_hbm,
    recv,
    ctx_recv,
    send,
    ctx_send,
    near,
    ctx_near,
    relay,
    h_mlp,
    acc,
    x_sem,
    w_sem,
    bounce_sem,
    own_sem,
    out_sem,
    up_sem,
    down_sem,
    qkv_sem,
    near_sem,
    send_sem,
    recv_sem,
    ctx_send_sem,
    ctx_recv_sem,
    near_send_sem,
    near_recv_sem,
    ctx_near_send_sem,
    ctx_near_recv_sem,
    relay_recv_sem,
    relay_send_sem,
):
    me = lax.axis_index("sp")
    n_batch, _, heads, seq_dev, head_dim = send.shape[1:]
    width = x_hbm.shape[1]
    nb = n_batch // N_CHUNKS
    rows = nb * seq_dev
    ffn = w_up.shape[1]
    dests = QKV_HEADS // heads
    parts = n // dests
    blocks = 3 * parts

    def peer(step):
        return lax.bitwise_xor(me, step)

    def put(chunk, kind, to, frm):
        bs = pl.ds(chunk * nb, nb)
        return pltpu.make_async_remote_copy(
            src_ref=send.at[kind, bs, to],
            dst_ref=recv.at[kind, bs, :, frm],
            send_sem=send_sem.at[chunk, kind, to],
            recv_sem=recv_sem.at[chunk, kind, frm],
            device_id={"sp": to},
            device_id_type=pl.DeviceIdType.MESH,
        )

    def put_ctx(chunk, to, frm):
        bs = pl.ds(chunk * nb, nb)
        return pltpu.make_async_remote_copy(
            src_ref=ctx_send.at[bs, to],
            dst_ref=ctx_recv.at[bs, frm],
            send_sem=ctx_send_sem.at[chunk, to],
            recv_sem=ctx_recv_sem.at[chunk, frm],
            device_id={"sp": to},
            device_id_type=pl.DeviceIdType.MESH,
        )

    def put_relay(chunk, to, slot):
        bs = pl.ds(chunk * nb, nb)
        return pltpu.make_async_remote_copy(
            src_ref=ctx_send.at[bs, to],
            dst_ref=relay.at[bs, slot],
            send_sem=ctx_send_sem.at[chunk, to],
            recv_sem=relay_recv_sem.at[chunk, slot],
            device_id={"sp": to - FIRST},
            device_id_type=pl.DeviceIdType.MESH,
        )

    def forward(chunk, slot):
        bs = pl.ds(chunk * nb, nb)
        return pltpu.make_async_remote_copy(
            src_ref=relay.at[bs, slot],
            dst_ref=ctx_recv.at[bs, 2 * FIRST + slot],
            send_sem=relay_send_sem.at[chunk, slot],
            recv_sem=ctx_recv_sem.at[chunk, 2 * FIRST + slot],
            device_id={"sp": me + FIRST},
            device_id_type=pl.DeviceIdType.MESH,
        )

    def put_near(chunk, kind):
        bs = pl.ds(chunk * nb, nb)
        return pltpu.make_async_remote_copy(
            src_ref=send.at[kind, bs, pl.ds((1 - me) * dests, dests)],
            dst_ref=near.at[kind, bs],
            send_sem=near_send_sem.at[chunk, kind],
            recv_sem=near_recv_sem.at[chunk, kind],
            device_id={"sp": 1 - me},
            device_id_type=pl.DeviceIdType.MESH,
        )

    def put_ctx_near(chunk):
        bs = pl.ds(chunk * nb, nb)
        return pltpu.make_async_remote_copy(
            src_ref=ctx_near.at[bs, 1 - me],
            dst_ref=ctx_recv.at[bs, pl.ds(me * dests, dests)],
            send_sem=ctx_near_send_sem.at[chunk],
            recv_sem=ctx_near_recv_sem.at[chunk],
            device_id={"sp": 1 - me},
            device_id_type=pl.DeviceIdType.MESH,
        )

    is_first = me < FIRST

    def each_peer(do, lowest=0):
        for other in range(lowest, n):
            pl.when(other != me)(functools.partial(do, other))

    def qkv_phase(x_buf, h_attn, w_nat, w_cols, out_buf, own, cos_ref, sin_ref):
        mine = pl.ds(pl.multiple_of(me * seq_dev, seq_dev), seq_dev)
        get_cos = pltpu.make_async_copy(cos_hbm.at[mine], cos_ref, own_sem.at[3])
        get_sin = pltpu.make_async_copy(sin_hbm.at[mine], sin_ref, own_sem.at[4])

        def get_x(chunk):
            return pltpu.make_async_copy(x_hbm.at[pl.ds(chunk * rows, rows)], x_buf, x_sem)

        def get_w(block):
            slot = lax.rem(block, 2)
            src = w_qkv.at[:, block // parts, pl.ds(lax.rem(block, parts) * QKV_HEADS, QKV_HEADS)]
            return pltpu.make_async_copy(src, w_nat.at[slot], w_sem.at[slot])

        def bounce(step):
            slot, block = lax.rem(step, 2), lax.rem(step, blocks)
            dst = send.at[
                block // parts, pl.ds(step // blocks * nb, nb), pl.ds(lax.rem(block, parts) * dests, dests)
            ]
            return pltpu.make_async_copy(out_buf.at[slot], dst, bounce_sem.at[slot])

        def put_own(chunk, kind):
            dst = recv.at[kind, pl.ds(chunk * nb, nb), :, me]
            return pltpu.make_async_copy(own.at[kind], dst, own_sem.at[kind])

        def send_block(step):
            bounce(step).wait()
            block = lax.rem(step, blocks)
            for d in range(dests):
                to = lax.rem(block, parts) * dests + lax.rem(me + d, dests)

                @pl.when((to != me) & jnp.logical_not(is_first & (block < parts)))
                def _():
                    put(step // blocks, block // parts, to, me).start()

            @pl.when(is_first & (lax.rem(block, parts) == 1 - me))
            def _():
                put_near(step // blocks, block // parts).start()

        get_x(0).start()
        get_w(0).start()
        get_cos.start()
        get_sin.start()
        barrier = pltpu.get_barrier_semaphore()
        for step in range(1, n):
            pl.semaphore_signal(
                barrier, inc=1, device_id={"sp": peer(step)}, device_id_type=pl.DeviceIdType.MESH
            )

        get_cos.wait()
        get_sin.wait()

        @pl.loop(0, N_CHUNKS * blocks)
        def _(step):
            chunk, block = step // blocks, lax.rem(step, blocks)
            kind, part = block // parts, lax.rem(block, parts)
            slot = lax.rem(step, 2)

            with jax.named_scope("ln"):
                @pl.when(block == 0)
                def _():
                    get_x(chunk).wait()

                    @pl.loop(0, nb)
                    def _(i):
                        r = pl.ds(pl.multiple_of(i * seq_dev, seq_dev), seq_dev)
                        g = pl.ds(pl.multiple_of(chunk * rows + i * seq_dev, seq_dev), seq_dev)
                        xf = x_buf[r, :].astype(F32)
                        mean = jnp.sum(xf, axis=-1, keepdims=True) * (1.0 / width)
                        dev = xf - mean
                        var = jnp.sum(dev * dev, axis=-1, keepdims=True) * (1.0 / width)
                        unit = dev * lax.rsqrt(var + LN_EPS)
                        h_attn[r, :] = (unit * ln_aw[...] + ln_ab[...]).astype(BF16)
                        h_mlp[g, :] = (unit * ln_mw[...] + ln_mb[...]).astype(BF16)
                        acc[g, :] = xf

                    @pl.when(chunk + 1 < N_CHUNKS)
                    def _():
                        get_x(chunk + 1).start()

            with jax.named_scope("relayout"):
                @pl.when(chunk == 0)
                def _():
                    get_w(block).wait()

                    @pl.when(block + 1 < blocks)
                    def _():
                        get_w(block + 1).start()

                    @pl.loop(0, width // 128)
                    def _(i):
                        r = pl.ds(pl.multiple_of(i * 128, 128), 128)
                        by_head = jnp.swapaxes(w_nat[slot, r].astype(F32), 0, 1)
                        for h in range(QKV_HEADS):
                            w_cols[block, r, h * head_dim : (h + 1) * head_dim] = by_head[h].astype(BF16)

            with jax.named_scope("qkv_dot"):
                for d in range(dests):
                    cs = slice(d * heads * head_dim, (d + 1) * heads * head_dim)
                    cols = jnp.dot(h_attn[...], w_cols[block, :, cs], preferred_element_type=F32)
                    for h in range(heads):
                        for b in range(nb):
                            u = cols[b * seq_dev : (b + 1) * seq_dev, h * head_dim : (h + 1) * head_dim]
                            u = u.astype(BF16).astype(F32)
                            turned = u * cos_ref[...] + pltpu.roll(u, head_dim // 2, 1) * sin_ref[...]
                            out_buf[slot, b, d, h] = jnp.where(kind < 2, turned, u).astype(BF16)

            with jax.named_scope("qkv_send"):
                bounce(step).start()

                @pl.when(me // dests == part)
                def _():
                    @pl.when(chunk > 0)
                    def _():
                        put_own(chunk - 1, kind).wait()

                    own[kind] = out_buf[slot, :, lax.rem(me, dests)]
                    put_own(chunk, kind).start()

                @pl.when(step == 0)
                def _():
                    pl.semaphore_wait(barrier, n - 1)

                @pl.when(chunk == 0)
                def _():
                    send_block(step)

                @pl.when(step > blocks)
                def _():
                    send_block(step - 1)

        send_block(N_CHUNKS * blocks - 1)
        for kind in range(3):
            put_own(N_CHUNKS - 1, kind).wait()

    pl.run_scoped(
        qkv_phase,
        pltpu.VMEM((rows, width), BF16),
        pltpu.VMEM((rows, width), BF16),
        pltpu.VMEM((2, width, QKV_HEADS, head_dim), BF16),
        pltpu.VMEM((blocks, width, QKV_HEADS * head_dim), BF16),
        pltpu.VMEM((2, nb, dests, heads, seq_dev, head_dim), BF16),
        pltpu.VMEM((3, nb, heads, seq_dev, head_dim), BF16),
        pltpu.VMEM((seq_dev, head_dim), F32),
        pltpu.VMEM((seq_dev, head_dim), F32),
    )

    def rest(up_buf, down_buf, w_buf, qkv_buf, ctx_buf, both, near_buf, ctx_in, ctx_rows, y_buf):
        later = n - FIRST
        steps = ffn // UP_TILE

        def get_up(f):
            cols = pl.ds(pl.multiple_of(f * UP_TILE, UP_TILE), UP_TILE)
            slot = lax.rem(f, 2)
            return pltpu.make_async_copy(w_up.at[:, cols], up_buf.at[slot], up_sem.at[slot])

        def get_down(f):
            cols = pl.ds(pl.multiple_of(f * UP_TILE, UP_TILE), UP_TILE)
            slot = lax.rem(f, 2)
            return pltpu.make_async_copy(w_down.at[cols], down_buf.at[slot], down_sem.at[slot])

        def get_w_out():
            return pltpu.make_async_copy(w_out, w_buf, w_sem.at[0])

        def get_qkv(chunk, kind):
            return pltpu.make_async_copy(recv.at[kind, pl.ds(chunk * nb, nb)], qkv_buf.at[kind], qkv_sem.at[kind])

        def get_own_near(chunk, kind):
            src = send.at[kind, pl.ds(chunk * nb, nb), pl.ds(me * dests, dests)]
            return pltpu.make_async_copy(src, both.at[kind, :, :, :, me], near_sem.at[kind, 0])

        def get_other_near(chunk, kind):
            src = near.at[kind, pl.ds(chunk * nb, nb)]
            return pltpu.make_async_copy(src, both.at[kind, :, :, :, 1 - me], near_sem.at[kind, 1])

        def bounce_ctx(chunk):
            dst = ctx_send.at[pl.ds(chunk * nb, nb), pl.ds(FIRST, later)]
            return pltpu.make_async_copy(ctx_buf, dst, bounce_sem.at[0])

        def bounce_near(chunk):
            return pltpu.make_async_copy(near_buf, ctx_near.at[pl.ds(chunk * nb, nb)], bounce_sem.at[1])

        def put_own_ctx(chunk):
            dst = ctx_recv.at[pl.ds(chunk * nb, nb), me]
            return pltpu.make_async_copy(ctx_buf.at[:, me - FIRST], dst, own_sem.at[3])

        def put_own_near(chunk):
            dst = ctx_recv.at[pl.ds(chunk * nb, nb), pl.ds(me * dests, dests)]
            return pltpu.make_async_copy(near_buf.at[:, me], dst, own_sem.at[4])

        def put_y(chunk):
            return pltpu.make_async_copy(y_buf, y_hbm.at[pl.ds(chunk * rows, rows)], out_sem)

        def send_ctx(chunk):
            bounce_ctx(chunk).wait()
            relays = (me // FIRST == 2) & (chunk < RELAYED)

            def one(other):
                if other // FIRST == 1:

                    @pl.when(relays)
                    def _():
                        put_relay(chunk, other, me - 2 * FIRST).start()

                    @pl.when(jnp.logical_not(relays))
                    def _():
                        put_ctx(chunk, other, me).start()

                else:
                    put_ctx(chunk, other, me).start()

            each_peer(one, FIRST)

            @pl.when(jnp.logical_not(is_first))
            def _():
                put_own_ctx(chunk).wait()

            @pl.when(is_first)
            def _():
                bounce_near(chunk).wait()
                put_ctx_near(chunk).start()
                put_own_near(chunk).wait()

        get_up(0).start()
        get_down(0).start()
        get_w_out().start()

        @pl.loop(0, N_CHUNKS)
        def _(chunk):
            first, last = chunk * steps // N_CHUNKS, (chunk + 1) * steps // N_CHUNKS

            @pl.loop(first, last)
            def _(f):
                slot = lax.rem(f, 2)

                @pl.when(f + 1 < steps)
                def _():
                    get_up(f + 1).start()
                    get_down(f + 1).start()

                with jax.named_scope("wait_qkv"):
                    @pl.when(f == last - 1)
                    def _():
                        each_peer(lambda other: put(chunk, 0, me, other).wait_recv(), FIRST)
                        each_peer(lambda other: put(chunk, 1, me, other).wait_recv())
                        each_peer(lambda other: put(chunk, 2, me, other).wait_recv())
                        for kind in range(3):
                            get_qkv(chunk, kind).start()

                        @pl.when(is_first)
                        def _():
                            for kind in range(3):
                                put_near(chunk, kind).wait_recv()
                                get_own_near(chunk, kind).start()
                                get_other_near(chunk, kind).start()

                with jax.named_scope("wait_w"):
                    get_up(f).wait()
                    get_down(f).wait()
                with jax.named_scope("mlp"):
                    for r in range(n_batch * seq_dev // 512):
                        rs = pl.ds(r * 512, 512)
                        up = jnp.dot(h_mlp[rs, :], up_buf[slot], preferred_element_type=F32)
                        hid = (0.5 * up * (1.0 + lax.erf(up * 0.5**0.5))).astype(BF16)
                        acc[rs, :] += jnp.dot(hid, down_buf[slot], preferred_element_type=F32)

                with jax.named_scope("send_ctx"):
                    @pl.when((f == first) & (chunk > 0))
                    def _():
                        send_ctx(chunk - 1)

            with jax.named_scope("near"):
                @pl.when(is_first)
                def _():
                    for kind in range(3):
                        get_own_near(chunk, kind).wait()
                        get_other_near(chunk, kind).wait()

                    @pl.loop(0, nb)
                    def _(b):
                        for d in range(dests):
                            for h in range(heads):
                                q, k, v = (both[t, b, d, h].reshape(Q_TILE, head_dim) for t in range(3))

                                def write(i, out):
                                    near_buf[b, :, d, h] = out.reshape(FIRST, seq_dev, head_dim)

                                causal_head(q, k, v, write)

                    bounce_near(chunk).start()
                    put_own_near(chunk).start()

            with jax.named_scope("attn"):
                for kind in range(3):
                    get_qkv(chunk, kind).wait()
                for b in range(nb):
                    for h in range(heads):
                        q = qkv_buf[0, b, h, FIRST:].reshape(later * seq_dev, head_dim)
                        k, v = (qkv_buf[t, b, h].reshape(n * seq_dev, head_dim) for t in (1, 2))
                        per = Q_TILE // seq_dev

                        def write(i, out):
                            ctx_buf[b, i * per : (i + 1) * per, h] = out.reshape(per, seq_dev, head_dim)

                        causal_head(q, k, v, write)
            bounce_ctx(chunk).start()

            @pl.when(jnp.logical_not(is_first))
            def _():
                put_own_ctx(chunk).start()

        @pl.when(is_first)
        def _():
            @pl.loop(0, RELAYED)
            def _(chunk):
                for slot in range(FIRST):
                    put_relay(chunk, me + FIRST, slot).wait_recv()
                    forward(chunk, slot).start()

        send_ctx(N_CHUNKS - 1)
        get_w_out().wait()

        @pl.loop(0, N_CHUNKS)
        def _(chunk):
            with jax.named_scope("wait_ctx"):
                @pl.when(is_first)
                def _():
                    put_ctx_near(chunk).wait_recv()

                @pl.when(jnp.logical_not(is_first))
                def _():
                    each_peer(lambda other: put_ctx(chunk, me, other).wait_recv())

            with jax.named_scope("out_proj"):
                get_ctx = pltpu.make_async_copy(ctx_recv.at[pl.ds(chunk * nb, nb)], ctx_in, x_sem)
                get_ctx.start()
                get_ctx.wait()
                for b in range(nb):
                    for s in range(n):
                        for h in range(heads):
                            col = (s * heads + h) * head_dim
                            ctx_rows[b * seq_dev : (b + 1) * seq_dev, col : col + head_dim] = ctx_in[b, s, h]

                @pl.when(chunk > 0)
                def _():
                    put_y(chunk - 1).wait()

                g = pl.ds(pl.multiple_of(chunk * rows, rows), rows)
                for c in range(0, width, 1024):
                    cs = slice(c, c + 1024)
                    attn = jnp.dot(ctx_rows[...], w_buf[:, cs], preferred_element_type=F32)
                    y_buf[:, cs] = (acc[g, cs] + attn).astype(BF16)
                put_y(chunk).start()

        put_y(N_CHUNKS - 1).wait()

    pl.run_scoped(
        rest,
        pltpu.VMEM((2, width, UP_TILE), BF16),
        pltpu.VMEM((2, UP_TILE, width), BF16),
        pltpu.VMEM((width, width), BF16),
        pltpu.VMEM((3, nb, heads, n, seq_dev, head_dim), BF16),
        pltpu.VMEM((nb, n - FIRST, heads, seq_dev, head_dim), BF16),
        pltpu.VMEM((3, nb, dests, heads, FIRST, seq_dev, head_dim), BF16),
        pltpu.VMEM((nb, FIRST, dests, heads, seq_dev, head_dim), BF16),
        pltpu.VMEM((nb, n, heads, seq_dev, head_dim), BF16),
        pltpu.VMEM((rows, width), BF16),
        pltpu.VMEM((rows, width), BF16),
    )

    @pl.loop(0, N_CHUNKS)
    def _(chunk):
        def sent(other):
            put(chunk, 1, other, me).wait_send()
            put(chunk, 2, other, me).wait_send()

        each_peer(sent)
        each_peer(lambda other: put_ctx(chunk, other, me).wait_send(), FIRST)

        @pl.when(is_first)
        def _():
            for kind in range(3):
                put_near(chunk, kind).wait_send()
            put_ctx_near(chunk).wait_send()

            @pl.when(chunk < RELAYED)
            def _():
                for slot in range(FIRST):
                    forward(chunk, slot).wait_send()

        @pl.when(jnp.logical_not(is_first))
        def _():
            each_peer(lambda other: put(chunk, 0, other, me).wait_send())


def solution(mesh):
    n = mesh.shape["sp"]

    def local_layer(x_blk, ln_attn_w, ln_attn_b, ln_mlp_w, ln_mlp_b, w_qkv, w_out, w_up, w_down):
        n_batch, seq_dev, width = x_blk.shape
        groups, head_dim = w_qkv.shape[1], w_qkv.shape[3]
        heads = groups // n
        nb = n_batch // N_CHUNKS
        rows = n_batch * seq_dev
        dests = QKV_HEADS // heads
        ffn = w_up.shape[1]
        cos_t, sin_t = rope_tables(n * seq_dev, head_dim)
        row = lambda p: p.reshape(1, width)
        anywhere = pl.BlockSpec(memory_space=pl.ANY)
        vmem = pl.BlockSpec(memory_space=pltpu.VMEM)
        flops = 2 * rows * width * (3 * width + 2 * ffn) + 2 * rows * n * seq_dev * width * 2
        y_out, recv, *_ = pl.pallas_call(
            functools.partial(layer_kernel, n),
            out_shape=[
                jax.ShapeDtypeStruct((rows, width), BF16),
                jax.ShapeDtypeStruct((3, n_batch, heads, n, seq_dev, head_dim), BF16),
                jax.ShapeDtypeStruct((n_batch, n, heads, seq_dev, head_dim), BF16),
                jax.ShapeDtypeStruct((3, n_batch, n, heads, seq_dev, head_dim), BF16),
                jax.ShapeDtypeStruct((n_batch, n, heads, seq_dev, head_dim), BF16),
                jax.ShapeDtypeStruct((3, n_batch, dests, heads, seq_dev, head_dim), BF16),
                jax.ShapeDtypeStruct((n_batch, FIRST, dests, heads, seq_dev, head_dim), BF16),
                jax.ShapeDtypeStruct((n_batch, FIRST, heads, seq_dev, head_dim), BF16),
            ],
            in_specs=[anywhere] * 3 + [vmem] * 4 + [anywhere] * 4,
            out_specs=[anywhere] * 8,
            scratch_shapes=[
                pltpu.VMEM((rows, width), BF16),
                pltpu.VMEM((rows, width), F32),
                pltpu.SemaphoreType.DMA,
                pltpu.SemaphoreType.DMA((2,)),
                pltpu.SemaphoreType.DMA((2,)),
                pltpu.SemaphoreType.DMA((5,)),
                pltpu.SemaphoreType.DMA,
                pltpu.SemaphoreType.DMA((2,)),
                pltpu.SemaphoreType.DMA((2,)),
                pltpu.SemaphoreType.DMA((3,)),
                pltpu.SemaphoreType.DMA((3, 2)),
                pltpu.SemaphoreType.DMA((N_CHUNKS, 3, n)),
                pltpu.SemaphoreType.DMA((N_CHUNKS, 3, n)),
                pltpu.SemaphoreType.DMA((N_CHUNKS, n)),
                pltpu.SemaphoreType.DMA((N_CHUNKS, n)),
                pltpu.SemaphoreType.DMA((N_CHUNKS, 3)),
                pltpu.SemaphoreType.DMA((N_CHUNKS, 3)),
                pltpu.SemaphoreType.DMA((N_CHUNKS,)),
                pltpu.SemaphoreType.DMA((N_CHUNKS,)),
                pltpu.SemaphoreType.DMA((N_CHUNKS, FIRST)),
                pltpu.SemaphoreType.DMA((N_CHUNKS, FIRST)),
            ],
            compiler_params=pltpu.CompilerParams(
                collective_id=0, has_side_effects=True, vmem_limit_bytes=63 * 2**20
            ),
            cost_estimate=pl.CostEstimate(flops=flops, bytes_accessed=3 * 10**8, transcendentals=10**7),
            name="layer",
        )(
            x_blk.reshape(rows, width),
            cos_t,
            sin_t,
            row(ln_attn_w),
            row(ln_attn_b),
            row(ln_mlp_w),
            row(ln_mlp_b),
            w_qkv.transpose(0, 2, 1, 3),
            w_out,
            w_up,
            w_down,
        )
        shape = (n_batch, heads, n * seq_dev, head_dim)
        return y_out.reshape(x_blk.shape), recv[1].reshape(shape), recv[2].reshape(shape)

    act_spec, cache_spec = P("dp", "sp", None), P("dp", "sp", None, None)
    return jax.shard_map(
        local_layer,
        mesh=mesh,
        in_specs=(act_spec,) + (P(),) * 8,
        out_specs=(act_spec, cache_spec, cache_spec),
        check_vma=False,
    )
```

```python
import functools

import jax
import jax.numpy as jnp
import numpy as np
from jax import lax
from jax.experimental import pallas as pl
from jax.experimental.pallas import tpu as pltpu
from jax.sharding import PartitionSpec as P

LN_EPS = 1e-5
ROPE_BASE = 10000.0
LOG2E = 1.4426950408889634
N_CHUNKS = 6
UP_TILE = 512
QKV_HEADS = 8
Q_TILE = 256
FIRST = 2
LATE_STEPS = 2
RELAYED = 4
F32 = jnp.float32
BF16 = jnp.bfloat16


def rope_tables(positions, head_dim):
    half_dim = head_dim // 2
    inv_freq = np.float32(ROPE_BASE) ** (np.float32(-2.0) * np.arange(half_dim, dtype=np.float32) / np.float32(head_dim))
    angles = np.arange(positions, dtype=np.float32)[:, None] * inv_freq[None, :]
    cos_t, sin_t = np.cos(angles.astype(np.float64)), np.sin(angles.astype(np.float64))
    wide = lambda a, b: jnp.asarray(np.concatenate([a, b], -1).astype(np.float32))
    return wide(cos_t, cos_t), wide(-sin_t, sin_t)


def causal_head(q, k, v, write):
    seq, head_dim = k.shape
    scale = LOG2E * head_dim**-0.5
    keys = lax.broadcasted_iota(jnp.int32, (Q_TILE, Q_TILE), 0)
    queries = lax.broadcasted_iota(jnp.int32, (Q_TILE, Q_TILE), 1)
    for i in range(q.shape[0] // Q_TILE):
        lo = seq - q.shape[0] + i * Q_TILE
        hi = lo + Q_TILE
        q_i = q[i * Q_TILE : (i + 1) * Q_TILE]
        scores = lax.dot_general(k[:hi], q_i, (((1,), (1,)), ((), ())), preferred_element_type=F32)
        diag = jnp.where(keys <= queries, scores[lo:], -1e30)
        scores = jnp.concatenate([scores[:lo], diag], axis=0) if lo else diag
        prob = jnp.exp2((scores - jnp.max(scores, axis=0, keepdims=True)) * scale)
        prob = (prob * (1.0 / jnp.sum(prob, axis=0, keepdims=True))).astype(BF16)
        out = lax.dot_general(prob, v[:hi], (((0,), (0,)), ((), ())), preferred_element_type=F32)
        write(i, out.astype(BF16))


def layer_kernel(
    n,
    x_hbm,
    cos_hbm,
    sin_hbm,
    ln_aw,
    ln_ab,
    ln_mw,
    ln_mb,
    w_qkv,
    w_out,
    w_up,
    w_down,
    y_hbm,
    recv,
    ctx_recv,
    send,
    ctx_send,
    near,
    ctx_near,
    relay,
    h_mlp,
    acc,
    x_sem,
    w_sem,
    bounce_sem,
    own_sem,
    out_sem,
    up_sem,
    down_sem,
    qkv_sem,
    near_sem,
    send_sem,
    recv_sem,
    ctx_send_sem,
    ctx_recv_sem,
    near_send_sem,
    near_recv_sem,
    ctx_near_send_sem,
    ctx_near_recv_sem,
    relay_recv_sem,
    relay_send_sem,
):
    me = lax.axis_index("sp")
    n_batch, _, heads, seq_dev, head_dim = send.shape[1:]
    width = x_hbm.shape[1]
    nb = n_batch // N_CHUNKS
    rows = nb * seq_dev
    ffn = w_up.shape[1]
    dests = QKV_HEADS // heads
    parts = n // dests
    blocks = 3 * parts

    def peer(step):
        return lax.bitwise_xor(me, step)

    def put(chunk, kind, to, frm):
        bs = pl.ds(chunk * nb, nb)
        return pltpu.make_async_remote_copy(
            src_ref=send.at[kind, bs, to],
            dst_ref=recv.at[kind, bs, :, frm],
            send_sem=send_sem.at[chunk, kind, to],
            recv_sem=recv_sem.at[chunk, kind, frm],
            device_id={"sp": to},
            device_id_type=pl.DeviceIdType.MESH,
        )

    def put_ctx(chunk, to, frm):
        bs = pl.ds(chunk * nb, nb)
        return pltpu.make_async_remote_copy(
            src_ref=ctx_send.at[bs, to],
            dst_ref=ctx_recv.at[bs, frm],
            send_sem=ctx_send_sem.at[chunk, to],
            recv_sem=ctx_recv_sem.at[chunk, frm],
            device_id={"sp": to},
            device_id_type=pl.DeviceIdType.MESH,
        )

    def put_relay(chunk, to, slot):
        bs = pl.ds(chunk * nb, nb)
        return pltpu.make_async_remote_copy(
            src_ref=ctx_send.at[bs, to],
            dst_ref=relay.at[bs, slot],
            send_sem=ctx_send_sem.at[chunk, to],
            recv_sem=relay_recv_sem.at[chunk, slot],
            device_id={"sp": to - FIRST},
            device_id_type=pl.DeviceIdType.MESH,
        )

    def forward(chunk, slot):
        bs = pl.ds(chunk * nb, nb)
        return pltpu.make_async_remote_copy(
            src_ref=relay.at[bs, slot],
            dst_ref=ctx_recv.at[bs, 2 * FIRST + slot],
            send_sem=relay_send_sem.at[chunk, slot],
            recv_sem=ctx_recv_sem.at[chunk, 2 * FIRST + slot],
            device_id={"sp": me + FIRST},
            device_id_type=pl.DeviceIdType.MESH,
        )

    def put_near(chunk, kind):
        bs = pl.ds(chunk * nb, nb)
        return pltpu.make_async_remote_copy(
            src_ref=send.at[kind, bs, pl.ds((1 - me) * dests, dests)],
            dst_ref=near.at[kind, bs],
            send_sem=near_send_sem.at[chunk, kind],
            recv_sem=near_recv_sem.at[chunk, kind],
            device_id={"sp": 1 - me},
            device_id_type=pl.DeviceIdType.MESH,
        )

    def put_ctx_near(chunk):
        bs = pl.ds(chunk * nb, nb)
        return pltpu.make_async_remote_copy(
            src_ref=ctx_near.at[bs, 1 - me],
            dst_ref=ctx_recv.at[bs, pl.ds(me * dests, dests)],
            send_sem=ctx_near_send_sem.at[chunk],
            recv_sem=ctx_near_recv_sem.at[chunk],
            device_id={"sp": 1 - me},
            device_id_type=pl.DeviceIdType.MESH,
        )

    is_first = me < FIRST

    def each_peer(do, lowest=0):
        for other in range(lowest, n):
            pl.when(other != me)(functools.partial(do, other))

    def qkv_phase(x_buf, h_attn, w_nat, w_cols, out_buf, own, cos_ref, sin_ref):
        mine = pl.ds(pl.multiple_of(me * seq_dev, seq_dev), seq_dev)
        get_cos = pltpu.make_async_copy(cos_hbm.at[mine], cos_ref, own_sem.at[3])
        get_sin = pltpu.make_async_copy(sin_hbm.at[mine], sin_ref, own_sem.at[4])

        def get_x(chunk):
            return pltpu.make_async_copy(x_hbm.at[pl.ds(chunk * rows, rows)], x_buf, x_sem)

        def get_w(block):
            slot = lax.rem(block, 2)
            src = w_qkv.at[:, block // parts, pl.ds(lax.rem(block, parts) * QKV_HEADS, QKV_HEADS)]
            return pltpu.make_async_copy(src, w_nat.at[slot], w_sem.at[slot])

        def bounce(step):
            slot, block = lax.rem(step, 2), lax.rem(step, blocks)
            dst = send.at[
                block // parts, pl.ds(step // blocks * nb, nb), pl.ds(lax.rem(block, parts) * dests, dests)
            ]
            return pltpu.make_async_copy(out_buf.at[slot], dst, bounce_sem.at[slot])

        def put_own(chunk, kind):
            dst = recv.at[kind, pl.ds(chunk * nb, nb), :, me]
            return pltpu.make_async_copy(own.at[kind], dst, own_sem.at[kind])

        def send_block(step):
            bounce(step).wait()
            block = lax.rem(step, blocks)
            for d in range(dests):
                to = lax.rem(block, parts) * dests + lax.rem(me + d, dests)

                @pl.when((to != me) & jnp.logical_not(is_first & (block < parts)))
                def _():
                    put(step // blocks, block // parts, to, me).start()

            @pl.when(is_first & (lax.rem(block, parts) == 1 - me))
            def _():
                put_near(step // blocks, block // parts).start()

        get_x(0).start()
        get_w(0).start()
        get_cos.start()
        get_sin.start()
        barrier = pltpu.get_barrier_semaphore()
        for step in range(1, n):
            pl.semaphore_signal(
                barrier, inc=1, device_id={"sp": peer(step)}, device_id_type=pl.DeviceIdType.MESH
            )

        @pl.loop(0, N_CHUNKS * blocks)
        def _(step):
            chunk, block = step // blocks, lax.rem(step, blocks)
            kind, part = block // parts, lax.rem(block, parts)
            slot = lax.rem(step, 2)

            with jax.named_scope("ln"):
                @pl.when(block == 0)
                def _():
                    get_x(chunk).wait()

                    @pl.loop(0, nb)
                    def _(i):
                        r = pl.ds(pl.multiple_of(i * seq_dev, seq_dev), seq_dev)
                        g = pl.ds(pl.multiple_of(chunk * rows + i * seq_dev, seq_dev), seq_dev)
                        xf = x_buf[r, :].astype(F32)
                        mean = jnp.sum(xf, axis=-1, keepdims=True) * (1.0 / width)
                        dev = xf - mean
                        var = jnp.sum(dev * dev, axis=-1, keepdims=True) * (1.0 / width)
                        unit = dev * lax.rsqrt(var + LN_EPS)
                        h_attn[r, :] = (unit * ln_aw[...] + ln_ab[...]).astype(BF16)
                        h_mlp[g, :] = (unit * ln_mw[...] + ln_mb[...]).astype(BF16)
                        acc[g, :] = xf

                    @pl.when(chunk + 1 < N_CHUNKS)
                    def _():
                        get_x(chunk + 1).start()

            with jax.named_scope("relayout"):
                @pl.when(chunk == 0)
                def _():
                    get_w(block).wait()

                    @pl.when(block + 1 < blocks)
                    def _():
                        get_w(block + 1).start()

                    @pl.when(block == 0)
                    def _():
                        get_cos.wait()
                        get_sin.wait()

                    @pl.loop(0, width // 128)
                    def _(i):
                        r = pl.ds(pl.multiple_of(i * 128, 128), 128)
                        by_head = jnp.swapaxes(w_nat[slot, r].astype(F32), 0, 1)
                        for h in range(QKV_HEADS):
                            w_cols[block, r, h * head_dim : (h + 1) * head_dim] = by_head[h].astype(BF16)

            with jax.named_scope("qkv_dot"):
                for d in range(dests):
                    cs = slice(d * heads * head_dim, (d + 1) * heads * head_dim)
                    cols = jnp.dot(h_attn[...], w_cols[block, :, cs], preferred_element_type=F32)
                    for h in range(heads):
                        for b in range(nb):
                            u = cols[b * seq_dev : (b + 1) * seq_dev, h * head_dim : (h + 1) * head_dim]
                            u = u.astype(BF16).astype(F32)
                            turned = u * cos_ref[...] + pltpu.roll(u, head_dim // 2, 1) * sin_ref[...]
                            out_buf[slot, b, d, h] = jnp.where(kind < 2, turned, u).astype(BF16)

            with jax.named_scope("qkv_send"):
                bounce(step).start()

                @pl.when(me // dests == part)
                def _():
                    @pl.when(chunk > 0)
                    def _():
                        put_own(chunk - 1, kind).wait()

                    own[kind] = out_buf[slot, :, lax.rem(me, dests)]
                    put_own(chunk, kind).start()

                @pl.when(step == 0)
                def _():
                    pl.semaphore_wait(barrier, n - 1)

                @pl.when(chunk == 0)
                def _():
                    send_block(step)

                @pl.when(step > blocks)
                def _():
                    send_block(step - 1)

        send_block(N_CHUNKS * blocks - 1)
        for kind in range(3):
            put_own(N_CHUNKS - 1, kind).wait()

    pl.run_scoped(
        qkv_phase,
        pltpu.VMEM((rows, width), BF16),
        pltpu.VMEM((rows, width), BF16),
        pltpu.VMEM((2, width, QKV_HEADS, head_dim), BF16),
        pltpu.VMEM((blocks, width, QKV_HEADS * head_dim), BF16),
        pltpu.VMEM((2, nb, dests, heads, seq_dev, head_dim), BF16),
        pltpu.VMEM((3, nb, heads, seq_dev, head_dim), BF16),
        pltpu.VMEM((seq_dev, head_dim), F32),
        pltpu.VMEM((seq_dev, head_dim), F32),
    )

    def rest(up_buf, down_buf, w_buf, qkv_buf, ctx_buf, both, near_buf, ctx_in, ctx_rows, y_buf):
        later = n - FIRST
        steps = ffn // UP_TILE

        def get_up(f):
            cols = pl.ds(pl.multiple_of(f * UP_TILE, UP_TILE), UP_TILE)
            slot = lax.rem(f, 2)
            return pltpu.make_async_copy(w_up.at[:, cols], up_buf.at[slot], up_sem.at[slot])

        def get_down(f):
            cols = pl.ds(pl.multiple_of(f * UP_TILE, UP_TILE), UP_TILE)
            slot = lax.rem(f, 2)
            return pltpu.make_async_copy(w_down.at[cols], down_buf.at[slot], down_sem.at[slot])

        def get_w_out():
            return pltpu.make_async_copy(w_out, w_buf, w_sem.at[0])

        def get_qkv(chunk, kind):
            return pltpu.make_async_copy(recv.at[kind, pl.ds(chunk * nb, nb)], qkv_buf.at[kind], qkv_sem.at[kind])

        def get_own_near(chunk, kind):
            src = send.at[kind, pl.ds(chunk * nb, nb), pl.ds(me * dests, dests)]
            return pltpu.make_async_copy(src, both.at[kind, :, :, :, me], near_sem.at[kind, 0])

        def get_other_near(chunk, kind):
            src = near.at[kind, pl.ds(chunk * nb, nb)]
            return pltpu.make_async_copy(src, both.at[kind, :, :, :, 1 - me], near_sem.at[kind, 1])

        def bounce_ctx(chunk):
            dst = ctx_send.at[pl.ds(chunk * nb, nb), pl.ds(FIRST, later)]
            return pltpu.make_async_copy(ctx_buf, dst, bounce_sem.at[0])

        def bounce_near(chunk):
            return pltpu.make_async_copy(near_buf, ctx_near.at[pl.ds(chunk * nb, nb)], bounce_sem.at[1])

        def put_own_ctx(chunk):
            dst = ctx_recv.at[pl.ds(chunk * nb, nb), me]
            return pltpu.make_async_copy(ctx_buf.at[:, me - FIRST], dst, own_sem.at[3])

        def put_own_near(chunk):
            dst = ctx_recv.at[pl.ds(chunk * nb, nb), pl.ds(me * dests, dests)]
            return pltpu.make_async_copy(near_buf.at[:, me], dst, own_sem.at[4])

        def put_y(chunk):
            return pltpu.make_async_copy(y_buf, y_hbm.at[pl.ds(chunk * rows, rows)], out_sem)

        def send_ctx(chunk):
            bounce_ctx(chunk).wait()
            relays = (me // FIRST == 2) & (chunk < RELAYED)

            def one(other):
                if other // FIRST == 1:

                    @pl.when(relays)
                    def _():
                        put_relay(chunk, other, me - 2 * FIRST).start()

                    @pl.when(jnp.logical_not(relays))
                    def _():
                        put_ctx(chunk, other, me).start()

                else:
                    put_ctx(chunk, other, me).start()

            each_peer(one, FIRST)

            @pl.when(jnp.logical_not(is_first))
            def _():
                put_own_ctx(chunk).wait()

        def send_near(chunk):
            bounce_near(chunk).wait()
            put_ctx_near(chunk).start()
            put_own_near(chunk).wait()

        def pass_on(chunk):
            for slot in range(FIRST):
                put_relay(chunk, me + FIRST, slot).wait_recv()
                forward(chunk, slot).start()

        def load_qkv(chunk):
            with jax.named_scope("wait_qkv"):
                each_peer(lambda other: put(chunk, 0, me, other).wait_recv(), FIRST)
                each_peer(lambda other: put(chunk, 1, me, other).wait_recv())
                each_peer(lambda other: put(chunk, 2, me, other).wait_recv())
            for kind in range(3):
                get_qkv(chunk, kind).start()

            @pl.when(is_first)
            def _():
                for kind in range(3):
                    put_near(chunk, kind).wait_recv()
                    get_own_near(chunk, kind).start()
                    get_other_near(chunk, kind).start()

        get_up(0).start()
        get_down(0).start()
        get_w_out().start()

        @pl.loop(0, N_CHUNKS + 1)
        def _(chunk):
            early = steps - LATE_STEPS
            first = chunk * early // N_CHUNKS
            last = jnp.where(chunk < N_CHUNKS, (chunk + 1) * early // N_CHUNKS, steps)

            @pl.loop(first, last)
            def _(f):
                slot = lax.rem(f, 2)

                @pl.when(f + 1 < steps)
                def _():
                    get_up(f + 1).start()
                    get_down(f + 1).start()

                @pl.when((f == last - 1) & (chunk < N_CHUNKS - 1))
                def _():
                    load_qkv(chunk)

                with jax.named_scope("wait_w"):
                    get_up(f).wait()
                    get_down(f).wait()
                with jax.named_scope("mlp"):
                    for r in range(n_batch * seq_dev // 512):
                        rs = pl.ds(r * 512, 512)
                        up = jnp.dot(h_mlp[rs, :], up_buf[slot], preferred_element_type=F32)
                        hid = (0.5 * up * (1.0 + lax.erf(up * 0.5**0.5))).astype(BF16)
                        acc[rs, :] += jnp.dot(hid, down_buf[slot], preferred_element_type=F32)

                with jax.named_scope("send_ctx"):
                    @pl.when((f == first) & (chunk > 0))
                    def _():
                        @pl.when(chunk < N_CHUNKS)
                        def _():
                            send_ctx(chunk - 1)

                        @pl.when(is_first)
                        def _():
                            send_near(chunk - 1)

                with jax.named_scope("pass_on"):
                    @pl.when(is_first & (chunk == N_CHUNKS))
                    def _():
                        first_relay = 1 + (f - first) * 2

                        @pl.loop(first_relay, jnp.minimum(jnp.where(f == steps - 1, RELAYED, first_relay + 2), RELAYED))
                        def _(c):
                            pass_on(c)

            @pl.when(chunk < N_CHUNKS)
            def _():
                @pl.when(chunk == N_CHUNKS - 1)
                def _():
                    load_qkv(chunk)

                with jax.named_scope("attn"):
                    for kind in range(3):
                        get_qkv(chunk, kind).wait()
                    for b in range(nb):
                        for h in range(heads):
                            q = qkv_buf[0, b, h, FIRST:].reshape(later * seq_dev, head_dim)
                            k, v = (qkv_buf[t, b, h].reshape(n * seq_dev, head_dim) for t in (1, 2))
                            per = Q_TILE // seq_dev

                            def write(i, out):
                                ctx_buf[b, i * per : (i + 1) * per, h] = out.reshape(per, seq_dev, head_dim)

                            causal_head(q, k, v, write)
                bounce_ctx(chunk).start()

                @pl.when(jnp.logical_not(is_first))
                def _():
                    put_own_ctx(chunk).start()

                with jax.named_scope("send_last"):
                    @pl.when(chunk == N_CHUNKS - 1)
                    def _():
                        send_ctx(chunk)

                        @pl.when(is_first)
                        def _():
                            pass_on(0)

                with jax.named_scope("near"):
                    @pl.when(is_first)
                    def _():
                        for kind in range(3):
                            get_own_near(chunk, kind).wait()
                            get_other_near(chunk, kind).wait()

                        @pl.loop(0, nb)
                        def _(b):
                            for d in range(dests):
                                for h in range(heads):
                                    q, k, v = (both[t, b, d, h].reshape(Q_TILE, head_dim) for t in range(3))

                                    def write(i, out):
                                        near_buf[b, :, d, h] = out.reshape(FIRST, seq_dev, head_dim)

                                    causal_head(q, k, v, write)

                        bounce_near(chunk).start()
                        put_own_near(chunk).start()

        get_w_out().wait()

        @pl.loop(0, N_CHUNKS)
        def _(chunk):
            def get_ctx(c):
                src = ctx_recv.at[pl.ds(c * nb, nb)]
                return pltpu.make_async_copy(src, ctx_in.at[lax.rem(c, 2)], qkv_sem.at[lax.rem(c, 2)])

            with jax.named_scope("wait_ctx"):
                @pl.when(is_first)
                def _():
                    def load(c):
                        put_ctx_near(c).wait_recv()
                        get_ctx(c).start()

                    pl.when(chunk == 0)(lambda: load(chunk))
                    pl.when(chunk + 1 < N_CHUNKS)(lambda: load(chunk + 1))

                @pl.when(jnp.logical_not(is_first))
                def _():
                    each_peer(lambda other: put_ctx(chunk, me, other).wait_recv())
                    get_ctx(chunk).start()

            with jax.named_scope("out_proj"):
                get_ctx(chunk).wait()
                for b in range(nb):
                    for s in range(n):
                        for h in range(heads):
                            col = (s * heads + h) * head_dim
                            ctx_rows[b * seq_dev : (b + 1) * seq_dev, col : col + head_dim] = ctx_in[lax.rem(chunk, 2), b, s, h]

                @pl.when(chunk > 0)
                def _():
                    put_y(chunk - 1).wait()

                g = pl.ds(pl.multiple_of(chunk * rows, rows), rows)
                for c in range(0, width, 1024):
                    cs = slice(c, c + 1024)
                    attn = jnp.dot(ctx_rows[...], w_buf[:, cs], preferred_element_type=F32)
                    y_buf[:, cs] = (acc[g, cs] + attn).astype(BF16)
                put_y(chunk).start()

        put_y(N_CHUNKS - 1).wait()

    pl.run_scoped(
        rest,
        pltpu.VMEM((2, width, UP_TILE), BF16),
        pltpu.VMEM((2, UP_TILE, width), BF16),
        pltpu.VMEM((width, width), BF16),
        pltpu.VMEM((3, nb, heads, n, seq_dev, head_dim), BF16),
        pltpu.VMEM((nb, n - FIRST, heads, seq_dev, head_dim), BF16),
        pltpu.VMEM((3, nb, dests, heads, FIRST, seq_dev, head_dim), BF16),
        pltpu.VMEM((nb, FIRST, dests, heads, seq_dev, head_dim), BF16),
        pltpu.VMEM((2, nb, n, heads, seq_dev, head_dim), BF16),
        pltpu.VMEM((rows, width), BF16),
        pltpu.VMEM((rows, width), BF16),
    )

    @pl.loop(0, N_CHUNKS)
    def _(chunk):
        def sent(other):
            put(chunk, 1, other, me).wait_send()
            put(chunk, 2, other, me).wait_send()

        each_peer(sent)
        each_peer(lambda other: put_ctx(chunk, other, me).wait_send(), FIRST)

        @pl.when(is_first)
        def _():
            for kind in range(3):
                put_near(chunk, kind).wait_send()
            put_ctx_near(chunk).wait_send()

            @pl.when(chunk < RELAYED)
            def _():
                for slot in range(FIRST):
                    forward(chunk, slot).wait_send()

        @pl.when(jnp.logical_not(is_first))
        def _():
            each_peer(lambda other: put(chunk, 0, other, me).wait_send())


def solution(mesh):
    n = mesh.shape["sp"]

    def local_layer(x_blk, ln_attn_w, ln_attn_b, ln_mlp_w, ln_mlp_b, w_qkv, w_out, w_up, w_down):
        n_batch, seq_dev, width = x_blk.shape
        groups, head_dim = w_qkv.shape[1], w_qkv.shape[3]
        heads = groups // n
        nb = n_batch // N_CHUNKS
        rows = n_batch * seq_dev
        dests = QKV_HEADS // heads
        ffn = w_up.shape[1]
        cos_t, sin_t = rope_tables(n * seq_dev, head_dim)
        row = lambda p: p.reshape(1, width)
        anywhere = pl.BlockSpec(memory_space=pl.ANY)
        vmem = pl.BlockSpec(memory_space=pltpu.VMEM)
        flops = 2 * rows * width * (3 * width + 2 * ffn) + 2 * rows * n * seq_dev * width * 2
        y_out, recv, *_ = pl.pallas_call(
            functools.partial(layer_kernel, n),
            out_shape=[
                jax.ShapeDtypeStruct((rows, width), BF16),
                jax.ShapeDtypeStruct((3, n_batch, heads, n, seq_dev, head_dim), BF16),
                jax.ShapeDtypeStruct((n_batch, n, heads, seq_dev, head_dim), BF16),
                jax.ShapeDtypeStruct((3, n_batch, n, heads, seq_dev, head_dim), BF16),
                jax.ShapeDtypeStruct((n_batch, n, heads, seq_dev, head_dim), BF16),
                jax.ShapeDtypeStruct((3, n_batch, dests, heads, seq_dev, head_dim), BF16),
                jax.ShapeDtypeStruct((n_batch, FIRST, dests, heads, seq_dev, head_dim), BF16),
                jax.ShapeDtypeStruct((n_batch, FIRST, heads, seq_dev, head_dim), BF16),
            ],
            in_specs=[anywhere] * 3 + [vmem] * 4 + [anywhere] * 4,
            out_specs=[anywhere] * 8,
            scratch_shapes=[
                pltpu.VMEM((rows, width), BF16),
                pltpu.VMEM((rows, width), F32),
                pltpu.SemaphoreType.DMA,
                pltpu.SemaphoreType.DMA((2,)),
                pltpu.SemaphoreType.DMA((2,)),
                pltpu.SemaphoreType.DMA((5,)),
                pltpu.SemaphoreType.DMA,
                pltpu.SemaphoreType.DMA((2,)),
                pltpu.SemaphoreType.DMA((2,)),
                pltpu.SemaphoreType.DMA((3,)),
                pltpu.SemaphoreType.DMA((3, 2)),
                pltpu.SemaphoreType.DMA((N_CHUNKS, 3, n)),
                pltpu.SemaphoreType.DMA((N_CHUNKS, 3, n)),
                pltpu.SemaphoreType.DMA((N_CHUNKS, n)),
                pltpu.SemaphoreType.DMA((N_CHUNKS, n)),
                pltpu.SemaphoreType.DMA((N_CHUNKS, 3)),
                pltpu.SemaphoreType.DMA((N_CHUNKS, 3)),
                pltpu.SemaphoreType.DMA((N_CHUNKS,)),
                pltpu.SemaphoreType.DMA((N_CHUNKS,)),
                pltpu.SemaphoreType.DMA((N_CHUNKS, FIRST)),
                pltpu.SemaphoreType.DMA((N_CHUNKS, FIRST)),
            ],
            compiler_params=pltpu.CompilerParams(
                collective_id=0, has_side_effects=True, vmem_limit_bytes=63 * 2**20
            ),
            cost_estimate=pl.CostEstimate(flops=flops, bytes_accessed=3 * 10**8, transcendentals=10**7),
            name="layer",
        )(
            x_blk.reshape(rows, width),
            cos_t,
            sin_t,
            row(ln_attn_w),
            row(ln_attn_b),
            row(ln_mlp_w),
            row(ln_mlp_b),
            w_qkv.transpose(0, 2, 1, 3),
            w_out,
            w_up,
            w_down,
        )
        shape = (n_batch, heads, n * seq_dev, head_dim)
        return y_out.reshape(x_blk.shape), recv[1].reshape(shape), recv[2].reshape(shape)

    act_spec, cache_spec = P("dp", "sp", None), P("dp", "sp", None, None)
    return jax.shard_map(
        local_layer,
        mesh=mesh,
        in_specs=(act_spec,) + (P(),) * 8,
        out_specs=(act_spec, cache_spec, cache_spec),
        check_vma=False,
    )
```

```python
import functools

import jax
import jax.numpy as jnp
import numpy as np
from jax import lax
from jax.experimental import pallas as pl
from jax.experimental.pallas import tpu as pltpu
from jax.sharding import PartitionSpec as P

LN_EPS = 1e-5
ROPE_BASE = 10000.0
LOG2E = 1.4426950408889634
N_CHUNKS = 6
UP_TILE = 512
QKV_HEADS = 8
Q_TILE = 256
FIRST = 2
LATE_STEPS = 2
RELAYED = 4
F32 = jnp.float32
BF16 = jnp.bfloat16


def rope_tables(positions, head_dim):
    half_dim = head_dim // 2
    inv_freq = np.float32(ROPE_BASE) ** (np.float32(-2.0) * np.arange(half_dim, dtype=np.float32) / np.float32(head_dim))
    angles = np.arange(positions, dtype=np.float32)[:, None] * inv_freq[None, :]
    cos_t, sin_t = np.cos(angles.astype(np.float64)), np.sin(angles.astype(np.float64))
    wide = lambda a, b: jnp.asarray(np.concatenate([a, b], -1).astype(np.float32))
    return wide(cos_t, cos_t), wide(-sin_t, sin_t)


def causal_head(q, k, v, write):
    seq, head_dim = k.shape
    scale = LOG2E * head_dim**-0.5
    keys = lax.broadcasted_iota(jnp.int32, (Q_TILE, Q_TILE), 0)
    queries = lax.broadcasted_iota(jnp.int32, (Q_TILE, Q_TILE), 1)
    for i in range(q.shape[0] // Q_TILE):
        lo = seq - q.shape[0] + i * Q_TILE
        hi = lo + Q_TILE
        q_i = q[i * Q_TILE : (i + 1) * Q_TILE]
        scores = lax.dot_general(k[:hi], q_i, (((1,), (1,)), ((), ())), preferred_element_type=F32)
        diag = jnp.where(keys <= queries, scores[lo:], -1e30)
        scores = jnp.concatenate([scores[:lo], diag], axis=0) if lo else diag
        prob = jnp.exp2((scores - jnp.max(scores, axis=0, keepdims=True)) * scale)
        prob = (prob * (1.0 / jnp.sum(prob, axis=0, keepdims=True))).astype(BF16)
        out = lax.dot_general(prob, v[:hi], (((0,), (0,)), ((), ())), preferred_element_type=F32)
        write(i, out.astype(BF16))


def layer_kernel(
    n,
    x_hbm,
    cos_hbm,
    sin_hbm,
    ln_aw_hbm,
    ln_ab_hbm,
    ln_mw_hbm,
    ln_mb_hbm,
    w_qkv,
    w_out,
    w_up,
    w_down,
    y_hbm,
    recv,
    send,
    ctx_send,
    near,
    ctx_near,
    relay,
    h_mlp,
    acc,
    ctx_rows,
    ln_buf,
    x_sem,
    ln_sem,
    w_sem,
    bounce_sem,
    own_sem,
    out_sem,
    up_sem,
    down_sem,
    qkv_sem,
    near_sem,
    send_sem,
    recv_sem,
    ctx_send_sem,
    ctx_recv_sem,
    near_send_sem,
    near_recv_sem,
    ctx_near_send_sem,
    ctx_near_recv_sem,
    relay_recv_sem,
    relay_send_sem,
):
    me = lax.axis_index("sp")
    n_batch, _, heads, seq_dev, head_dim = send.shape[1:]
    cols = heads * head_dim
    width = x_hbm.shape[1]
    nb = n_batch // N_CHUNKS
    rows = nb * seq_dev
    ffn = w_up.shape[1]
    dests = QKV_HEADS // heads
    parts = n // dests
    blocks = 3 * parts

    def peer(step):
        return lax.bitwise_xor(me, step)

    def rows_of(chunk, first, count=1):
        return ctx_rows.at[pl.ds(chunk * nb, nb), :, pl.ds(pl.multiple_of(first * cols, cols), count * cols)]

    def put(chunk, kind, to, frm):
        bs = pl.ds(chunk * nb, nb)
        return pltpu.make_async_remote_copy(
            src_ref=send.at[kind, bs, to],
            dst_ref=recv.at[kind, bs, :, frm],
            send_sem=send_sem.at[chunk, kind, to],
            recv_sem=recv_sem.at[chunk, kind, frm],
            device_id={"sp": to},
            device_id_type=pl.DeviceIdType.MESH,
        )

    def put_ctx(chunk, to, frm):
        bs = pl.ds(chunk * nb, nb)
        return pltpu.make_async_remote_copy(
            src_ref=ctx_send.at[bs, to],
            dst_ref=rows_of(chunk, frm),
            send_sem=ctx_send_sem.at[chunk, to],
            recv_sem=ctx_recv_sem.at[chunk, frm],
            device_id={"sp": to},
            device_id_type=pl.DeviceIdType.MESH,
        )

    def put_relay(chunk, to, slot):
        bs = pl.ds(chunk * nb, nb)
        return pltpu.make_async_remote_copy(
            src_ref=ctx_send.at[bs, to],
            dst_ref=relay.at[bs, slot],
            send_sem=ctx_send_sem.at[chunk, to],
            recv_sem=relay_recv_sem.at[chunk, slot],
            device_id={"sp": to - FIRST},
            device_id_type=pl.DeviceIdType.MESH,
        )

    def forward(chunk, slot):
        bs = pl.ds(chunk * nb, nb)
        return pltpu.make_async_remote_copy(
            src_ref=relay.at[bs, slot],
            dst_ref=rows_of(chunk, 2 * FIRST + slot),
            send_sem=relay_send_sem.at[chunk, slot],
            recv_sem=ctx_recv_sem.at[chunk, 2 * FIRST + slot],
            device_id={"sp": me + FIRST},
            device_id_type=pl.DeviceIdType.MESH,
        )

    def put_near(chunk, kind):
        bs = pl.ds(chunk * nb, nb)
        return pltpu.make_async_remote_copy(
            src_ref=send.at[kind, bs, pl.ds((1 - me) * dests, dests)],
            dst_ref=near.at[kind, bs],
            send_sem=near_send_sem.at[chunk, kind],
            recv_sem=near_recv_sem.at[chunk, kind],
            device_id={"sp": 1 - me},
            device_id_type=pl.DeviceIdType.MESH,
        )

    def put_ctx_near(chunk):
        bs = pl.ds(chunk * nb, nb)
        return pltpu.make_async_remote_copy(
            src_ref=ctx_near.at[bs, 1 - me],
            dst_ref=rows_of(chunk, me * dests, dests),
            send_sem=ctx_near_send_sem.at[chunk],
            recv_sem=ctx_near_recv_sem.at[chunk],
            device_id={"sp": 1 - me},
            device_id_type=pl.DeviceIdType.MESH,
        )

    is_first = me < FIRST

    def each_peer(do, lowest=0):
        for other in range(lowest, n):
            pl.when(other != me)(functools.partial(do, other))

    def qkv_phase(x_buf, h_attn, w_nat, w_cols, out_buf, own, cos_ref, sin_ref):
        mine = pl.ds(pl.multiple_of(me * seq_dev, seq_dev), seq_dev)
        get_cos = pltpu.make_async_copy(cos_hbm.at[mine], cos_ref, own_sem.at[3])
        get_sin = pltpu.make_async_copy(sin_hbm.at[mine], sin_ref, own_sem.at[4])

        def get_x(chunk):
            return pltpu.make_async_copy(x_hbm.at[pl.ds(chunk * rows, rows)], x_buf, x_sem)

        def get_w(half):
            block, slot = half // 2, lax.rem(half, 2)
            src = w_qkv.at[
                pl.ds(slot * (width // 2), width // 2),
                block // parts,
                pl.ds(lax.rem(block, parts) * QKV_HEADS, QKV_HEADS),
            ]
            return pltpu.make_async_copy(src, w_nat.at[slot], w_sem.at[slot])

        def bounce(step):
            slot, block = lax.rem(step, 2), lax.rem(step, blocks)
            dst = send.at[
                block // parts, pl.ds(step // blocks * nb, nb), pl.ds(lax.rem(block, parts) * dests, dests)
            ]
            return pltpu.make_async_copy(out_buf.at[slot], dst, bounce_sem.at[slot])

        def put_own(chunk, kind):
            dst = recv.at[kind, pl.ds(chunk * nb, nb), :, me]
            return pltpu.make_async_copy(own.at[kind], dst, own_sem.at[kind])

        def send_block(step):
            bounce(step).wait()
            block = lax.rem(step, blocks)
            for d in range(dests):
                to = lax.rem(block, parts) * dests + lax.rem(me + d, dests)

                @pl.when((to != me) & jnp.logical_not(is_first & (block < parts)))
                def _():
                    put(step // blocks, block // parts, to, me).start()

            @pl.when(is_first & (lax.rem(block, parts) == 1 - me))
            def _():
                put_near(step // blocks, block // parts).start()

        ln_hbm = (ln_aw_hbm, ln_ab_hbm, ln_mw_hbm, ln_mb_hbm)
        get_ln = [pltpu.make_async_copy(p, ln_buf.at[i], ln_sem.at[i]) for i, p in enumerate(ln_hbm)]
        ln_aw, ln_ab, ln_mw, ln_mb = (ln_buf.at[i] for i in range(4))
        get_x(0).start()
        for copy in get_ln:
            copy.start()
        get_w(0).start()
        get_w(1).start()
        get_cos.start()
        get_sin.start()
        barrier = pltpu.get_barrier_semaphore()
        for step in range(1, n):
            pl.semaphore_signal(
                barrier, inc=1, device_id={"sp": peer(step)}, device_id_type=pl.DeviceIdType.MESH
            )

        @pl.loop(0, N_CHUNKS * blocks)
        def _(step):
            chunk, block = step // blocks, lax.rem(step, blocks)
            kind, part = block // parts, lax.rem(block, parts)
            slot = lax.rem(step, 2)

            with jax.named_scope("ln"):
                @pl.when(block == 0)
                def _():
                    get_x(chunk).wait()

                    @pl.when(chunk == 0)
                    def _():
                        for copy in get_ln:
                            copy.wait()

                    @pl.loop(0, nb)
                    def _(i):
                        r = pl.ds(pl.multiple_of(i * seq_dev, seq_dev), seq_dev)
                        g = pl.ds(pl.multiple_of(chunk * rows + i * seq_dev, seq_dev), seq_dev)
                        xf = x_buf[r, :].astype(F32)
                        mean = jnp.sum(xf, axis=-1, keepdims=True) * (1.0 / width)
                        dev = xf - mean
                        var = jnp.sum(dev * dev, axis=-1, keepdims=True) * (1.0 / width)
                        unit = dev * lax.rsqrt(var + LN_EPS)
                        h_attn[r, :] = (unit * ln_aw[...] + ln_ab[...]).astype(BF16)
                        h_mlp[g, :] = (unit * ln_mw[...] + ln_mb[...]).astype(BF16)
                        acc[g, :] = xf

                    @pl.when(chunk + 1 < N_CHUNKS)
                    def _():
                        get_x(chunk + 1).start()

            with jax.named_scope("relayout"):
                @pl.when(chunk == 0)
                def _():
                    @pl.when(block == 0)
                    def _():
                        get_cos.wait()
                        get_sin.wait()

                    @pl.loop(2 * block, 2 * block + 2)
                    def _(half):
                        get_w(half).wait()

                        @pl.loop(0, width // 2 // 128)
                        def _(i):
                            r = pl.ds(pl.multiple_of(i * 128, 128), 128)
                            top = lax.rem(half, 2) * (width // 2)
                            to = pl.ds(pl.multiple_of(top + i * 128, 128), 128)
                            by_head = jnp.swapaxes(w_nat[lax.rem(half, 2), r].astype(F32), 0, 1)
                            for h in range(QKV_HEADS):
                                w_cols[block, to, h * head_dim : (h + 1) * head_dim] = by_head[h].astype(BF16)

                        @pl.when(half + 2 < 2 * blocks)
                        def _():
                            get_w(half + 2).start()

            with jax.named_scope("qkv_dot"):
                for d in range(dests):
                    cs = slice(d * heads * head_dim, (d + 1) * heads * head_dim)
                    cols = jnp.dot(h_attn[...], w_cols[block, :, cs], preferred_element_type=F32)
                    for h in range(heads):
                        for b in range(nb):
                            u = cols[b * seq_dev : (b + 1) * seq_dev, h * head_dim : (h + 1) * head_dim]
                            u = u.astype(BF16).astype(F32)
                            turned = u * cos_ref[...] + pltpu.roll(u, head_dim // 2, 1) * sin_ref[...]
                            out_buf[slot, b, d, h] = jnp.where(kind < 2, turned, u).astype(BF16)

            with jax.named_scope("qkv_send"):
                bounce(step).start()

                @pl.when(me // dests == part)
                def _():
                    @pl.when(chunk > 0)
                    def _():
                        put_own(chunk - 1, kind).wait()

                    own[kind] = out_buf[slot, :, lax.rem(me, dests)]
                    put_own(chunk, kind).start()

                @pl.when(step == 0)
                def _():
                    pl.semaphore_wait(barrier, n - 1)

                @pl.when(chunk == 0)
                def _():
                    send_block(step)

                @pl.when(step > blocks)
                def _():
                    send_block(step - 1)

        send_block(N_CHUNKS * blocks - 1)
        for kind in range(3):
            put_own(N_CHUNKS - 1, kind).wait()

    pl.run_scoped(
        qkv_phase,
        pltpu.VMEM((rows, width), BF16),
        pltpu.VMEM((rows, width), BF16),
        pltpu.VMEM((2, width // 2, QKV_HEADS, head_dim), BF16),
        pltpu.VMEM((blocks, width, QKV_HEADS * head_dim), BF16),
        pltpu.VMEM((2, nb, dests, heads, seq_dev, head_dim), BF16),
        pltpu.VMEM((3, nb, heads, seq_dev, head_dim), BF16),
        pltpu.VMEM((seq_dev, head_dim), F32),
        pltpu.VMEM((seq_dev, head_dim), F32),
    )

    def rest(up_buf, down_buf, w_buf, qkv_buf, ctx_buf, both, near_buf, y_buf):
        later = n - FIRST
        steps = ffn // UP_TILE

        def get_up(f):
            cols = pl.ds(pl.multiple_of(f * UP_TILE, UP_TILE), UP_TILE)
            slot = lax.rem(f, 2)
            return pltpu.make_async_copy(w_up.at[:, cols], up_buf.at[slot], up_sem.at[slot])

        def get_down(f):
            cols = pl.ds(pl.multiple_of(f * UP_TILE, UP_TILE), UP_TILE)
            slot = lax.rem(f, 2)
            return pltpu.make_async_copy(w_down.at[cols], down_buf.at[slot], down_sem.at[slot])

        def get_w_out():
            return pltpu.make_async_copy(w_out, w_buf, w_sem.at[0])

        def get_qkv(chunk, kind):
            return pltpu.make_async_copy(recv.at[kind, pl.ds(chunk * nb, nb)], qkv_buf.at[kind], qkv_sem.at[kind])

        def get_own_near(chunk, kind):
            src = send.at[kind, pl.ds(chunk * nb, nb), pl.ds(me * dests, dests)]
            return pltpu.make_async_copy(src, both.at[kind, :, :, :, me], near_sem.at[kind, 0])

        def get_other_near(chunk, kind):
            src = near.at[kind, pl.ds(chunk * nb, nb)]
            return pltpu.make_async_copy(src, both.at[kind, :, :, :, 1 - me], near_sem.at[kind, 1])

        def bounce_ctx(chunk):
            dst = ctx_send.at[pl.ds(chunk * nb, nb), pl.ds(FIRST, later)]
            return pltpu.make_async_copy(ctx_buf, dst, bounce_sem.at[0])

        def bounce_near(chunk):
            return pltpu.make_async_copy(near_buf, ctx_near.at[pl.ds(chunk * nb, nb)], bounce_sem.at[1])

        def put_y(chunk):
            return pltpu.make_async_copy(y_buf, y_hbm.at[pl.ds(chunk * rows, rows)], out_sem)

        def send_ctx(chunk):
            bounce_ctx(chunk).wait()
            relays = (me // FIRST == 2) & (chunk < RELAYED)

            def one(other):
                if other // FIRST == 1:

                    @pl.when(relays)
                    def _():
                        put_relay(chunk, other, me - 2 * FIRST).start()

                    @pl.when(jnp.logical_not(relays))
                    def _():
                        put_ctx(chunk, other, me).start()

                else:
                    put_ctx(chunk, other, me).start()

            each_peer(one, FIRST)

        def send_near(chunk):
            bounce_near(chunk).wait()
            put_ctx_near(chunk).start()

        def pass_on(chunk):
            for slot in range(FIRST):
                put_relay(chunk, me + FIRST, slot).wait_recv()
                forward(chunk, slot).start()

        def load_qkv(chunk):
            with jax.named_scope("wait_qkv"):
                for kind in range(3):
                    each_peer(lambda other: put(chunk, kind, me, other).wait_recv(), 0 if kind else FIRST)
                    get_qkv(chunk, kind).start()

            @pl.when(is_first)
            def _():
                for kind in range(3):
                    put_near(chunk, kind).wait_recv()
                    get_own_near(chunk, kind).start()
                    get_other_near(chunk, kind).start()

        get_up(0).start()
        get_down(0).start()
        get_w_out().start()

        @pl.loop(0, N_CHUNKS + 1)
        def _(chunk):
            early = steps - LATE_STEPS
            first = chunk * early // N_CHUNKS
            last = jnp.where(chunk < N_CHUNKS, (chunk + 1) * early // N_CHUNKS, steps)

            @pl.loop(first, last)
            def _(f):
                slot = lax.rem(f, 2)

                @pl.when(f + 1 < steps)
                def _():
                    get_up(f + 1).start()
                    get_down(f + 1).start()

                @pl.when((f == last - 1) & (chunk < N_CHUNKS - 1))
                def _():
                    load_qkv(chunk)

                with jax.named_scope("wait_w"):
                    get_up(f).wait()
                    get_down(f).wait()
                with jax.named_scope("mlp"):
                    for r in range(n_batch * seq_dev // 512):
                        rs = pl.ds(r * 512, 512)
                        up = jnp.dot(h_mlp[rs, :], up_buf[slot], preferred_element_type=F32)
                        hid = (0.5 * up * (1.0 + lax.erf(up * 0.5**0.5))).astype(BF16)
                        acc[rs, :] += jnp.dot(hid, down_buf[slot], preferred_element_type=F32)

                with jax.named_scope("send_ctx"):
                    @pl.when((f == first) & (chunk > 0))
                    def _():
                        @pl.when(chunk < N_CHUNKS)
                        def _():
                            send_ctx(chunk - 1)

                        @pl.when(is_first)
                        def _():
                            send_near(chunk - 1)

                with jax.named_scope("pass_on"):
                    @pl.when(is_first & (chunk == N_CHUNKS))
                    def _():
                        first_relay = 1 + (f - first) * 2

                        @pl.loop(first_relay, jnp.minimum(jnp.where(f == steps - 1, RELAYED, first_relay + 2), RELAYED))
                        def _(c):
                            pass_on(c)

            @pl.when(chunk < N_CHUNKS)
            def _():
                @pl.when(chunk == N_CHUNKS - 1)
                def _():
                    load_qkv(chunk)

                with jax.named_scope("attn"):
                    for kind in range(3):
                        get_qkv(chunk, kind).wait()
                    for b in range(nb):
                        for h in range(heads):
                            q = qkv_buf[0, b, h, FIRST:].reshape(later * seq_dev, head_dim)
                            k, v = (qkv_buf[t, b, h].reshape(n * seq_dev, head_dim) for t in (1, 2))
                            per = Q_TILE // seq_dev

                            def write(i, out):
                                ctx_buf[b, i * per : (i + 1) * per, :, h * head_dim : (h + 1) * head_dim] = out.reshape(
                                    per, seq_dev, head_dim
                                )

                            causal_head(q, k, v, write)
                bounce_ctx(chunk).start()

                @pl.when(jnp.logical_not(is_first))
                def _():
                    rows_of(chunk, me)[...] = ctx_buf[:, me - FIRST]

                with jax.named_scope("send_last"):
                    @pl.when(chunk == N_CHUNKS - 1)
                    def _():
                        send_ctx(chunk)

                        @pl.when(is_first)
                        def _():
                            pass_on(0)

                with jax.named_scope("near"):
                    @pl.when(is_first)
                    def _():
                        for kind in range(3):
                            get_own_near(chunk, kind).wait()
                            get_other_near(chunk, kind).wait()

                        @pl.loop(0, nb)
                        def _(b):
                            for d in range(dests):
                                for h in range(heads):
                                    q, k, v = (both[t, b, d, h].reshape(Q_TILE, head_dim) for t in range(3))

                                    def write(i, out):
                                        col = (d * heads + h) * head_dim
                                        near_buf[b, :, :, col : col + head_dim] = out.reshape(
                                            FIRST, seq_dev, head_dim
                                        )

                                    causal_head(q, k, v, write)

                        bounce_near(chunk).start()
                        rows_of(chunk, me * dests, dests)[...] = near_buf[:, me]

        get_w_out().wait()

        @pl.loop(0, N_CHUNKS)
        def _(turn):
            chunk = jnp.where(turn == 2, RELAYED, jnp.where((turn > 2) & (turn <= RELAYED), turn - 1, turn))

            with jax.named_scope("wait_ctx"):
                @pl.when(is_first)
                def _():
                    put_ctx_near(chunk).wait_recv()

                @pl.when(jnp.logical_not(is_first))
                def _():
                    each_peer(lambda other: put_ctx(chunk, me, other).wait_recv())

            with jax.named_scope("out_proj"):
                @pl.when(turn > 0)
                def _():
                    put_y(chunk).wait()

                g = pl.ds(pl.multiple_of(chunk * rows, rows), rows)
                for c in range(0, width, 1024):
                    cs = slice(c, c + 1024)
                    left = ctx_rows[pl.ds(chunk * nb, nb)].reshape(rows, width)
                    attn = jnp.dot(left, w_buf[:, cs], preferred_element_type=F32)
                    y_buf[:, cs] = (acc[g, cs] + attn).astype(BF16)
                put_y(chunk).start()

        put_y(N_CHUNKS - 1).wait()

    pl.run_scoped(
        rest,
        pltpu.VMEM((2, width, UP_TILE), BF16),
        pltpu.VMEM((2, UP_TILE, width), BF16),
        pltpu.VMEM((width, width), BF16),
        pltpu.VMEM((3, nb, heads, n, seq_dev, head_dim), BF16),
        pltpu.VMEM((nb, n - FIRST, seq_dev, cols), BF16),
        pltpu.VMEM((3, nb, dests, heads, FIRST, seq_dev, head_dim), BF16),
        pltpu.VMEM((nb, FIRST, seq_dev, dests * cols), BF16),
        pltpu.VMEM((rows, width), BF16),
    )

    @pl.loop(0, N_CHUNKS)
    def _(chunk):
        def sent(other):
            put(chunk, 1, other, me).wait_send()
            put(chunk, 2, other, me).wait_send()

        each_peer(sent)
        each_peer(lambda other: put_ctx(chunk, other, me).wait_send(), FIRST)

        @pl.when(is_first)
        def _():
            for kind in range(3):
                put_near(chunk, kind).wait_send()
            put_ctx_near(chunk).wait_send()

            @pl.when(chunk < RELAYED)
            def _():
                for slot in range(FIRST):
                    forward(chunk, slot).wait_send()

        @pl.when(jnp.logical_not(is_first))
        def _():
            each_peer(lambda other: put(chunk, 0, other, me).wait_send())


def solution(mesh):
    n = mesh.shape["sp"]

    def local_layer(x_blk, ln_attn_w, ln_attn_b, ln_mlp_w, ln_mlp_b, w_qkv, w_out, w_up, w_down):
        n_batch, seq_dev, width = x_blk.shape
        groups, head_dim = w_qkv.shape[1], w_qkv.shape[3]
        heads = groups // n
        nb = n_batch // N_CHUNKS
        rows = n_batch * seq_dev
        dests = QKV_HEADS // heads
        ffn = w_up.shape[1]
        cos_t, sin_t = rope_tables(n * seq_dev, head_dim)
        row = lambda p: p.reshape(1, width)
        anywhere = pl.BlockSpec(memory_space=pl.ANY)
        flops = 2 * rows * width * (3 * width + 2 * ffn) + 2 * rows * n * seq_dev * width * 2
        y_out, recv, *_ = pl.pallas_call(
            functools.partial(layer_kernel, n),
            out_shape=[
                jax.ShapeDtypeStruct((rows, width), BF16),
                jax.ShapeDtypeStruct((3, n_batch, heads, n, seq_dev, head_dim), BF16),
                jax.ShapeDtypeStruct((3, n_batch, n, heads, seq_dev, head_dim), BF16),
                jax.ShapeDtypeStruct((n_batch, n, seq_dev, heads * head_dim), BF16),
                jax.ShapeDtypeStruct((3, n_batch, dests, heads, seq_dev, head_dim), BF16),
                jax.ShapeDtypeStruct((n_batch, FIRST, seq_dev, dests * heads * head_dim), BF16),
                jax.ShapeDtypeStruct((n_batch, FIRST, seq_dev, heads * head_dim), BF16),
            ],
            in_specs=[anywhere] * 11,
            out_specs=[anywhere] * 7,
            scratch_shapes=[
                pltpu.VMEM((rows, width), BF16),
                pltpu.VMEM((rows, width), F32),
                pltpu.VMEM((n_batch, seq_dev, width), BF16),
                pltpu.VMEM((4, 1, width), F32),
                pltpu.SemaphoreType.DMA,
                pltpu.SemaphoreType.DMA((4,)),
                pltpu.SemaphoreType.DMA((2,)),
                pltpu.SemaphoreType.DMA((2,)),
                pltpu.SemaphoreType.DMA((5,)),
                pltpu.SemaphoreType.DMA,
                pltpu.SemaphoreType.DMA((2,)),
                pltpu.SemaphoreType.DMA((2,)),
                pltpu.SemaphoreType.DMA((3,)),
                pltpu.SemaphoreType.DMA((3, 2)),
                pltpu.SemaphoreType.DMA((N_CHUNKS, 3, n)),
                pltpu.SemaphoreType.DMA((N_CHUNKS, 3, n)),
                pltpu.SemaphoreType.DMA((N_CHUNKS, n)),
                pltpu.SemaphoreType.DMA((N_CHUNKS, n)),
                pltpu.SemaphoreType.DMA((N_CHUNKS, 3)),
                pltpu.SemaphoreType.DMA((N_CHUNKS, 3)),
                pltpu.SemaphoreType.DMA((N_CHUNKS,)),
                pltpu.SemaphoreType.DMA((N_CHUNKS,)),
                pltpu.SemaphoreType.DMA((N_CHUNKS, FIRST)),
                pltpu.SemaphoreType.DMA((N_CHUNKS, FIRST)),
            ],
            compiler_params=pltpu.CompilerParams(
                collective_id=0, has_side_effects=True, vmem_limit_bytes=63 * 2**20
            ),
            cost_estimate=pl.CostEstimate(flops=flops, bytes_accessed=3 * 10**8, transcendentals=10**7),
            name="layer",
        )(
            x_blk.reshape(rows, width),
            cos_t,
            sin_t,
            row(ln_attn_w),
            row(ln_attn_b),
            row(ln_mlp_w),
            row(ln_mlp_b),
            w_qkv.transpose(0, 2, 1, 3),
            w_out,
            w_up,
            w_down,
        )
        shape = (n_batch, heads, n * seq_dev, head_dim)
        return y_out.reshape(x_blk.shape), recv[1].reshape(shape), recv[2].reshape(shape)

    act_spec, cache_spec = P("dp", "sp", None), P("dp", "sp", None, None)
    return jax.shard_map(
        local_layer,
        mesh=mesh,
        in_specs=(act_spec,) + (P(),) * 8,
        out_specs=(act_spec, cache_spec, cache_spec),
        check_vma=False,
    )
```

```python
import functools

import jax
import jax.numpy as jnp
import numpy as np
from jax import lax
from jax.experimental import pallas as pl
from jax.experimental.pallas import tpu as pltpu
from jax.sharding import PartitionSpec as P

LN_EPS = 1e-5
ROPE_BASE = 10000.0
LOG2E = 1.4426950408889634
N_CHUNKS = 6
UP_TILE = 512
QKV_HEADS = 8
Q_TILE = 256
FIRST = 2
LATE_STEPS = 2
RELAYED = 4
F32 = jnp.float32
BF16 = jnp.bfloat16


def rope_tables(positions, head_dim):
    half_dim = head_dim // 2
    inv_freq = np.float32(ROPE_BASE) ** (np.float32(-2.0) * np.arange(half_dim, dtype=np.float32) / np.float32(head_dim))
    angles = np.arange(positions, dtype=np.float32)[:, None] * inv_freq[None, :]
    cos_t, sin_t = np.cos(angles.astype(np.float64)), np.sin(angles.astype(np.float64))
    wide = lambda a, b: jnp.asarray(np.concatenate([a, b], -1).astype(np.float32))
    return wide(cos_t, cos_t), wide(-sin_t, sin_t)


def causal_head(q, k, v, write):
    seq, head_dim = k.shape
    scale = LOG2E * head_dim**-0.5
    keys = lax.broadcasted_iota(jnp.int32, (Q_TILE, Q_TILE), 0)
    queries = lax.broadcasted_iota(jnp.int32, (Q_TILE, Q_TILE), 1)
    for i in range(q.shape[0] // Q_TILE):
        lo = seq - q.shape[0] + i * Q_TILE
        hi = lo + Q_TILE
        q_i = q[i * Q_TILE : (i + 1) * Q_TILE]
        scores = lax.dot_general(k[:hi], q_i, (((1,), (1,)), ((), ())), preferred_element_type=F32)
        diag = jnp.where(keys <= queries, scores[lo:], -1e30)
        scores = jnp.concatenate([scores[:lo], diag], axis=0) if lo else diag
        prob = jnp.exp2((scores - jnp.max(scores, axis=0, keepdims=True)) * scale)
        prob = (prob * (1.0 / jnp.sum(prob, axis=0, keepdims=True))).astype(BF16)
        out = lax.dot_general(prob, v[:hi], (((0,), (0,)), ((), ())), preferred_element_type=F32)
        write(i, out.astype(BF16))


def layer_kernel(
    n,
    x_hbm,
    cos_hbm,
    sin_hbm,
    ln_aw_hbm,
    ln_ab_hbm,
    ln_mw_hbm,
    ln_mb_hbm,
    w_qkv,
    w_out,
    w_up,
    w_down,
    y_hbm,
    recv,
    send,
    ctx_send,
    near,
    ctx_near,
    relay,
    h_mlp,
    acc,
    ctx_rows,
    ln_buf,
    x_sem,
    ln_sem,
    w_sem,
    bounce_sem,
    own_sem,
    out_sem,
    up_sem,
    down_sem,
    qkv_sem,
    near_sem,
    send_sem,
    recv_sem,
    ctx_send_sem,
    ctx_recv_sem,
    near_send_sem,
    near_recv_sem,
    ctx_near_send_sem,
    ctx_near_recv_sem,
    relay_recv_sem,
    relay_send_sem,
):
    me = lax.axis_index("sp")
    n_batch, _, heads, seq_dev, head_dim = send.shape[1:]
    cols = heads * head_dim
    width = x_hbm.shape[1]
    nb = n_batch // N_CHUNKS
    rows = nb * seq_dev
    ffn = w_up.shape[1]
    dests = QKV_HEADS // heads
    parts = n // dests
    blocks = 3 * parts

    def peer(step):
        return lax.bitwise_xor(me, step)

    def rows_of(chunk, first, count=1):
        return ctx_rows.at[pl.ds(chunk * nb, nb), :, pl.ds(pl.multiple_of(first * cols, cols), count * cols)]

    def put(chunk, kind, to, frm):
        bs = pl.ds(chunk * nb, nb)
        return pltpu.make_async_remote_copy(
            src_ref=send.at[kind, bs, to],
            dst_ref=recv.at[kind, bs, :, frm],
            send_sem=send_sem.at[chunk],
            recv_sem=recv_sem.at[chunk, kind],
            device_id={"sp": to},
            device_id_type=pl.DeviceIdType.MESH,
        )

    def put_ctx(chunk, to, frm):
        bs = pl.ds(chunk * nb, nb)
        return pltpu.make_async_remote_copy(
            src_ref=ctx_send.at[bs, to],
            dst_ref=rows_of(chunk, frm),
            send_sem=ctx_send_sem.at[chunk],
            recv_sem=ctx_recv_sem.at[chunk],
            device_id={"sp": to},
            device_id_type=pl.DeviceIdType.MESH,
        )

    def put_relay(chunk, to, slot):
        bs = pl.ds(chunk * nb, nb)
        return pltpu.make_async_remote_copy(
            src_ref=ctx_send.at[bs, to],
            dst_ref=relay.at[bs, slot],
            send_sem=ctx_send_sem.at[chunk],
            recv_sem=relay_recv_sem.at[chunk],
            device_id={"sp": to - FIRST},
            device_id_type=pl.DeviceIdType.MESH,
        )

    def forward(chunk, slot):
        bs = pl.ds(chunk * nb, nb)
        return pltpu.make_async_remote_copy(
            src_ref=relay.at[bs, slot],
            dst_ref=rows_of(chunk, 2 * FIRST + slot),
            send_sem=relay_send_sem.at[chunk],
            recv_sem=ctx_recv_sem.at[chunk],
            device_id={"sp": me + FIRST},
            device_id_type=pl.DeviceIdType.MESH,
        )

    def put_near(chunk, kind):
        bs = pl.ds(chunk * nb, nb)
        return pltpu.make_async_remote_copy(
            src_ref=send.at[kind, bs, pl.ds((1 - me) * dests, dests)],
            dst_ref=near.at[kind, bs],
            send_sem=near_send_sem.at[chunk],
            recv_sem=near_recv_sem.at[chunk],
            device_id={"sp": 1 - me},
            device_id_type=pl.DeviceIdType.MESH,
        )

    def put_ctx_near(chunk):
        bs = pl.ds(chunk * nb, nb)
        return pltpu.make_async_remote_copy(
            src_ref=ctx_near.at[bs, 1 - me],
            dst_ref=rows_of(chunk, me * dests, dests),
            send_sem=ctx_near_send_sem.at[chunk],
            recv_sem=ctx_near_recv_sem.at[chunk],
            device_id={"sp": 1 - me},
            device_id_type=pl.DeviceIdType.MESH,
        )

    def drain(ref, sem):
        pltpu.make_async_copy(ref, ref, sem).wait()

    is_first = me < FIRST
    later_on = jnp.logical_not(is_first)

    def each_peer(do, lowest=0):
        for other in range(lowest, n):
            pl.when(other != me)(functools.partial(do, other))

    def qkv_phase(x_buf, h_attn, w_nat, w_cols, out_buf, own, cos_ref, sin_ref):
        mine = pl.ds(pl.multiple_of(me * seq_dev, seq_dev), seq_dev)
        get_cos = pltpu.make_async_copy(cos_hbm.at[mine], cos_ref, own_sem.at[3])
        get_sin = pltpu.make_async_copy(sin_hbm.at[mine], sin_ref, own_sem.at[4])

        def get_x(chunk):
            return pltpu.make_async_copy(x_hbm.at[pl.ds(chunk * rows, rows)], x_buf, x_sem)

        def get_w(half):
            block, slot = half // 2, lax.rem(half, 2)
            src = w_qkv.at[
                pl.ds(slot * (width // 2), width // 2),
                block // parts,
                pl.ds(lax.rem(block, parts) * QKV_HEADS, QKV_HEADS),
            ]
            return pltpu.make_async_copy(src, w_nat.at[slot], w_sem.at[slot])

        def bounce(step):
            slot, block = lax.rem(step, 2), lax.rem(step, blocks)
            dst = send.at[
                block // parts, pl.ds(step // blocks * nb, nb), pl.ds(lax.rem(block, parts) * dests, dests)
            ]
            return pltpu.make_async_copy(out_buf.at[slot], dst, bounce_sem.at[slot])

        def put_own(chunk, kind):
            dst = recv.at[kind, pl.ds(chunk * nb, nb), :, me]
            return pltpu.make_async_copy(own.at[kind], dst, own_sem.at[kind])

        def send_block(step):
            bounce(step).wait()
            block = lax.rem(step, blocks)
            for d in range(dests):
                to = lax.rem(block, parts) * dests + lax.rem(me + d, dests)

                @pl.when((to != me) & jnp.logical_not(is_first & (block < parts)))
                def _():
                    put(step // blocks, block // parts, to, me).start()

            @pl.when(is_first & (lax.rem(block, parts) == 1 - me))
            def _():
                put_near(step // blocks, block // parts).start()

        ln_hbm = (ln_aw_hbm, ln_ab_hbm, ln_mw_hbm, ln_mb_hbm)
        get_ln = [pltpu.make_async_copy(p, ln_buf.at[i], ln_sem.at[i]) for i, p in enumerate(ln_hbm)]
        ln_aw, ln_ab, ln_mw, ln_mb = (ln_buf.at[i] for i in range(4))
        get_x(0).start()
        for copy in get_ln:
            copy.start()
        get_w(0).start()
        get_w(1).start()
        get_cos.start()
        get_sin.start()
        barrier = pltpu.get_barrier_semaphore()
        for step in range(1, n):
            pl.semaphore_signal(
                barrier, inc=1, device_id={"sp": peer(step)}, device_id_type=pl.DeviceIdType.MESH
            )

        @pl.loop(0, N_CHUNKS * blocks)
        def _(step):
            chunk, block = step // blocks, lax.rem(step, blocks)
            kind, part = block // parts, lax.rem(block, parts)
            slot = lax.rem(step, 2)

            with jax.named_scope("ln"):
                @pl.when(block == 0)
                def _():
                    get_x(chunk).wait()

                    @pl.when(chunk == 0)
                    def _():
                        for copy in get_ln:
                            copy.wait()

                    @pl.loop(0, nb)
                    def _(i):
                        r = pl.ds(pl.multiple_of(i * seq_dev, seq_dev), seq_dev)
                        g = pl.ds(pl.multiple_of(chunk * rows + i * seq_dev, seq_dev), seq_dev)
                        xf = x_buf[r, :].astype(F32)
                        mean = jnp.sum(xf, axis=-1, keepdims=True) * (1.0 / width)
                        dev = xf - mean
                        var = jnp.sum(dev * dev, axis=-1, keepdims=True) * (1.0 / width)
                        unit = dev * lax.rsqrt(var + LN_EPS)
                        h_attn[r, :] = (unit * ln_aw[...] + ln_ab[...]).astype(BF16)
                        h_mlp[g, :] = (unit * ln_mw[...] + ln_mb[...]).astype(BF16)
                        acc[g, :] = xf

                    @pl.when(chunk + 1 < N_CHUNKS)
                    def _():
                        get_x(chunk + 1).start()

            with jax.named_scope("relayout"):
                @pl.when(chunk == 0)
                def _():
                    @pl.when(block == 0)
                    def _():
                        get_cos.wait()
                        get_sin.wait()

                    @pl.loop(2 * block, 2 * block + 2)
                    def _(half):
                        get_w(half).wait()

                        @pl.loop(0, width // 2 // 128)
                        def _(i):
                            r = pl.ds(pl.multiple_of(i * 128, 128), 128)
                            top = lax.rem(half, 2) * (width // 2)
                            to = pl.ds(pl.multiple_of(top + i * 128, 128), 128)
                            by_head = jnp.swapaxes(w_nat[lax.rem(half, 2), r].astype(F32), 0, 1)
                            for h in range(QKV_HEADS):
                                w_cols[block, to, h * head_dim : (h + 1) * head_dim] = by_head[h].astype(BF16)

                        @pl.when(half + 2 < 2 * blocks)
                        def _():
                            get_w(half + 2).start()

            with jax.named_scope("qkv_dot"):
                for d in range(dests):
                    cs = slice(d * heads * head_dim, (d + 1) * heads * head_dim)
                    cols = jnp.dot(h_attn[...], w_cols[block, :, cs], preferred_element_type=F32)
                    for h in range(heads):
                        for b in range(nb):
                            u = cols[b * seq_dev : (b + 1) * seq_dev, h * head_dim : (h + 1) * head_dim]
                            u = u.astype(BF16).astype(F32)
                            turned = u * cos_ref[...] + pltpu.roll(u, head_dim // 2, 1) * sin_ref[...]
                            out_buf[slot, b, d, h] = jnp.where(kind < 2, turned, u).astype(BF16)

            with jax.named_scope("qkv_send"):
                bounce(step).start()

                @pl.when(me // dests == part)
                def _():
                    @pl.when(chunk > 0)
                    def _():
                        put_own(chunk - 1, kind).wait()

                    own[kind] = out_buf[slot, :, lax.rem(me, dests)]
                    put_own(chunk, kind).start()

                @pl.when(step == 0)
                def _():
                    pl.semaphore_wait(barrier, n - 1)

                @pl.when(chunk == 0)
                def _():
                    send_block(step)

                @pl.when(step > blocks)
                def _():
                    send_block(step - 1)

        send_block(N_CHUNKS * blocks - 1)
        for kind in range(3):
            put_own(N_CHUNKS - 1, kind).wait()

    pl.run_scoped(
        qkv_phase,
        pltpu.VMEM((rows, width), BF16),
        pltpu.VMEM((rows, width), BF16),
        pltpu.VMEM((2, width // 2, QKV_HEADS, head_dim), BF16),
        pltpu.VMEM((blocks, width, QKV_HEADS * head_dim), BF16),
        pltpu.VMEM((2, nb, dests, heads, seq_dev, head_dim), BF16),
        pltpu.VMEM((3, nb, heads, seq_dev, head_dim), BF16),
        pltpu.VMEM((seq_dev, head_dim), F32),
        pltpu.VMEM((seq_dev, head_dim), F32),
    )

    def rest(up_buf, down_buf, w_buf, qkv_buf, ctx_buf, both, near_buf, y_buf):
        later = n - FIRST
        steps = ffn // UP_TILE

        def get_up(f):
            cols = pl.ds(pl.multiple_of(f * UP_TILE, UP_TILE), UP_TILE)
            slot = lax.rem(f, 2)
            return pltpu.make_async_copy(w_up.at[:, cols], up_buf.at[slot], up_sem.at[slot])

        def get_down(f):
            cols = pl.ds(pl.multiple_of(f * UP_TILE, UP_TILE), UP_TILE)
            slot = lax.rem(f, 2)
            return pltpu.make_async_copy(w_down.at[cols], down_buf.at[slot], down_sem.at[slot])

        def get_w_out():
            return pltpu.make_async_copy(w_out, w_buf, w_sem.at[0])

        def get_qkv(chunk, kind):
            return pltpu.make_async_copy(recv.at[kind, pl.ds(chunk * nb, nb)], qkv_buf.at[kind], qkv_sem.at[kind])

        def get_own_near(chunk, kind):
            src = send.at[kind, pl.ds(chunk * nb, nb), pl.ds(me * dests, dests)]
            return pltpu.make_async_copy(src, both.at[kind, :, :, :, me], near_sem.at[kind, 0])

        def get_other_near(chunk, kind):
            src = near.at[kind, pl.ds(chunk * nb, nb)]
            return pltpu.make_async_copy(src, both.at[kind, :, :, :, 1 - me], near_sem.at[kind, 1])

        def bounce_ctx(chunk):
            dst = ctx_send.at[pl.ds(chunk * nb, nb), pl.ds(FIRST, later)]
            return pltpu.make_async_copy(ctx_buf, dst, bounce_sem.at[0])

        def bounce_near(chunk):
            return pltpu.make_async_copy(near_buf, ctx_near.at[pl.ds(chunk * nb, nb)], bounce_sem.at[1])

        def put_y(chunk, slot):
            return pltpu.make_async_copy(y_buf.at[slot], y_hbm.at[pl.ds(chunk * rows, rows)], out_sem.at[slot])

        def send_ctx(chunk):
            bounce_ctx(chunk).wait()
            relays = (me // FIRST == 2) & (chunk < RELAYED)

            def one(other):
                if other // FIRST == 1:

                    @pl.when(relays)
                    def _():
                        put_relay(chunk, other, me - 2 * FIRST).start()

                    @pl.when(jnp.logical_not(relays))
                    def _():
                        put_ctx(chunk, other, me).start()

                else:
                    put_ctx(chunk, other, me).start()

            each_peer(one, FIRST)

        def send_near(chunk):
            bounce_near(chunk).wait()
            put_ctx_near(chunk).start()

        def pass_on(chunk):
            drain(relay.at[pl.ds(chunk * nb, nb)], relay_recv_sem.at[chunk])
            for slot in range(FIRST):
                forward(chunk, slot).start()

        def load_qkv(chunk):
            with jax.named_scope("wait_qkv"):
                for kind in range(3):
                    got = lambda count: recv.at[kind, pl.ds(chunk * nb, nb), :, pl.ds(0, count)]
                    if kind:
                        drain(got(n - 1), recv_sem.at[chunk, kind])
                    else:
                        pl.when(is_first)(lambda: drain(got(n - FIRST), recv_sem.at[chunk, kind]))
                        pl.when(later_on)(lambda: drain(got(n - FIRST - 1), recv_sem.at[chunk, kind]))
                    get_qkv(chunk, kind).start()

            @pl.when(is_first)
            def _():
                drain(near.at[:, pl.ds(chunk * nb, nb)], near_recv_sem.at[chunk])
                for kind in range(3):
                    get_own_near(chunk, kind).start()
                    get_other_near(chunk, kind).start()

        get_up(0).start()
        get_down(0).start()
        get_w_out().start()

        @pl.loop(0, N_CHUNKS + 1)
        def _(chunk):
            early = steps - LATE_STEPS
            first = chunk * early // N_CHUNKS
            last = jnp.where(chunk < N_CHUNKS, (chunk + 1) * early // N_CHUNKS, steps)

            @pl.loop(first, last)
            def _(f):
                slot = lax.rem(f, 2)

                @pl.when(f + 1 < steps)
                def _():
                    get_up(f + 1).start()
                    get_down(f + 1).start()

                @pl.when((f == last - 1) & (chunk < N_CHUNKS - 1))
                def _():
                    load_qkv(chunk)

                with jax.named_scope("wait_w"):
                    get_up(f).wait()
                    get_down(f).wait()
                with jax.named_scope("mlp"):
                    for r in range(n_batch * seq_dev // 512):
                        rs = pl.ds(r * 512, 512)
                        up = jnp.dot(h_mlp[rs, :], up_buf[slot], preferred_element_type=F32)
                        hid = (0.5 * up * (1.0 + lax.erf(up * 0.5**0.5))).astype(BF16)
                        acc[rs, :] += jnp.dot(hid, down_buf[slot], preferred_element_type=F32)

                with jax.named_scope("send_ctx"):
                    @pl.when((f == first) & (chunk > 0))
                    def _():
                        @pl.when(chunk < N_CHUNKS)
                        def _():
                            send_ctx(chunk - 1)

                        @pl.when(is_first)
                        def _():
                            send_near(chunk - 1)

                with jax.named_scope("pass_on"):
                    @pl.when(is_first & (chunk == N_CHUNKS))
                    def _():
                        first_relay = 1 + (f - first) * 2

                        @pl.loop(first_relay, jnp.minimum(jnp.where(f == steps - 1, RELAYED, first_relay + 2), RELAYED))
                        def _(c):
                            pass_on(c)

            @pl.when(chunk < N_CHUNKS)
            def _():
                @pl.when(chunk == N_CHUNKS - 1)
                def _():
                    load_qkv(chunk)

                with jax.named_scope("attn"):
                    for kind in range(3):
                        get_qkv(chunk, kind).wait()
                    for b in range(nb):
                        for h in range(heads):
                            q = qkv_buf[0, b, h, FIRST:].reshape(later * seq_dev, head_dim)
                            k, v = (qkv_buf[t, b, h].reshape(n * seq_dev, head_dim) for t in (1, 2))
                            per = Q_TILE // seq_dev

                            def write(i, out):
                                ctx_buf[b, i * per : (i + 1) * per, :, h * head_dim : (h + 1) * head_dim] = out.reshape(
                                    per, seq_dev, head_dim
                                )

                            causal_head(q, k, v, write)
                bounce_ctx(chunk).start()

                @pl.when(later_on)
                def _():
                    rows_of(chunk, me)[...] = ctx_buf[:, me - FIRST]

                with jax.named_scope("send_last"):
                    @pl.when(chunk == N_CHUNKS - 1)
                    def _():
                        send_ctx(chunk)

                        @pl.when(is_first)
                        def _():
                            pass_on(0)

                with jax.named_scope("near"):
                    @pl.when(is_first)
                    def _():
                        for kind in range(3):
                            get_own_near(chunk, kind).wait()
                            get_other_near(chunk, kind).wait()

                        @pl.loop(0, nb)
                        def _(b):
                            for d in range(dests):
                                for h in range(heads):
                                    q, k, v = (both[t, b, d, h].reshape(Q_TILE, head_dim) for t in range(3))

                                    def write(i, out):
                                        col = (d * heads + h) * head_dim
                                        near_buf[b, :, :, col : col + head_dim] = out.reshape(
                                            FIRST, seq_dev, head_dim
                                        )

                                    causal_head(q, k, v, write)

                        bounce_near(chunk).start()
                        rows_of(chunk, me * dests, dests)[...] = near_buf[:, me]

        get_w_out().wait()

        @pl.loop(0, N_CHUNKS)
        def _(turn):
            chunk = jnp.where(turn == 2, RELAYED, jnp.where((turn > 2) & (turn <= RELAYED), turn - 1, turn))

            with jax.named_scope("wait_ctx"):
                @pl.when(is_first)
                def _():
                    put_ctx_near(chunk).wait_recv()

                @pl.when(later_on)
                def _():
                    drain(rows_of(chunk, 0, n - 1), ctx_recv_sem.at[chunk])

            with jax.named_scope("out_proj"):
                slot = lax.rem(turn, 2)

                @pl.when(turn > 1)
                def _():
                    put_y(chunk, slot).wait()

                g = pl.ds(pl.multiple_of(chunk * rows, rows), rows)
                for c in range(0, width, 1024):
                    cs = slice(c, c + 1024)
                    left = ctx_rows[pl.ds(chunk * nb, nb)].reshape(rows, width)
                    attn = jnp.dot(left, w_buf[:, cs], preferred_element_type=F32)
                    y_buf[slot, :, cs] = (acc[g, cs] + attn).astype(BF16)
                put_y(chunk, slot).start()

        for slot in range(2):
            put_y(0, slot).wait()

    pl.run_scoped(
        rest,
        pltpu.VMEM((2, width, UP_TILE), BF16),
        pltpu.VMEM((2, UP_TILE, width), BF16),
        pltpu.VMEM((width, width), BF16),
        pltpu.VMEM((3, nb, heads, n, seq_dev, head_dim), BF16),
        pltpu.VMEM((nb, n - FIRST, seq_dev, cols), BF16),
        pltpu.VMEM((3, nb, dests, heads, FIRST, seq_dev, head_dim), BF16),
        pltpu.VMEM((nb, FIRST, seq_dev, dests * cols), BF16),
        pltpu.VMEM((2, rows, width), BF16),
    )

    @pl.loop(0, N_CHUNKS)
    def _(chunk):
        bs = pl.ds(chunk * nb, nb)

        @pl.when(is_first)
        def _():
            drain(send.at[pl.ds(1, 2), bs, pl.ds(0, n - 1)], send_sem.at[chunk])
            drain(near.at[:, bs], near_send_sem.at[chunk])
            drain(ctx_send.at[bs, pl.ds(0, n - FIRST)], ctx_send_sem.at[chunk])
            drain(ctx_near.at[bs, 0], ctx_near_send_sem.at[chunk])
            pl.when(chunk < RELAYED)(lambda: drain(relay.at[bs], relay_send_sem.at[chunk]))

        @pl.when(later_on)
        def _():
            drain(send.at[:, bs, pl.ds(0, n - 1)], send_sem.at[chunk])
            drain(ctx_send.at[bs, pl.ds(0, n - FIRST - 1)], ctx_send_sem.at[chunk])


def solution(mesh):
    n = mesh.shape["sp"]

    def local_layer(x_blk, ln_attn_w, ln_attn_b, ln_mlp_w, ln_mlp_b, w_qkv, w_out, w_up, w_down):
        n_batch, seq_dev, width = x_blk.shape
        groups, head_dim = w_qkv.shape[1], w_qkv.shape[3]
        heads = groups // n
        nb = n_batch // N_CHUNKS
        rows = n_batch * seq_dev
        dests = QKV_HEADS // heads
        ffn = w_up.shape[1]
        cos_t, sin_t = rope_tables(n * seq_dev, head_dim)
        row = lambda p: p.reshape(1, width)
        anywhere = pl.BlockSpec(memory_space=pl.ANY)
        flops = 2 * rows * width * (3 * width + 2 * ffn) + 2 * rows * n * seq_dev * width * 2
        y_out, recv, *_ = pl.pallas_call(
            functools.partial(layer_kernel, n),
            out_shape=[
                jax.ShapeDtypeStruct((rows, width), BF16),
                jax.ShapeDtypeStruct((3, n_batch, heads, n, seq_dev, head_dim), BF16),
                jax.ShapeDtypeStruct((3, n_batch, n, heads, seq_dev, head_dim), BF16),
                jax.ShapeDtypeStruct((n_batch, n, seq_dev, heads * head_dim), BF16),
                jax.ShapeDtypeStruct((3, n_batch, dests, heads, seq_dev, head_dim), BF16),
                jax.ShapeDtypeStruct((n_batch, FIRST, seq_dev, dests * heads * head_dim), BF16),
                jax.ShapeDtypeStruct((n_batch, FIRST, seq_dev, heads * head_dim), BF16),
            ],
            in_specs=[anywhere] * 11,
            out_specs=[anywhere] * 7,
            scratch_shapes=[
                pltpu.VMEM((rows, width), BF16),
                pltpu.VMEM((rows, width), F32),
                pltpu.VMEM((n_batch, seq_dev, width), BF16),
                pltpu.VMEM((4, 1, width), F32),
                pltpu.SemaphoreType.DMA,
                pltpu.SemaphoreType.DMA((4,)),
                pltpu.SemaphoreType.DMA((2,)),
                pltpu.SemaphoreType.DMA((2,)),
                pltpu.SemaphoreType.DMA((5,)),
                pltpu.SemaphoreType.DMA((2,)),
                pltpu.SemaphoreType.DMA((2,)),
                pltpu.SemaphoreType.DMA((2,)),
                pltpu.SemaphoreType.DMA((3,)),
                pltpu.SemaphoreType.DMA((3, 2)),
                pltpu.SemaphoreType.DMA((N_CHUNKS,)),
                pltpu.SemaphoreType.DMA((N_CHUNKS, 3)),
                pltpu.SemaphoreType.DMA((N_CHUNKS,)),
                pltpu.SemaphoreType.DMA((N_CHUNKS,)),
                pltpu.SemaphoreType.DMA((N_CHUNKS,)),
                pltpu.SemaphoreType.DMA((N_CHUNKS,)),
                pltpu.SemaphoreType.DMA((N_CHUNKS,)),
                pltpu.SemaphoreType.DMA((N_CHUNKS,)),
                pltpu.SemaphoreType.DMA((N_CHUNKS,)),
                pltpu.SemaphoreType.DMA((N_CHUNKS,)),
            ],
            compiler_params=pltpu.CompilerParams(
                collective_id=0, has_side_effects=True, vmem_limit_bytes=63 * 2**20
            ),
            cost_estimate=pl.CostEstimate(flops=flops, bytes_accessed=3 * 10**8, transcendentals=10**7),
            name="layer",
        )(
            x_blk.reshape(rows, width),
            cos_t,
            sin_t,
            row(ln_attn_w),
            row(ln_attn_b),
            row(ln_mlp_w),
            row(ln_mlp_b),
            w_qkv.transpose(0, 2, 1, 3),
            w_out,
            w_up,
            w_down,
        )
        shape = (n_batch, heads, n * seq_dev, head_dim)
        return y_out.reshape(x_blk.shape), recv[1].reshape(shape), recv[2].reshape(shape)

    act_spec, cache_spec = P("dp", "sp", None), P("dp", "sp", None, None)
    return jax.shard_map(
        local_layer,
        mesh=mesh,
        in_specs=(act_spec,) + (P(),) * 8,
        out_specs=(act_spec, cache_spec, cache_spec),
        check_vma=False,
    )
```

```python
import functools

import jax
import jax.numpy as jnp
import numpy as np
from jax import lax
from jax.experimental import pallas as pl
from jax.experimental.pallas import tpu as pltpu
from jax.sharding import PartitionSpec as P

LN_EPS = 1e-5
ROPE_BASE = 10000.0
LOG2E = 1.4426950408889634
N_CHUNKS = 6
UP_TILE = 512
QKV_HEADS = 8
Q_TILE = 256
FIRST = 2
LATE_STEPS = 2
RELAYED = 4
F32 = jnp.float32
BF16 = jnp.bfloat16


def rope_tables(positions, head_dim):
    half_dim = head_dim // 2
    inv_freq = np.float32(ROPE_BASE) ** (np.float32(-2.0) * np.arange(half_dim, dtype=np.float32) / np.float32(head_dim))
    angles = np.arange(positions, dtype=np.float32)[:, None] * inv_freq[None, :]
    cos_t, sin_t = np.cos(angles.astype(np.float64)), np.sin(angles.astype(np.float64))
    wide = lambda a, b: jnp.asarray(np.concatenate([a, b], -1).astype(np.float32))
    return wide(cos_t, cos_t), wide(-sin_t, sin_t)


def causal_head(q, k, v, write):
    seq, head_dim = k.shape
    scale = LOG2E * head_dim**-0.5
    keys = lax.broadcasted_iota(jnp.int32, (Q_TILE, Q_TILE), 0)
    queries = lax.broadcasted_iota(jnp.int32, (Q_TILE, Q_TILE), 1)
    for i in range(q.shape[0] // Q_TILE):
        lo = seq - q.shape[0] + i * Q_TILE
        hi = lo + Q_TILE
        q_i = q[i * Q_TILE : (i + 1) * Q_TILE]
        scores = lax.dot_general(k[:hi], q_i, (((1,), (1,)), ((), ())), preferred_element_type=F32)
        diag = jnp.where(keys <= queries, scores[lo:], -1e30)
        scores = jnp.concatenate([scores[:lo], diag], axis=0) if lo else diag
        prob = jnp.exp2((scores - jnp.max(scores, axis=0, keepdims=True)) * scale)
        prob = (prob * (1.0 / jnp.sum(prob, axis=0, keepdims=True))).astype(BF16)
        out = lax.dot_general(prob, v[:hi], (((0,), (0,)), ((), ())), preferred_element_type=F32)
        write(i, out.astype(BF16))


def layer_kernel(
    n,
    x_hbm,
    cos_hbm,
    sin_hbm,
    ln_aw_hbm,
    ln_ab_hbm,
    ln_mw_hbm,
    ln_mb_hbm,
    w_qkv,
    w_out,
    w_up,
    w_down,
    h_mlp,
    recv,
    send,
    ctx_send,
    near,
    ctx_near,
    relay,
    acc,
    ctx_rows,
    ln_buf,
    x_sem,
    ln_sem,
    w_sem,
    bounce_sem,
    own_sem,
    up_sem,
    down_sem,
    qkv_sem,
    near_sem,
    send_sem,
    recv_sem,
    ctx_send_sem,
    ctx_recv_sem,
    near_send_sem,
    near_recv_sem,
    ctx_near_send_sem,
    ctx_near_recv_sem,
    relay_recv_sem,
    relay_send_sem,
):
    me = lax.axis_index("sp")
    n_batch, _, heads, seq_dev, head_dim = send.shape[1:]
    cols = heads * head_dim
    width = x_hbm.shape[1]
    nb = n_batch // N_CHUNKS
    rows = nb * seq_dev
    ffn = w_up.shape[1]
    dests = QKV_HEADS // heads
    parts = n // dests
    blocks = 3 * parts

    def peer(step):
        return lax.bitwise_xor(me, step)

    def rows_of(chunk, first, count=1):
        return ctx_rows.at[pl.ds(chunk * nb, nb), :, pl.ds(pl.multiple_of(first * cols, cols), count * cols)]

    def put(chunk, kind, to, frm):
        bs = pl.ds(chunk * nb, nb)
        return pltpu.make_async_remote_copy(
            src_ref=send.at[kind, bs, to],
            dst_ref=recv.at[kind, bs, :, frm],
            send_sem=send_sem.at[chunk],
            recv_sem=recv_sem.at[chunk, kind],
            device_id={"sp": to},
            device_id_type=pl.DeviceIdType.MESH,
        )

    def put_ctx(chunk, to, frm):
        bs = pl.ds(chunk * nb, nb)
        return pltpu.make_async_remote_copy(
            src_ref=ctx_send.at[bs, to],
            dst_ref=rows_of(chunk, frm),
            send_sem=ctx_send_sem.at[chunk],
            recv_sem=ctx_recv_sem.at[chunk],
            device_id={"sp": to},
            device_id_type=pl.DeviceIdType.MESH,
        )

    def put_relay(chunk, to, slot):
        bs = pl.ds(chunk * nb, nb)
        return pltpu.make_async_remote_copy(
            src_ref=ctx_send.at[bs, to],
            dst_ref=relay.at[bs, slot],
            send_sem=ctx_send_sem.at[chunk],
            recv_sem=relay_recv_sem.at[chunk],
            device_id={"sp": to - FIRST},
            device_id_type=pl.DeviceIdType.MESH,
        )

    def forward(chunk, slot):
        bs = pl.ds(chunk * nb, nb)
        return pltpu.make_async_remote_copy(
            src_ref=relay.at[bs, slot],
            dst_ref=rows_of(chunk, 2 * FIRST + slot),
            send_sem=relay_send_sem.at[chunk],
            recv_sem=ctx_recv_sem.at[chunk],
            device_id={"sp": me + FIRST},
            device_id_type=pl.DeviceIdType.MESH,
        )

    def put_near(chunk, kind):
        bs = pl.ds(chunk * nb, nb)
        return pltpu.make_async_remote_copy(
            src_ref=send.at[kind, bs, pl.ds((1 - me) * dests, dests)],
            dst_ref=near.at[kind, bs],
            send_sem=near_send_sem.at[chunk],
            recv_sem=near_recv_sem.at[chunk],
            device_id={"sp": 1 - me},
            device_id_type=pl.DeviceIdType.MESH,
        )

    def put_ctx_near(chunk):
        bs = pl.ds(chunk * nb, nb)
        return pltpu.make_async_remote_copy(
            src_ref=ctx_near.at[bs, 1 - me],
            dst_ref=rows_of(chunk, me * dests, dests),
            send_sem=ctx_near_send_sem.at[chunk],
            recv_sem=ctx_near_recv_sem.at[chunk],
            device_id={"sp": 1 - me},
            device_id_type=pl.DeviceIdType.MESH,
        )

    def drain(ref, sem):
        pltpu.make_async_copy(ref, ref, sem).wait()

    is_first = me < FIRST
    later_on = jnp.logical_not(is_first)

    def each_peer(do, lowest=0):
        for other in range(lowest, n):
            pl.when(other != me)(functools.partial(do, other))

    def qkv_phase(x_buf, h_attn, w_nat, w_cols, out_buf, own, cos_ref, sin_ref):
        mine = pl.ds(pl.multiple_of(me * seq_dev, seq_dev), seq_dev)
        get_cos = pltpu.make_async_copy(cos_hbm.at[mine], cos_ref, own_sem.at[3])
        get_sin = pltpu.make_async_copy(sin_hbm.at[mine], sin_ref, own_sem.at[4])

        def get_x(chunk):
            return pltpu.make_async_copy(x_hbm.at[pl.ds(chunk * rows, rows)], x_buf, x_sem)

        def get_w(half):
            block, slot = half // 2, lax.rem(half, 2)
            src = w_qkv.at[
                pl.ds(slot * (width // 2), width // 2),
                block // parts,
                pl.ds(lax.rem(block, parts) * QKV_HEADS, QKV_HEADS),
            ]
            return pltpu.make_async_copy(src, w_nat.at[slot], w_sem.at[slot])

        def bounce(step):
            slot, block = lax.rem(step, 2), lax.rem(step, blocks)
            dst = send.at[
                block // parts, pl.ds(step // blocks * nb, nb), pl.ds(lax.rem(block, parts) * dests, dests)
            ]
            return pltpu.make_async_copy(out_buf.at[slot], dst, bounce_sem.at[slot])

        def put_own(chunk, kind):
            dst = recv.at[kind, pl.ds(chunk * nb, nb), :, me]
            return pltpu.make_async_copy(own.at[kind], dst, own_sem.at[kind])

        def send_block(step):
            bounce(step).wait()
            block = lax.rem(step, blocks)
            for d in range(dests):
                to = lax.rem(block, parts) * dests + lax.rem(me + d, dests)

                @pl.when((to != me) & jnp.logical_not(is_first & (block < parts)))
                def _():
                    put(step // blocks, block // parts, to, me).start()

            @pl.when(is_first & (lax.rem(block, parts) == 1 - me))
            def _():
                put_near(step // blocks, block // parts).start()

        ln_hbm = (ln_aw_hbm, ln_ab_hbm, ln_mw_hbm, ln_mb_hbm)
        get_ln = [pltpu.make_async_copy(p, ln_buf.at[i], ln_sem.at[i]) for i, p in enumerate(ln_hbm)]
        ln_aw, ln_ab, ln_mw, ln_mb = (ln_buf.at[i] for i in range(4))
        get_x(0).start()
        for copy in get_ln:
            copy.start()
        get_w(0).start()
        get_w(1).start()
        get_cos.start()
        get_sin.start()
        barrier = pltpu.get_barrier_semaphore()
        for step in range(1, n):
            pl.semaphore_signal(
                barrier, inc=1, device_id={"sp": peer(step)}, device_id_type=pl.DeviceIdType.MESH
            )

        @pl.loop(0, N_CHUNKS * blocks)
        def _(step):
            chunk, block = step // blocks, lax.rem(step, blocks)
            kind, part = block // parts, lax.rem(block, parts)
            slot = lax.rem(step, 2)

            with jax.named_scope("ln"):
                @pl.when(block == 0)
                def _():
                    get_x(chunk).wait()

                    @pl.when(chunk == 0)
                    def _():
                        for copy in get_ln:
                            copy.wait()

                    @pl.loop(0, nb)
                    def _(i):
                        r = pl.ds(pl.multiple_of(i * seq_dev, seq_dev), seq_dev)
                        g = pl.ds(pl.multiple_of(chunk * rows + i * seq_dev, seq_dev), seq_dev)
                        xf = x_buf[r, :].astype(F32)
                        mean = jnp.sum(xf, axis=-1, keepdims=True) * (1.0 / width)
                        dev = xf - mean
                        var = jnp.sum(dev * dev, axis=-1, keepdims=True) * (1.0 / width)
                        unit = dev * lax.rsqrt(var + LN_EPS)
                        h_attn[r, :] = (unit * ln_aw[...] + ln_ab[...]).astype(BF16)
                        h_mlp[g, :] = (unit * ln_mw[...] + ln_mb[...]).astype(BF16)
                        acc[g, :] = xf

                    @pl.when(chunk + 1 < N_CHUNKS)
                    def _():
                        get_x(chunk + 1).start()

            with jax.named_scope("relayout"):
                @pl.when(chunk == 0)
                def _():
                    @pl.when(block == 0)
                    def _():
                        get_cos.wait()
                        get_sin.wait()

                    @pl.loop(2 * block, 2 * block + 2)
                    def _(half):
                        get_w(half).wait()

                        @pl.loop(0, width // 2 // 128)
                        def _(i):
                            r = pl.ds(pl.multiple_of(i * 128, 128), 128)
                            top = lax.rem(half, 2) * (width // 2)
                            to = pl.ds(pl.multiple_of(top + i * 128, 128), 128)
                            by_head = jnp.swapaxes(w_nat[lax.rem(half, 2), r].astype(F32), 0, 1)
                            for h in range(QKV_HEADS):
                                w_cols[block, to, h * head_dim : (h + 1) * head_dim] = by_head[h].astype(BF16)

                        @pl.when(half + 2 < 2 * blocks)
                        def _():
                            get_w(half + 2).start()

            with jax.named_scope("qkv_dot"):
                for d in range(dests):
                    cs = slice(d * heads * head_dim, (d + 1) * heads * head_dim)
                    cols = jnp.dot(h_attn[...], w_cols[block, :, cs], preferred_element_type=F32)
                    for h in range(heads):
                        for b in range(nb):
                            u = cols[b * seq_dev : (b + 1) * seq_dev, h * head_dim : (h + 1) * head_dim]
                            u = u.astype(BF16).astype(F32)
                            turned = u * cos_ref[...] + pltpu.roll(u, head_dim // 2, 1) * sin_ref[...]
                            out_buf[slot, b, d, h] = jnp.where(kind < 2, turned, u).astype(BF16)

            with jax.named_scope("qkv_send"):
                bounce(step).start()

                @pl.when(me // dests == part)
                def _():
                    @pl.when(chunk > 0)
                    def _():
                        put_own(chunk - 1, kind).wait()

                    own[kind] = out_buf[slot, :, lax.rem(me, dests)]
                    put_own(chunk, kind).start()

                @pl.when(step == 0)
                def _():
                    pl.semaphore_wait(barrier, n - 1)

                @pl.when(chunk == 0)
                def _():
                    send_block(step)

                @pl.when(step > blocks)
                def _():
                    send_block(step - 1)

        send_block(N_CHUNKS * blocks - 1)
        for kind in range(3):
            put_own(N_CHUNKS - 1, kind).wait()

    pl.run_scoped(
        qkv_phase,
        pltpu.VMEM((rows, width), BF16),
        pltpu.VMEM((rows, width), BF16),
        pltpu.VMEM((2, width // 2, QKV_HEADS, head_dim), BF16),
        pltpu.VMEM((blocks, width, QKV_HEADS * head_dim), BF16),
        pltpu.VMEM((2, nb, dests, heads, seq_dev, head_dim), BF16),
        pltpu.VMEM((3, nb, heads, seq_dev, head_dim), BF16),
        pltpu.VMEM((seq_dev, head_dim), F32),
        pltpu.VMEM((seq_dev, head_dim), F32),
    )

    def rest(up_buf, down_buf, w_buf, qkv_buf, ctx_buf, both, near_buf):
        later = n - FIRST
        steps = ffn // UP_TILE

        def get_up(f):
            cols = pl.ds(pl.multiple_of(f * UP_TILE, UP_TILE), UP_TILE)
            slot = lax.rem(f, 2)
            return pltpu.make_async_copy(w_up.at[:, cols], up_buf.at[slot], up_sem.at[slot])

        def get_down(f):
            cols = pl.ds(pl.multiple_of(f * UP_TILE, UP_TILE), UP_TILE)
            slot = lax.rem(f, 2)
            return pltpu.make_async_copy(w_down.at[cols], down_buf.at[slot], down_sem.at[slot])

        def get_w_out():
            return pltpu.make_async_copy(w_out, w_buf, w_sem.at[0])

        def get_qkv(chunk, kind):
            return pltpu.make_async_copy(recv.at[kind, pl.ds(chunk * nb, nb)], qkv_buf.at[kind], qkv_sem.at[kind])

        def get_own_near(chunk, kind):
            src = send.at[kind, pl.ds(chunk * nb, nb), pl.ds(me * dests, dests)]
            return pltpu.make_async_copy(src, both.at[kind, :, :, :, me], near_sem.at[kind, 0])

        def get_other_near(chunk, kind):
            src = near.at[kind, pl.ds(chunk * nb, nb)]
            return pltpu.make_async_copy(src, both.at[kind, :, :, :, 1 - me], near_sem.at[kind, 1])

        def bounce_ctx(chunk):
            dst = ctx_send.at[pl.ds(chunk * nb, nb), pl.ds(FIRST, later)]
            return pltpu.make_async_copy(ctx_buf, dst, bounce_sem.at[0])

        def bounce_near(chunk):
            return pltpu.make_async_copy(near_buf, ctx_near.at[pl.ds(chunk * nb, nb)], bounce_sem.at[1])

        def send_ctx(chunk):
            bounce_ctx(chunk).wait()
            relays = (me // FIRST == 2) & (chunk < RELAYED)

            def one(other):
                if other // FIRST == 1:

                    @pl.when(relays)
                    def _():
                        put_relay(chunk, other, me - 2 * FIRST).start()

                    @pl.when(jnp.logical_not(relays))
                    def _():
                        put_ctx(chunk, other, me).start()

                else:
                    put_ctx(chunk, other, me).start()

            each_peer(one, FIRST)

        def send_near(chunk):
            bounce_near(chunk).wait()
            put_ctx_near(chunk).start()

        def pass_on(chunk):
            drain(relay.at[pl.ds(chunk * nb, nb)], relay_recv_sem.at[chunk])
            for slot in range(FIRST):
                forward(chunk, slot).start()

        def load_qkv(chunk):
            with jax.named_scope("wait_qkv"):
                for kind in range(3):
                    got = lambda count: recv.at[kind, pl.ds(chunk * nb, nb), :, pl.ds(0, count)]
                    if kind:
                        drain(got(n - 1), recv_sem.at[chunk, kind])
                    else:
                        pl.when(is_first)(lambda: drain(got(n - FIRST), recv_sem.at[chunk, kind]))
                        pl.when(later_on)(lambda: drain(got(n - FIRST - 1), recv_sem.at[chunk, kind]))
                    get_qkv(chunk, kind).start()

            @pl.when(is_first)
            def _():
                drain(near.at[:, pl.ds(chunk * nb, nb)], near_recv_sem.at[chunk])
                for kind in range(3):
                    get_own_near(chunk, kind).start()
                    get_other_near(chunk, kind).start()

        get_up(0).start()
        get_down(0).start()
        get_w_out().start()

        @pl.loop(0, N_CHUNKS + 1)
        def _(chunk):
            early = steps - LATE_STEPS
            first = chunk * early // N_CHUNKS
            last = jnp.where(chunk < N_CHUNKS, (chunk + 1) * early // N_CHUNKS, steps)

            @pl.loop(first, last)
            def _(f):
                slot = lax.rem(f, 2)

                @pl.when(f + 1 < steps)
                def _():
                    get_up(f + 1).start()
                    get_down(f + 1).start()

                @pl.when((f == last - 1) & (chunk < N_CHUNKS - 1))
                def _():
                    load_qkv(chunk)

                with jax.named_scope("wait_w"):
                    get_up(f).wait()
                    get_down(f).wait()
                with jax.named_scope("mlp"):
                    for r in range(n_batch * seq_dev // 512):
                        rs = pl.ds(r * 512, 512)
                        up = jnp.dot(h_mlp[rs, :], up_buf[slot], preferred_element_type=F32)
                        hid = (0.5 * up * (1.0 + lax.erf(up * 0.5**0.5))).astype(BF16)
                        acc[rs, :] += jnp.dot(hid, down_buf[slot], preferred_element_type=F32)

                with jax.named_scope("send_ctx"):
                    @pl.when((f == first) & (chunk > 0))
                    def _():
                        @pl.when(chunk < N_CHUNKS)
                        def _():
                            send_ctx(chunk - 1)

                        @pl.when(is_first)
                        def _():
                            send_near(chunk - 1)

                with jax.named_scope("pass_on"):
                    @pl.when(is_first & (chunk == N_CHUNKS))
                    def _():
                        first_relay = 1 + (f - first) * 2

                        @pl.loop(first_relay, jnp.minimum(jnp.where(f == steps - 1, RELAYED, first_relay + 2), RELAYED))
                        def _(c):
                            pass_on(c)

            @pl.when(chunk < N_CHUNKS)
            def _():
                @pl.when(chunk == N_CHUNKS - 1)
                def _():
                    load_qkv(chunk)

                with jax.named_scope("attn"):
                    for kind in range(3):
                        get_qkv(chunk, kind).wait()
                    for b in range(nb):
                        for h in range(heads):
                            q = qkv_buf[0, b, h, FIRST:].reshape(later * seq_dev, head_dim)
                            k, v = (qkv_buf[t, b, h].reshape(n * seq_dev, head_dim) for t in (1, 2))
                            per = Q_TILE // seq_dev

                            def write(i, out):
                                ctx_buf[b, i * per : (i + 1) * per, :, h * head_dim : (h + 1) * head_dim] = out.reshape(
                                    per, seq_dev, head_dim
                                )

                            causal_head(q, k, v, write)
                bounce_ctx(chunk).start()

                @pl.when(later_on)
                def _():
                    rows_of(chunk, me)[...] = ctx_buf[:, me - FIRST]

                with jax.named_scope("send_last"):
                    @pl.when(chunk == N_CHUNKS - 1)
                    def _():
                        send_ctx(chunk)

                        @pl.when(is_first)
                        def _():
                            pass_on(0)

                with jax.named_scope("near"):
                    @pl.when(is_first)
                    def _():
                        for kind in range(3):
                            get_own_near(chunk, kind).wait()
                            get_other_near(chunk, kind).wait()

                        @pl.loop(0, nb)
                        def _(b):
                            for d in range(dests):
                                for h in range(heads):
                                    q, k, v = (both[t, b, d, h].reshape(Q_TILE, head_dim) for t in range(3))

                                    def write(i, out):
                                        col = (d * heads + h) * head_dim
                                        near_buf[b, :, :, col : col + head_dim] = out.reshape(
                                            FIRST, seq_dev, head_dim
                                        )

                                    causal_head(q, k, v, write)

                        bounce_near(chunk).start()
                        rows_of(chunk, me * dests, dests)[...] = near_buf[:, me]

        get_w_out().wait()

        @pl.loop(0, N_CHUNKS)
        def _(turn):
            chunk = jnp.where(turn == 2, RELAYED, jnp.where((turn > 2) & (turn <= RELAYED), turn - 1, turn))

            with jax.named_scope("wait_ctx"):
                @pl.when(is_first)
                def _():
                    put_ctx_near(chunk).wait_recv()

                @pl.when(later_on)
                def _():
                    drain(rows_of(chunk, 0, n - 1), ctx_recv_sem.at[chunk])

            with jax.named_scope("out_proj"):
                g = pl.ds(pl.multiple_of(chunk * rows, rows), rows)
                for c in range(0, width, 1024):
                    cs = slice(c, c + 1024)
                    left = ctx_rows[pl.ds(chunk * nb, nb)].reshape(rows, width)
                    attn = jnp.dot(left, w_buf[:, cs], preferred_element_type=F32)
                    h_mlp[g, cs] = (acc[g, cs] + attn).astype(BF16)


    pl.run_scoped(
        rest,
        pltpu.VMEM((2, width, UP_TILE), BF16),
        pltpu.VMEM((2, UP_TILE, width), BF16),
        pltpu.VMEM((width, width), BF16),
        pltpu.VMEM((3, nb, heads, n, seq_dev, head_dim), BF16),
        pltpu.VMEM((nb, n - FIRST, seq_dev, cols), BF16),
        pltpu.VMEM((3, nb, dests, heads, FIRST, seq_dev, head_dim), BF16),
        pltpu.VMEM((nb, FIRST, seq_dev, dests * cols), BF16),
    )

    @pl.loop(0, N_CHUNKS)
    def _(chunk):
        bs = pl.ds(chunk * nb, nb)

        @pl.when(is_first)
        def _():
            drain(send.at[pl.ds(1, 2), bs, pl.ds(0, n - 1)], send_sem.at[chunk])
            drain(near.at[:, bs], near_send_sem.at[chunk])
            drain(ctx_send.at[bs, pl.ds(0, n - FIRST)], ctx_send_sem.at[chunk])
            drain(ctx_near.at[bs, 0], ctx_near_send_sem.at[chunk])
            pl.when(chunk < RELAYED)(lambda: drain(relay.at[bs], relay_send_sem.at[chunk]))

        @pl.when(later_on)
        def _():
            drain(send.at[:, bs, pl.ds(0, n - 1)], send_sem.at[chunk])
            drain(ctx_send.at[bs, pl.ds(0, n - FIRST - 1)], ctx_send_sem.at[chunk])


def solution(mesh):
    n = mesh.shape["sp"]

    def local_layer(x_blk, ln_attn_w, ln_attn_b, ln_mlp_w, ln_mlp_b, w_qkv, w_out, w_up, w_down):
        n_batch, seq_dev, width = x_blk.shape
        groups, head_dim = w_qkv.shape[1], w_qkv.shape[3]
        heads = groups // n
        nb = n_batch // N_CHUNKS
        rows = n_batch * seq_dev
        dests = QKV_HEADS // heads
        ffn = w_up.shape[1]
        cos_t, sin_t = rope_tables(n * seq_dev, head_dim)
        row = lambda p: p.reshape(1, width)
        anywhere = pl.BlockSpec(memory_space=pl.ANY)
        flops = 2 * rows * width * (3 * width + 2 * ffn) + 2 * rows * n * seq_dev * width * 2
        y_out, recv, *_ = pl.pallas_call(
            functools.partial(layer_kernel, n),
            out_shape=[
                pltpu.VMEM((rows, width), BF16),
                jax.ShapeDtypeStruct((3, n_batch, heads, n, seq_dev, head_dim), BF16),
                jax.ShapeDtypeStruct((3, n_batch, n, heads, seq_dev, head_dim), BF16),
                jax.ShapeDtypeStruct((n_batch, n, seq_dev, heads * head_dim), BF16),
                jax.ShapeDtypeStruct((3, n_batch, dests, heads, seq_dev, head_dim), BF16),
                jax.ShapeDtypeStruct((n_batch, FIRST, seq_dev, dests * heads * head_dim), BF16),
                jax.ShapeDtypeStruct((n_batch, FIRST, seq_dev, heads * head_dim), BF16),
            ],
            in_specs=[anywhere] * 11,
            out_specs=[pl.BlockSpec(memory_space=pltpu.VMEM)] + [anywhere] * 6,
            scratch_shapes=[
                pltpu.VMEM((rows, width), F32),
                pltpu.VMEM((n_batch, seq_dev, width), BF16),
                pltpu.VMEM((4, 1, width), F32),
                pltpu.SemaphoreType.DMA,
                pltpu.SemaphoreType.DMA((4,)),
                pltpu.SemaphoreType.DMA((2,)),
                pltpu.SemaphoreType.DMA((2,)),
                pltpu.SemaphoreType.DMA((5,)),
                pltpu.SemaphoreType.DMA((2,)),
                pltpu.SemaphoreType.DMA((2,)),
                pltpu.SemaphoreType.DMA((3,)),
                pltpu.SemaphoreType.DMA((3, 2)),
                pltpu.SemaphoreType.DMA((N_CHUNKS,)),
                pltpu.SemaphoreType.DMA((N_CHUNKS, 3)),
                pltpu.SemaphoreType.DMA((N_CHUNKS,)),
                pltpu.SemaphoreType.DMA((N_CHUNKS,)),
                pltpu.SemaphoreType.DMA((N_CHUNKS,)),
                pltpu.SemaphoreType.DMA((N_CHUNKS,)),
                pltpu.SemaphoreType.DMA((N_CHUNKS,)),
                pltpu.SemaphoreType.DMA((N_CHUNKS,)),
                pltpu.SemaphoreType.DMA((N_CHUNKS,)),
                pltpu.SemaphoreType.DMA((N_CHUNKS,)),
            ],
            compiler_params=pltpu.CompilerParams(
                collective_id=0, has_side_effects=True, vmem_limit_bytes=57 * 2**20
            ),
            cost_estimate=pl.CostEstimate(flops=flops, bytes_accessed=3 * 10**8, transcendentals=10**7),
            name="layer",
        )(
            x_blk.reshape(rows, width),
            cos_t,
            sin_t,
            row(ln_attn_w),
            row(ln_attn_b),
            row(ln_mlp_w),
            row(ln_mlp_b),
            w_qkv.transpose(0, 2, 1, 3),
            w_out,
            w_up,
            w_down,
        )
        shape = (n_batch, heads, n * seq_dev, head_dim)
        return y_out.reshape(x_blk.shape), recv[1].reshape(shape), recv[2].reshape(shape)

    act_spec, cache_spec = P("dp", "sp", None), P("dp", "sp", None, None)
    return jax.shard_map(
        local_layer,
        mesh=mesh,
        in_specs=(act_spec,) + (P(),) * 8,
        out_specs=(act_spec, cache_spec, cache_spec),
        check_vma=False,
    )
```

```python
import functools

import jax
import jax.numpy as jnp
import numpy as np
from jax import lax
from jax.experimental import pallas as pl
from jax.experimental.pallas import tpu as pltpu
from jax.sharding import PartitionSpec as P

LN_EPS = 1e-5
ROPE_BASE = 10000.0
LOG2E = 1.4426950408889634
N_CHUNKS = 6
UP_TILE = 512
QKV_HEADS = 8
Q_TILE = 256
FIRST = 2
LATE_STEPS = 2
RELAYED = 4
F32 = jnp.float32
BF16 = jnp.bfloat16


def rope_tables(positions, head_dim):
    half_dim = head_dim // 2
    inv_freq = np.float32(ROPE_BASE) ** (np.float32(-2.0) * np.arange(half_dim, dtype=np.float32) / np.float32(head_dim))
    angles = np.arange(positions, dtype=np.float32)[:, None] * inv_freq[None, :]
    cos_t, sin_t = np.cos(angles.astype(np.float64)), np.sin(angles.astype(np.float64))
    wide = lambda a, b: jnp.asarray(np.concatenate([a, b], -1).astype(np.float32))
    return wide(cos_t, cos_t), wide(-sin_t, sin_t)


def causal_head(q, k, v, write):
    seq, head_dim = k.shape
    scale = LOG2E * head_dim**-0.5
    keys = lax.broadcasted_iota(jnp.int32, (Q_TILE, Q_TILE), 0)
    queries = lax.broadcasted_iota(jnp.int32, (Q_TILE, Q_TILE), 1)
    for i in range(q.shape[0] // Q_TILE):
        lo = seq - q.shape[0] + i * Q_TILE
        hi = lo + Q_TILE
        q_i = q[i * Q_TILE : (i + 1) * Q_TILE]
        scores = lax.dot_general(k[:hi], q_i, (((1,), (1,)), ((), ())), preferred_element_type=F32)
        diag = jnp.where(keys <= queries, scores[lo:], -1e30)
        scores = jnp.concatenate([scores[:lo], diag], axis=0) if lo else diag
        prob = jnp.exp2((scores - jnp.max(scores, axis=0, keepdims=True)) * scale)
        prob = (prob * (1.0 / jnp.sum(prob, axis=0, keepdims=True))).astype(BF16)
        out = lax.dot_general(prob, v[:hi], (((0,), (0,)), ((), ())), preferred_element_type=F32)
        write(i, out.astype(BF16))


def layer_kernel(
    n,
    x_hbm,
    cos_hbm,
    sin_hbm,
    ln_aw_hbm,
    ln_ab_hbm,
    ln_mw_hbm,
    ln_mb_hbm,
    w_qkv,
    w_out,
    w_up,
    w_down,
    h_mlp,
    recv,
    send,
    ctx_send,
    near,
    ctx_near,
    relay,
    acc,
    ctx_rows,
    ln_buf,
    x_sem,
    ln_sem,
    w_sem,
    bounce_sem,
    own_sem,
    up_sem,
    down_sem,
    qkv_sem,
    near_sem,
    send_sem,
    recv_sem,
    ctx_send_sem,
    ctx_recv_sem,
    near_send_sem,
    near_recv_sem,
    ctx_near_send_sem,
    ctx_near_recv_sem,
    relay_recv_sem,
    relay_send_sem,
):
    me = lax.axis_index("sp")
    n_batch, _, heads, seq_dev, head_dim = send.shape[1:]
    cols = heads * head_dim
    width = x_hbm.shape[1]
    nb = n_batch // N_CHUNKS
    rows = nb * seq_dev
    ffn = w_up.shape[1]
    dests = QKV_HEADS // heads
    parts = n // dests
    blocks = 3 * parts

    def peer(step):
        return lax.bitwise_xor(me, step)

    def rows_of(chunk, first, count=1):
        return ctx_rows.at[pl.ds(chunk * nb, nb), :, pl.ds(pl.multiple_of(first * cols, cols), count * cols)]

    def put(chunk, kind, to, frm):
        bs = pl.ds(chunk * nb, nb)
        return pltpu.make_async_remote_copy(
            src_ref=send.at[kind, bs, to],
            dst_ref=recv.at[kind, bs, :, frm],
            send_sem=send_sem.at[chunk],
            recv_sem=recv_sem.at[chunk, kind],
            device_id={"sp": to},
            device_id_type=pl.DeviceIdType.MESH,
        )

    def put_ctx(chunk, to, frm):
        bs = pl.ds(chunk * nb, nb)
        return pltpu.make_async_remote_copy(
            src_ref=ctx_send.at[bs, to],
            dst_ref=rows_of(chunk, frm),
            send_sem=ctx_send_sem.at[chunk],
            recv_sem=ctx_recv_sem.at[chunk, frm // FIRST],
            device_id={"sp": to},
            device_id_type=pl.DeviceIdType.MESH,
        )

    def put_relay(chunk, to, slot):
        bs = pl.ds(chunk * nb, nb)
        return pltpu.make_async_remote_copy(
            src_ref=ctx_send.at[bs, to],
            dst_ref=relay.at[bs, slot],
            send_sem=ctx_send_sem.at[chunk],
            recv_sem=relay_recv_sem.at[chunk],
            device_id={"sp": to - FIRST},
            device_id_type=pl.DeviceIdType.MESH,
        )

    def forward(chunk, slot):
        bs = pl.ds(chunk * nb, nb)
        return pltpu.make_async_remote_copy(
            src_ref=relay.at[bs, slot],
            dst_ref=rows_of(chunk, 2 * FIRST + slot),
            send_sem=relay_send_sem.at[chunk],
            recv_sem=ctx_recv_sem.at[chunk, 2],
            device_id={"sp": me + FIRST},
            device_id_type=pl.DeviceIdType.MESH,
        )

    def put_near(chunk, kind):
        bs = pl.ds(chunk * nb, nb)
        return pltpu.make_async_remote_copy(
            src_ref=send.at[kind, bs, pl.ds((1 - me) * dests, dests)],
            dst_ref=near.at[kind, bs],
            send_sem=near_send_sem.at[chunk],
            recv_sem=near_recv_sem.at[chunk],
            device_id={"sp": 1 - me},
            device_id_type=pl.DeviceIdType.MESH,
        )

    def put_ctx_near(chunk):
        bs = pl.ds(chunk * nb, nb)
        return pltpu.make_async_remote_copy(
            src_ref=ctx_near.at[bs, 1 - me],
            dst_ref=rows_of(chunk, me * dests, dests),
            send_sem=ctx_near_send_sem.at[chunk],
            recv_sem=ctx_near_recv_sem.at[chunk],
            device_id={"sp": 1 - me},
            device_id_type=pl.DeviceIdType.MESH,
        )

    def drain(ref, sem):
        pltpu.make_async_copy(ref, ref, sem).wait()

    is_first = me < FIRST
    later_on = jnp.logical_not(is_first)

    def each_peer(do, lowest=0):
        for other in range(lowest, n):
            pl.when(other != me)(functools.partial(do, other))

    def qkv_phase(x_buf, h_attn, w_nat, w_cols, out_buf, own, cos_ref, sin_ref):
        mine = pl.ds(pl.multiple_of(me * seq_dev, seq_dev), seq_dev)
        get_cos = pltpu.make_async_copy(cos_hbm.at[mine], cos_ref, own_sem.at[3])
        get_sin = pltpu.make_async_copy(sin_hbm.at[mine], sin_ref, own_sem.at[4])

        def get_x(chunk):
            return pltpu.make_async_copy(x_hbm.at[pl.ds(chunk * rows, rows)], x_buf, x_sem)

        def get_w(half):
            block, slot = half // 2, lax.rem(half, 2)
            src = w_qkv.at[
                pl.ds(slot * (width // 2), width // 2),
                block // parts,
                pl.ds(lax.rem(block, parts) * QKV_HEADS, QKV_HEADS),
            ]
            return pltpu.make_async_copy(src, w_nat.at[slot], w_sem.at[slot])

        def bounce(step):
            slot, block = lax.rem(step, 2), lax.rem(step, blocks)
            dst = send.at[
                block // parts, pl.ds(step // blocks * nb, nb), pl.ds(lax.rem(block, parts) * dests, dests)
            ]
            return pltpu.make_async_copy(out_buf.at[slot], dst, bounce_sem.at[slot])

        def put_own(chunk, kind):
            dst = recv.at[kind, pl.ds(chunk * nb, nb), :, me]
            return pltpu.make_async_copy(own.at[kind], dst, own_sem.at[kind])

        def send_block(step):
            bounce(step).wait()
            block = lax.rem(step, blocks)
            for d in range(dests):
                to = lax.rem(block, parts) * dests + lax.rem(me + d, dests)

                @pl.when((to != me) & jnp.logical_not(is_first & (block < parts)))
                def _():
                    put(step // blocks, block // parts, to, me).start()

            @pl.when(is_first & (lax.rem(block, parts) == 1 - me))
            def _():
                put_near(step // blocks, block // parts).start()

        ln_hbm = (ln_aw_hbm, ln_ab_hbm, ln_mw_hbm, ln_mb_hbm)
        get_ln = [pltpu.make_async_copy(p, ln_buf.at[i], ln_sem.at[i]) for i, p in enumerate(ln_hbm)]
        ln_aw, ln_ab, ln_mw, ln_mb = (ln_buf.at[i] for i in range(4))
        get_x(0).start()
        for copy in get_ln:
            copy.start()
        get_w(0).start()
        get_w(1).start()
        get_cos.start()
        get_sin.start()
        barrier = pltpu.get_barrier_semaphore()
        for step in range(1, n):
            pl.semaphore_signal(
                barrier, inc=1, device_id={"sp": peer(step)}, device_id_type=pl.DeviceIdType.MESH
            )

        @pl.loop(0, N_CHUNKS * blocks)
        def _(step):
            chunk, block = step // blocks, lax.rem(step, blocks)
            kind, part = block // parts, lax.rem(block, parts)
            slot = lax.rem(step, 2)

            @pl.when(block == 0)
            def _():
                get_x(chunk).wait()

                @pl.when(chunk == 0)
                def _():
                    for copy in get_ln:
                        copy.wait()

                @pl.loop(0, nb)
                def _(i):
                    r = pl.ds(pl.multiple_of(i * seq_dev, seq_dev), seq_dev)
                    g = pl.ds(pl.multiple_of(chunk * rows + i * seq_dev, seq_dev), seq_dev)
                    xf = x_buf[r, :].astype(F32)
                    mean = jnp.sum(xf, axis=-1, keepdims=True) * (1.0 / width)
                    dev = xf - mean
                    var = jnp.sum(dev * dev, axis=-1, keepdims=True) * (1.0 / width)
                    unit = dev * lax.rsqrt(var + LN_EPS)
                    h_attn[r, :] = (unit * ln_aw[...] + ln_ab[...]).astype(BF16)
                    h_mlp[g, :] = (unit * ln_mw[...] + ln_mb[...]).astype(BF16)
                    acc[g, :] = xf

                @pl.when(chunk + 1 < N_CHUNKS)
                def _():
                    get_x(chunk + 1).start()

            @pl.when(chunk == 0)
            def _():
                @pl.when(block == 0)
                def _():
                    get_cos.wait()
                    get_sin.wait()

                @pl.loop(2 * block, 2 * block + 2)
                def _(half):
                    get_w(half).wait()

                    @pl.loop(0, width // 2 // 128)
                    def _(i):
                        r = pl.ds(pl.multiple_of(i * 128, 128), 128)
                        top = lax.rem(half, 2) * (width // 2)
                        to = pl.ds(pl.multiple_of(top + i * 128, 128), 128)
                        by_head = jnp.swapaxes(w_nat[lax.rem(half, 2), r].astype(F32), 0, 1)
                        for h in range(QKV_HEADS):
                            w_cols[block, to, h * head_dim : (h + 1) * head_dim] = by_head[h].astype(BF16)

                    @pl.when(half + 2 < 2 * blocks)
                    def _():
                        get_w(half + 2).start()

            for d in range(dests):
                cs = slice(d * heads * head_dim, (d + 1) * heads * head_dim)
                cols = jnp.dot(h_attn[...], w_cols[block, :, cs], preferred_element_type=F32)
                for h in range(heads):
                    for b in range(nb):
                        u = cols[b * seq_dev : (b + 1) * seq_dev, h * head_dim : (h + 1) * head_dim]
                        u = u.astype(BF16).astype(F32)
                        turned = u * cos_ref[...] + pltpu.roll(u, head_dim // 2, 1) * sin_ref[...]
                        out_buf[slot, b, d, h] = jnp.where(kind < 2, turned, u).astype(BF16)

            bounce(step).start()

            @pl.when(me // dests == part)
            def _():
                @pl.when(chunk > 0)
                def _():
                    put_own(chunk - 1, kind).wait()

                own[kind] = out_buf[slot, :, lax.rem(me, dests)]
                put_own(chunk, kind).start()

            @pl.when(step == 0)
            def _():
                pl.semaphore_wait(barrier, n - 1)

            @pl.when(chunk == 0)
            def _():
                send_block(step)

            @pl.when(step > blocks)
            def _():
                send_block(step - 1)

        send_block(N_CHUNKS * blocks - 1)
        for kind in range(3):
            put_own(N_CHUNKS - 1, kind).wait()

    pl.run_scoped(
        qkv_phase,
        pltpu.VMEM((rows, width), BF16),
        pltpu.VMEM((rows, width), BF16),
        pltpu.VMEM((2, width // 2, QKV_HEADS, head_dim), BF16),
        pltpu.VMEM((blocks, width, QKV_HEADS * head_dim), BF16),
        pltpu.VMEM((2, nb, dests, heads, seq_dev, head_dim), BF16),
        pltpu.VMEM((3, nb, heads, seq_dev, head_dim), BF16),
        pltpu.VMEM((seq_dev, head_dim), F32),
        pltpu.VMEM((seq_dev, head_dim), F32),
    )

    def rest(up_buf, down_buf, w_buf, qkv_buf, ctx_buf, both, near_buf):
        later = n - FIRST
        steps = ffn // UP_TILE

        def get_up(f):
            cols = pl.ds(pl.multiple_of(f * UP_TILE, UP_TILE), UP_TILE)
            slot = lax.rem(f, 2)
            return pltpu.make_async_copy(w_up.at[:, cols], up_buf.at[slot], up_sem.at[slot])

        def get_down(f):
            cols = pl.ds(pl.multiple_of(f * UP_TILE, UP_TILE), UP_TILE)
            slot = lax.rem(f, 2)
            return pltpu.make_async_copy(w_down.at[cols], down_buf.at[slot], down_sem.at[slot])

        def get_w_out():
            return pltpu.make_async_copy(w_out, w_buf, w_sem.at[0])

        def get_qkv(chunk, kind):
            return pltpu.make_async_copy(recv.at[kind, pl.ds(chunk * nb, nb)], qkv_buf.at[kind], qkv_sem.at[kind])

        def get_own_near(chunk, kind):
            src = send.at[kind, pl.ds(chunk * nb, nb), pl.ds(me * dests, dests)]
            return pltpu.make_async_copy(src, both.at[kind, :, :, :, me], near_sem.at[kind, 0])

        def get_other_near(chunk, kind):
            src = near.at[kind, pl.ds(chunk * nb, nb)]
            return pltpu.make_async_copy(src, both.at[kind, :, :, :, 1 - me], near_sem.at[kind, 1])

        def bounce_ctx(chunk):
            dst = ctx_send.at[pl.ds(chunk * nb, nb), pl.ds(FIRST, later)]
            return pltpu.make_async_copy(ctx_buf, dst, bounce_sem.at[0])

        def bounce_near(chunk):
            return pltpu.make_async_copy(near_buf, ctx_near.at[pl.ds(chunk * nb, nb)], bounce_sem.at[1])

        def send_ctx(chunk):
            bounce_ctx(chunk).wait()
            relays = (me // FIRST == 2) & (chunk < RELAYED)

            def one(other):
                if other // FIRST == 1:

                    @pl.when(relays)
                    def _():
                        put_relay(chunk, other, me - 2 * FIRST).start()

                    @pl.when(jnp.logical_not(relays))
                    def _():
                        put_ctx(chunk, other, me).start()

                else:
                    put_ctx(chunk, other, me).start()

            each_peer(one, FIRST)

        def send_near(chunk):
            bounce_near(chunk).wait()
            put_ctx_near(chunk).start()

        def pass_on(chunk):
            drain(relay.at[pl.ds(chunk * nb, nb)], relay_recv_sem.at[chunk])
            for slot in range(FIRST):
                forward(chunk, slot).start()

        def load_qkv(chunk):
            for kind in range(3):
                got = lambda count: recv.at[kind, pl.ds(chunk * nb, nb), :, pl.ds(0, count)]
                if kind:
                    drain(got(n - 1), recv_sem.at[chunk, kind])
                else:
                    pl.when(is_first)(lambda: drain(got(n - FIRST), recv_sem.at[chunk, kind]))
                    pl.when(later_on)(lambda: drain(got(n - FIRST - 1), recv_sem.at[chunk, kind]))
                get_qkv(chunk, kind).start()

            @pl.when(is_first)
            def _():
                drain(near.at[:, pl.ds(chunk * nb, nb)], near_recv_sem.at[chunk])
                for kind in range(3):
                    get_own_near(chunk, kind).start()
                    get_other_near(chunk, kind).start()

        get_up(0).start()
        get_down(0).start()
        get_w_out().start()

        @pl.loop(0, N_CHUNKS + 1)
        def _(chunk):
            early = steps - LATE_STEPS
            first = chunk * early // N_CHUNKS
            last = jnp.where(chunk < N_CHUNKS, (chunk + 1) * early // N_CHUNKS, steps)

            @pl.loop(first, last)
            def _(f):
                slot = lax.rem(f, 2)

                @pl.when(f + 1 < steps)
                def _():
                    get_up(f + 1).start()
                    get_down(f + 1).start()

                @pl.when((f == last - 1) & (chunk < N_CHUNKS - 1))
                def _():
                    load_qkv(chunk)

                get_up(f).wait()
                get_down(f).wait()
                for r in range(n_batch * seq_dev // 512):
                    rs = pl.ds(r * 512, 512)
                    up = jnp.dot(h_mlp[rs, :], up_buf[slot], preferred_element_type=F32)
                    hid = (0.5 * up * (1.0 + lax.erf(up * 0.5**0.5))).astype(BF16)
                    acc[rs, :] += jnp.dot(hid, down_buf[slot], preferred_element_type=F32)

                @pl.when((f == first) & (chunk > 0))
                def _():
                    @pl.when(chunk < N_CHUNKS)
                    def _():
                        send_ctx(chunk - 1)

                    @pl.when(is_first)
                    def _():
                        send_near(chunk - 1)

                @pl.when(is_first & (chunk == N_CHUNKS))
                def _():
                    first_relay = 1 + (f - first) * 2

                    @pl.loop(first_relay, jnp.minimum(jnp.where(f == steps - 1, RELAYED, first_relay + 2), RELAYED))
                    def _(c):
                        pass_on(c)

            @pl.when(chunk < N_CHUNKS)
            def _():
                @pl.when(chunk == N_CHUNKS - 1)
                def _():
                    load_qkv(chunk)

                for kind in range(3):
                    get_qkv(chunk, kind).wait()
                for b in range(nb):
                    for h in range(heads):
                        q = qkv_buf[0, b, h, FIRST:].reshape(later * seq_dev, head_dim)
                        k, v = (qkv_buf[t, b, h].reshape(n * seq_dev, head_dim) for t in (1, 2))
                        per = Q_TILE // seq_dev

                        def write(i, out):
                            ctx_buf[b, i * per : (i + 1) * per, :, h * head_dim : (h + 1) * head_dim] = out.reshape(
                                per, seq_dev, head_dim
                            )

                        causal_head(q, k, v, write)
                bounce_ctx(chunk).start()

                @pl.when(later_on)
                def _():
                    rows_of(chunk, me)[...] = ctx_buf[:, me - FIRST]

                @pl.when(chunk == N_CHUNKS - 1)
                def _():
                    send_ctx(chunk)

                    @pl.when(is_first)
                    def _():
                        pass_on(0)

                @pl.when(is_first)
                def _():
                    for kind in range(3):
                        get_own_near(chunk, kind).wait()
                        get_other_near(chunk, kind).wait()

                    @pl.loop(0, nb)
                    def _(b):
                        for d in range(dests):
                            for h in range(heads):
                                q, k, v = (both[t, b, d, h].reshape(Q_TILE, head_dim) for t in range(3))

                                def write(i, out):
                                    col = (d * heads + h) * head_dim
                                    near_buf[b, :, :, col : col + head_dim] = out.reshape(
                                        FIRST, seq_dev, head_dim
                                    )

                                causal_head(q, k, v, write)

                    bounce_near(chunk).start()
                    rows_of(chunk, me * dests, dests)[...] = near_buf[:, me]

        get_w_out().wait()

        @pl.loop(0, N_CHUNKS)
        def _(turn):
            chunk = jnp.where(turn == 2, RELAYED, jnp.where((turn > 2) & (turn <= RELAYED), turn - 1, turn))

            g = pl.ds(pl.multiple_of(chunk * rows, rows), rows)
            pl.when(is_first)(lambda: put_ctx_near(chunk).wait_recv())
            for part in range(n // FIRST):
                home = me // FIRST
                source = jnp.where(part == 0, home, jnp.where(part <= home, part - 1, part))

                @pl.when(later_on)
                def _():
                    count = FIRST - (part == 0)
                    drain(rows_of(chunk, 0, count), ctx_recv_sem.at[chunk, source])

                span = pl.ds(pl.multiple_of(source * FIRST * cols, FIRST * cols), FIRST * cols)
                left = ctx_rows[pl.ds(chunk * nb, nb), :, span].reshape(rows, FIRST * cols)
                for c in range(0, width, 1024):
                    cs = slice(c, c + 1024)
                    total = acc[g, cs] + jnp.dot(left, w_buf[span, cs], preferred_element_type=F32)
                    if part < n // FIRST - 1:
                        acc[g, cs] = total
                    else:
                        h_mlp[g, cs] = total.astype(BF16)

    pl.run_scoped(
        rest,
        pltpu.VMEM((2, width, UP_TILE), BF16),
        pltpu.VMEM((2, UP_TILE, width), BF16),
        pltpu.VMEM((width, width), BF16),
        pltpu.VMEM((3, nb, heads, n, seq_dev, head_dim), BF16),
        pltpu.VMEM((nb, n - FIRST, seq_dev, cols), BF16),
        pltpu.VMEM((3, nb, dests, heads, FIRST, seq_dev, head_dim), BF16),
        pltpu.VMEM((nb, FIRST, seq_dev, dests * cols), BF16),
    )

    @pl.loop(0, N_CHUNKS)
    def _(chunk):
        bs = pl.ds(chunk * nb, nb)

        @pl.when(is_first)
        def _():
            drain(send.at[pl.ds(1, 2), bs, pl.ds(0, n - 1)], send_sem.at[chunk])
            drain(near.at[:, bs], near_send_sem.at[chunk])
            drain(ctx_send.at[bs, pl.ds(0, n - FIRST)], ctx_send_sem.at[chunk])
            drain(ctx_near.at[bs, 0], ctx_near_send_sem.at[chunk])
            pl.when(chunk < RELAYED)(lambda: drain(relay.at[bs], relay_send_sem.at[chunk]))

        @pl.when(later_on)
        def _():
            drain(send.at[:, bs, pl.ds(0, n - 1)], send_sem.at[chunk])
            drain(ctx_send.at[bs, pl.ds(0, n - FIRST - 1)], ctx_send_sem.at[chunk])


def store_kernel(y_ref, kv_hbm, y_hbm, k_hbm, v_hbm, buf, in_sem, out_sem, y_sem):
    n_batch = k_hbm.shape[0]
    y_out = pltpu.make_async_copy(y_ref, y_hbm, y_sem)
    pieces = [(t, b) for t in range(2) for b in range(n_batch)]
    get = [
        pltpu.make_async_copy(kv_hbm.at[1 + t, b], buf.at[t, b], in_sem.at[t, b]) for t, b in pieces
    ]
    put = [
        pltpu.make_async_copy(buf.at[t, b], (k_hbm, v_hbm)[t].at[b], out_sem.at[t, b]) for t, b in pieces
    ]
    for copy in get:
        copy.start()
    y_out.start()
    for got, going in zip(get, put):
        got.wait()
        going.start()
    for copy in put:
        copy.wait()
    y_out.wait()


def solution(mesh):
    n = mesh.shape["sp"]

    def local_layer(x_blk, ln_attn_w, ln_attn_b, ln_mlp_w, ln_mlp_b, w_qkv, w_out, w_up, w_down):
        n_batch, seq_dev, width = x_blk.shape
        groups, head_dim = w_qkv.shape[1], w_qkv.shape[3]
        heads = groups // n
        nb = n_batch // N_CHUNKS
        rows = n_batch * seq_dev
        dests = QKV_HEADS // heads
        ffn = w_up.shape[1]
        cos_t, sin_t = rope_tables(n * seq_dev, head_dim)
        row = lambda p: p.reshape(1, width)
        anywhere = pl.BlockSpec(memory_space=pl.ANY)
        flops = 2 * rows * width * (3 * width + 2 * ffn) + 2 * rows * n * seq_dev * width * 2
        y_out, recv, *_ = pl.pallas_call(
            functools.partial(layer_kernel, n),
            out_shape=[
                pltpu.VMEM((rows, width), BF16),
                jax.ShapeDtypeStruct((3, n_batch, heads, n, seq_dev, head_dim), BF16),
                jax.ShapeDtypeStruct((3, n_batch, n, heads, seq_dev, head_dim), BF16),
                jax.ShapeDtypeStruct((n_batch, n, seq_dev, heads * head_dim), BF16),
                jax.ShapeDtypeStruct((3, n_batch, dests, heads, seq_dev, head_dim), BF16),
                jax.ShapeDtypeStruct((n_batch, FIRST, seq_dev, dests * heads * head_dim), BF16),
                jax.ShapeDtypeStruct((n_batch, FIRST, seq_dev, heads * head_dim), BF16),
            ],
            in_specs=[anywhere] * 11,
            out_specs=[pl.BlockSpec(memory_space=pltpu.VMEM)] + [anywhere] * 6,
            scratch_shapes=[
                pltpu.VMEM((rows, width), F32),
                pltpu.VMEM((n_batch, seq_dev, width), BF16),
                pltpu.VMEM((4, 1, width), F32),
                pltpu.SemaphoreType.DMA,
                pltpu.SemaphoreType.DMA((4,)),
                pltpu.SemaphoreType.DMA((2,)),
                pltpu.SemaphoreType.DMA((2,)),
                pltpu.SemaphoreType.DMA((5,)),
                pltpu.SemaphoreType.DMA((2,)),
                pltpu.SemaphoreType.DMA((2,)),
                pltpu.SemaphoreType.DMA((3,)),
                pltpu.SemaphoreType.DMA((3, 2)),
                pltpu.SemaphoreType.DMA((N_CHUNKS,)),
                pltpu.SemaphoreType.DMA((N_CHUNKS, 3)),
                pltpu.SemaphoreType.DMA((N_CHUNKS,)),
                pltpu.SemaphoreType.DMA((N_CHUNKS, n // FIRST)),
                pltpu.SemaphoreType.DMA((N_CHUNKS,)),
                pltpu.SemaphoreType.DMA((N_CHUNKS,)),
                pltpu.SemaphoreType.DMA((N_CHUNKS,)),
                pltpu.SemaphoreType.DMA((N_CHUNKS,)),
                pltpu.SemaphoreType.DMA((N_CHUNKS,)),
                pltpu.SemaphoreType.DMA((N_CHUNKS,)),
            ],
            compiler_params=pltpu.CompilerParams(
                collective_id=0, has_side_effects=True, vmem_limit_bytes=57 * 2**20
            ),
            cost_estimate=pl.CostEstimate(flops=flops, bytes_accessed=3 * 10**8, transcendentals=10**7),
            name="layer",
        )(
            x_blk.reshape(rows, width),
            cos_t,
            sin_t,
            row(ln_attn_w),
            row(ln_attn_b),
            row(ln_mlp_w),
            row(ln_mlp_b),
            w_qkv.transpose(0, 2, 1, 3),
            w_out,
            w_up,
            w_down,
        )
        cache = jax.ShapeDtypeStruct((n_batch, heads, n, seq_dev, head_dim), BF16)
        y_out, k_cache, v_cache = pl.pallas_call(
            store_kernel,
            out_shape=[jax.ShapeDtypeStruct((rows, width), BF16), cache, cache],
            in_specs=[pl.BlockSpec(memory_space=pltpu.VMEM), pl.BlockSpec(memory_space=pltpu.HBM)],
            out_specs=[pl.BlockSpec(memory_space=pltpu.HBM)] * 3,
            scratch_shapes=[
                pltpu.VMEM((2, n_batch, heads, n, seq_dev, head_dim), BF16),
                pltpu.SemaphoreType.DMA((2, n_batch)),
                pltpu.SemaphoreType.DMA((2, n_batch)),
                pltpu.SemaphoreType.DMA,
            ],
            compiler_params=pltpu.CompilerParams(vmem_limit_bytes=56 * 2**20),
            cost_estimate=pl.CostEstimate(flops=10**6, bytes_accessed=3 * 10**7, transcendentals=0),
            name="store",
        )(y_out, recv)
        shape = (n_batch, heads, n * seq_dev, head_dim)
        return y_out.reshape(x_blk.shape), k_cache.reshape(shape), v_cache.reshape(shape)

    act_spec, cache_spec = P("dp", "sp", None), P("dp", "sp", None, None)
    return jax.shard_map(
        local_layer,
        mesh=mesh,
        in_specs=(act_spec,) + (P(),) * 8,
        out_specs=(act_spec, cache_spec, cache_spec),
        check_vma=False,
    )
```

```python
import functools

import jax
import jax.numpy as jnp
import numpy as np
from jax import lax
from jax.experimental import pallas as pl
from jax.experimental.pallas import tpu as pltpu
from jax.sharding import PartitionSpec as P

LN_EPS = 1e-5
ROPE_BASE = 10000.0
LOG2E = 1.4426950408889634
N_CHUNKS = 6
UP_TILE = 512
QKV_HEADS = 8
Q_TILE = 256
FIRST = 2
LATE_STEPS = 2
RELAYED = 4
F32 = jnp.float32
BF16 = jnp.bfloat16


def rope_tables(positions, head_dim):
    half_dim = head_dim // 2
    inv_freq = np.float32(ROPE_BASE) ** (np.float32(-2.0) * np.arange(half_dim, dtype=np.float32) / np.float32(head_dim))
    angles = np.arange(positions, dtype=np.float32)[:, None] * inv_freq[None, :]
    cos_t, sin_t = np.cos(angles.astype(np.float64)), np.sin(angles.astype(np.float64))
    wide = lambda a, b: jnp.asarray(np.concatenate([a, b], -1).astype(np.float32))
    return wide(cos_t, cos_t), wide(-sin_t, sin_t)


def causal_head(q, k, v, write):
    seq, head_dim = k.shape
    scale = LOG2E * head_dim**-0.5
    keys = lax.broadcasted_iota(jnp.int32, (Q_TILE, Q_TILE), 0)
    queries = lax.broadcasted_iota(jnp.int32, (Q_TILE, Q_TILE), 1)
    for i in range(q.shape[0] // Q_TILE):
        lo = seq - q.shape[0] + i * Q_TILE
        hi = lo + Q_TILE
        q_i = q[i * Q_TILE : (i + 1) * Q_TILE]
        scores = lax.dot_general(k[:hi], q_i, (((1,), (1,)), ((), ())), preferred_element_type=F32)
        diag = jnp.where(keys <= queries, scores[lo:], -1e30)
        scores = jnp.concatenate([scores[:lo], diag], axis=0) if lo else diag
        prob = jnp.exp2((scores - jnp.max(scores, axis=0, keepdims=True)) * scale)
        prob = (prob * (1.0 / jnp.sum(prob, axis=0, keepdims=True))).astype(BF16)
        out = lax.dot_general(prob, v[:hi], (((0,), (0,)), ((), ())), preferred_element_type=F32)
        write(i, out.astype(BF16))


def layer_kernel(
    n,
    x_hbm,
    cos_hbm,
    sin_hbm,
    ln_aw_hbm,
    ln_ab_hbm,
    ln_mw_hbm,
    ln_mb_hbm,
    w_qkv,
    w_out,
    w_up,
    w_down,
    h_mlp,
    recv,
    send,
    ctx_send,
    near,
    ctx_near,
    relay,
    acc,
    ctx_rows,
    ln_buf,
    x_sem,
    ln_sem,
    w_sem,
    bounce_sem,
    own_sem,
    up_sem,
    down_sem,
    qkv_sem,
    near_sem,
    send_sem,
    recv_sem,
    ctx_send_sem,
    ctx_recv_sem,
    near_send_sem,
    near_recv_sem,
    ctx_near_send_sem,
    ctx_near_recv_sem,
    relay_recv_sem,
    relay_send_sem,
):
    me = lax.axis_index("sp")
    n_batch, _, heads, seq_dev, head_dim = send.shape[1:]
    cols = heads * head_dim
    width = x_hbm.shape[1]
    nb = n_batch // N_CHUNKS
    rows = nb * seq_dev
    ffn = w_up.shape[1]
    dests = QKV_HEADS // heads
    parts = n // dests
    blocks = 3 * parts

    def peer(step):
        return lax.bitwise_xor(me, step)

    def rows_of(chunk, first, count=1):
        return ctx_rows.at[pl.ds(chunk * nb, nb), :, pl.ds(pl.multiple_of(first * cols, cols), count * cols)]

    def put(chunk, kind, to, frm):
        bs = pl.ds(chunk * nb, nb)
        return pltpu.make_async_remote_copy(
            src_ref=send.at[kind, bs, to],
            dst_ref=recv.at[kind, bs, :, frm],
            send_sem=send_sem.at[chunk],
            recv_sem=recv_sem.at[chunk, kind],
            device_id={"sp": to},
            device_id_type=pl.DeviceIdType.MESH,
        )

    def put_ctx(chunk, to, frm):
        bs = pl.ds(chunk * nb, nb)
        return pltpu.make_async_remote_copy(
            src_ref=ctx_send.at[bs, to],
            dst_ref=rows_of(chunk, frm),
            send_sem=ctx_send_sem.at[chunk],
            recv_sem=ctx_recv_sem.at[chunk, frm // FIRST],
            device_id={"sp": to},
            device_id_type=pl.DeviceIdType.MESH,
        )

    def put_relay(chunk, to, slot):
        bs = pl.ds(chunk * nb, nb)
        return pltpu.make_async_remote_copy(
            src_ref=ctx_send.at[bs, to],
            dst_ref=relay.at[bs, slot],
            send_sem=ctx_send_sem.at[chunk],
            recv_sem=relay_recv_sem.at[chunk],
            device_id={"sp": to - FIRST},
            device_id_type=pl.DeviceIdType.MESH,
        )

    def forward(chunk, slot):
        bs = pl.ds(chunk * nb, nb)
        return pltpu.make_async_remote_copy(
            src_ref=relay.at[bs, slot],
            dst_ref=rows_of(chunk, 2 * FIRST + slot),
            send_sem=relay_send_sem.at[chunk],
            recv_sem=ctx_recv_sem.at[chunk, 2],
            device_id={"sp": me + FIRST},
            device_id_type=pl.DeviceIdType.MESH,
        )

    def put_near(chunk, kind):
        bs = pl.ds(chunk * nb, nb)
        return pltpu.make_async_remote_copy(
            src_ref=send.at[kind, bs, pl.ds((1 - me) * dests, dests)],
            dst_ref=near.at[kind, bs],
            send_sem=near_send_sem.at[chunk],
            recv_sem=near_recv_sem.at[chunk],
            device_id={"sp": 1 - me},
            device_id_type=pl.DeviceIdType.MESH,
        )

    def put_ctx_near(chunk):
        bs = pl.ds(chunk * nb, nb)
        return pltpu.make_async_remote_copy(
            src_ref=ctx_near.at[bs, 1 - me],
            dst_ref=rows_of(chunk, me * dests, dests),
            send_sem=ctx_near_send_sem.at[chunk],
            recv_sem=ctx_near_recv_sem.at[chunk],
            device_id={"sp": 1 - me},
            device_id_type=pl.DeviceIdType.MESH,
        )

    def drain(ref, sem):
        pltpu.make_async_copy(ref, ref, sem).wait()

    is_first = me < FIRST
    later_on = jnp.logical_not(is_first)

    def each_peer(do, lowest=0):
        for other in range(lowest, n):
            pl.when(other != me)(functools.partial(do, other))

    def qkv_phase(x_buf, h_attn, w_nat, w_cols, out_buf, own, cos_ref, sin_ref):
        mine = pl.ds(pl.multiple_of(me * seq_dev, seq_dev), seq_dev)
        get_cos = pltpu.make_async_copy(cos_hbm.at[mine], cos_ref, own_sem.at[3])
        get_sin = pltpu.make_async_copy(sin_hbm.at[mine], sin_ref, own_sem.at[4])

        def get_x(chunk):
            return pltpu.make_async_copy(x_hbm.at[pl.ds(chunk * rows, rows)], x_buf, x_sem)

        def get_w(half):
            block, slot = half // 2, lax.rem(half, 2)
            src = w_qkv.at[
                pl.ds(slot * (width // 2), width // 2),
                block // parts,
                pl.ds(lax.rem(block, parts) * QKV_HEADS, QKV_HEADS),
            ]
            return pltpu.make_async_copy(src, w_nat.at[slot], w_sem.at[slot])

        def bounce(step):
            slot, block = lax.rem(step, 2), lax.rem(step, blocks)
            dst = send.at[
                block // parts, pl.ds(step // blocks * nb, nb), pl.ds(lax.rem(block, parts) * dests, dests)
            ]
            return pltpu.make_async_copy(out_buf.at[slot], dst, bounce_sem.at[slot])

        def put_own(chunk, kind):
            dst = recv.at[kind, pl.ds(chunk * nb, nb), :, me]
            return pltpu.make_async_copy(own.at[kind], dst, own_sem.at[kind])

        def send_block(step):
            bounce(step).wait()
            block = lax.rem(step, blocks)
            for d in range(dests):
                to = lax.rem(block, parts) * dests + lax.rem(me + d, dests)

                @pl.when((to != me) & jnp.logical_not(is_first & (block < parts)))
                def _():
                    put(step // blocks, block // parts, to, me).start()

            @pl.when(is_first & (lax.rem(block, parts) == 1 - me))
            def _():
                put_near(step // blocks, block // parts).start()

        ln_hbm = (ln_aw_hbm, ln_ab_hbm, ln_mw_hbm, ln_mb_hbm)
        get_ln = [pltpu.make_async_copy(p, ln_buf.at[i], ln_sem.at[i]) for i, p in enumerate(ln_hbm)]
        ln_aw, ln_ab, ln_mw, ln_mb = (ln_buf.at[i] for i in range(4))
        get_x(0).start()
        for copy in get_ln:
            copy.start()
        get_w(0).start()
        get_w(1).start()
        get_cos.start()
        get_sin.start()
        barrier = pltpu.get_barrier_semaphore()
        for step in range(1, n):
            pl.semaphore_signal(
                barrier, inc=1, device_id={"sp": peer(step)}, device_id_type=pl.DeviceIdType.MESH
            )

        @pl.loop(0, N_CHUNKS * blocks)
        def _(step):
            chunk, block = step // blocks, lax.rem(step, blocks)
            kind, part = block // parts, lax.rem(block, parts)
            slot = lax.rem(step, 2)

            @pl.when(block == 0)
            def _():
                get_x(chunk).wait()

                @pl.when(chunk == 0)
                def _():
                    for copy in get_ln:
                        copy.wait()

                @pl.loop(0, nb)
                def _(i):
                    r = pl.ds(pl.multiple_of(i * seq_dev, seq_dev), seq_dev)
                    g = pl.ds(pl.multiple_of(chunk * rows + i * seq_dev, seq_dev), seq_dev)
                    xf = x_buf[r, :].astype(F32)
                    mean = jnp.sum(xf, axis=-1, keepdims=True) * (1.0 / width)
                    dev = xf - mean
                    var = jnp.sum(dev * dev, axis=-1, keepdims=True) * (1.0 / width)
                    unit = dev * lax.rsqrt(var + LN_EPS)
                    h_attn[r, :] = (unit * ln_aw[...] + ln_ab[...]).astype(BF16)
                    h_mlp[g, :] = (unit * ln_mw[...] + ln_mb[...]).astype(BF16)
                    acc[g, :] = xf

                @pl.when(chunk + 1 < N_CHUNKS)
                def _():
                    get_x(chunk + 1).start()

            @pl.when(chunk == 0)
            def _():
                @pl.when(block == 0)
                def _():
                    get_cos.wait()
                    get_sin.wait()

                @pl.loop(2 * block, 2 * block + 2)
                def _(half):
                    get_w(half).wait()

                    @pl.loop(0, width // 2 // 128)
                    def _(i):
                        r = pl.ds(pl.multiple_of(i * 128, 128), 128)
                        top = lax.rem(half, 2) * (width // 2)
                        to = pl.ds(pl.multiple_of(top + i * 128, 128), 128)
                        by_head = jnp.swapaxes(w_nat[lax.rem(half, 2), r].astype(F32), 0, 1)
                        for h in range(QKV_HEADS):
                            w_cols[block, to, h * head_dim : (h + 1) * head_dim] = by_head[h].astype(BF16)

                    @pl.when(half + 2 < 2 * blocks)
                    def _():
                        get_w(half + 2).start()

            for d in range(dests):
                cs = slice(d * heads * head_dim, (d + 1) * heads * head_dim)
                cols = jnp.dot(h_attn[...], w_cols[block, :, cs], preferred_element_type=F32)
                for h in range(heads):
                    for b in range(nb):
                        u = cols[b * seq_dev : (b + 1) * seq_dev, h * head_dim : (h + 1) * head_dim]
                        u = u.astype(BF16).astype(F32)
                        turned = u * cos_ref[...] + pltpu.roll(u, head_dim // 2, 1) * sin_ref[...]
                        out_buf[slot, b, d, h] = jnp.where(kind < 2, turned, u).astype(BF16)

            bounce(step).start()

            @pl.when(me // dests == part)
            def _():
                @pl.when(chunk > 0)
                def _():
                    put_own(chunk - 1, kind).wait()

                own[kind] = out_buf[slot, :, lax.rem(me, dests)]
                put_own(chunk, kind).start()

            @pl.when(step == 0)
            def _():
                pl.semaphore_wait(barrier, n - 1)

            @pl.when(chunk == 0)
            def _():
                send_block(step)

            @pl.when(step > blocks)
            def _():
                send_block(step - 1)

        send_block(N_CHUNKS * blocks - 1)
        for kind in range(3):
            put_own(N_CHUNKS - 1, kind).wait()

    pl.run_scoped(
        qkv_phase,
        pltpu.VMEM((rows, width), BF16),
        pltpu.VMEM((rows, width), BF16),
        pltpu.VMEM((2, width // 2, QKV_HEADS, head_dim), BF16),
        pltpu.VMEM((blocks, width, QKV_HEADS * head_dim), BF16),
        pltpu.VMEM((2, nb, dests, heads, seq_dev, head_dim), BF16),
        pltpu.VMEM((3, nb, heads, seq_dev, head_dim), BF16),
        pltpu.VMEM((seq_dev, head_dim), F32),
        pltpu.VMEM((seq_dev, head_dim), F32),
    )

    def rest(up_buf, down_buf, w_buf, qkv_buf, ctx_buf, both, near_buf):
        later = n - FIRST
        steps = ffn // UP_TILE

        def get_up(f):
            cols = pl.ds(pl.multiple_of(f * UP_TILE, UP_TILE), UP_TILE)
            slot = lax.rem(f, 2)
            return pltpu.make_async_copy(w_up.at[:, cols], up_buf.at[slot], up_sem.at[slot])

        def get_down(f):
            cols = pl.ds(pl.multiple_of(f * UP_TILE, UP_TILE), UP_TILE)
            slot = lax.rem(f, 2)
            return pltpu.make_async_copy(w_down.at[cols], down_buf.at[slot], down_sem.at[slot])

        def get_w_out():
            return pltpu.make_async_copy(w_out, w_buf, w_sem.at[0])

        def get_qkv(chunk, kind):
            return pltpu.make_async_copy(recv.at[kind, pl.ds(chunk * nb, nb)], qkv_buf.at[kind], qkv_sem.at[kind])

        def get_own_near(chunk, kind):
            src = send.at[kind, pl.ds(chunk * nb, nb), pl.ds(me * dests, dests)]
            return pltpu.make_async_copy(src, both.at[kind, :, :, :, me], near_sem.at[kind, 0])

        def get_other_near(chunk, kind):
            src = near.at[kind, pl.ds(chunk * nb, nb)]
            return pltpu.make_async_copy(src, both.at[kind, :, :, :, 1 - me], near_sem.at[kind, 1])

        def bounce_ctx(chunk):
            dst = ctx_send.at[pl.ds(chunk * nb, nb), pl.ds(FIRST, later)]
            return pltpu.make_async_copy(ctx_buf, dst, bounce_sem.at[0])

        def bounce_near(chunk):
            return pltpu.make_async_copy(near_buf, ctx_near.at[pl.ds(chunk * nb, nb)], bounce_sem.at[1])

        def send_ctx(chunk):
            bounce_ctx(chunk).wait()
            relays = (me // FIRST == 2) & (chunk < RELAYED)

            def one(other):
                if other // FIRST == 1:

                    @pl.when(relays)
                    def _():
                        put_relay(chunk, other, me - 2 * FIRST).start()

                    @pl.when(jnp.logical_not(relays))
                    def _():
                        put_ctx(chunk, other, me).start()

                else:
                    put_ctx(chunk, other, me).start()

            each_peer(one, FIRST)

        def send_near(chunk):
            bounce_near(chunk).wait()
            put_ctx_near(chunk).start()

        def pass_on(chunk):
            drain(relay.at[pl.ds(chunk * nb, nb)], relay_recv_sem.at[chunk])
            for slot in range(FIRST):
                forward(chunk, slot).start()

        def load_qkv(chunk):
            for kind in range(3):
                got = lambda count: recv.at[kind, pl.ds(chunk * nb, nb), :, pl.ds(0, count)]
                if kind:
                    drain(got(n - 1), recv_sem.at[chunk, kind])
                else:
                    pl.when(is_first)(lambda: drain(got(n - FIRST), recv_sem.at[chunk, kind]))
                    pl.when(later_on)(lambda: drain(got(n - FIRST - 1), recv_sem.at[chunk, kind]))
                get_qkv(chunk, kind).start()

            @pl.when(is_first)
            def _():
                drain(near.at[:, pl.ds(chunk * nb, nb)], near_recv_sem.at[chunk])
                for kind in range(3):
                    get_own_near(chunk, kind).start()
                    get_other_near(chunk, kind).start()

        get_up(0).start()
        get_down(0).start()
        get_w_out().start()

        @pl.loop(0, N_CHUNKS + 1)
        def _(chunk):
            early = steps - LATE_STEPS
            first = chunk * early // N_CHUNKS
            last = jnp.where(chunk < N_CHUNKS, (chunk + 1) * early // N_CHUNKS, steps)

            @pl.loop(first, last)
            def _(f):
                slot = lax.rem(f, 2)

                @pl.when(f + 1 < steps)
                def _():
                    get_up(f + 1).start()
                    get_down(f + 1).start()

                @pl.when((f == last - 1) & (chunk < N_CHUNKS - 1))
                def _():
                    load_qkv(chunk)

                get_up(f).wait()
                get_down(f).wait()
                for r in range(n_batch * seq_dev // 512):
                    rs = pl.ds(r * 512, 512)
                    up = jnp.dot(h_mlp[rs, :], up_buf[slot], preferred_element_type=F32)
                    hid = (0.5 * up * (1.0 + lax.erf(up * 0.5**0.5))).astype(BF16)
                    acc[rs, :] += jnp.dot(hid, down_buf[slot], preferred_element_type=F32)

                @pl.when((f == first) & (chunk > 0))
                def _():
                    @pl.when(chunk < N_CHUNKS)
                    def _():
                        send_ctx(chunk - 1)

                    @pl.when(is_first)
                    def _():
                        send_near(chunk - 1)

                @pl.when(is_first & (chunk == N_CHUNKS))
                def _():
                    first_relay = 1 + (f - first) * 2

                    @pl.loop(first_relay, jnp.minimum(jnp.where(f == steps - 1, RELAYED, first_relay + 2), RELAYED))
                    def _(c):
                        pass_on(c)

            @pl.when(chunk < N_CHUNKS)
            def _():
                @pl.when(chunk == N_CHUNKS - 1)
                def _():
                    load_qkv(chunk)

                for kind in range(3):
                    get_qkv(chunk, kind).wait()
                for b in range(nb):
                    for h in range(heads):
                        q = qkv_buf[0, b, h, FIRST:].reshape(later * seq_dev, head_dim)
                        k, v = (qkv_buf[t, b, h].reshape(n * seq_dev, head_dim) for t in (1, 2))
                        per = Q_TILE // seq_dev

                        def write(i, out):
                            ctx_buf[b, i * per : (i + 1) * per, :, h * head_dim : (h + 1) * head_dim] = out.reshape(
                                per, seq_dev, head_dim
                            )

                        causal_head(q, k, v, write)
                bounce_ctx(chunk).start()

                @pl.when(later_on)
                def _():
                    rows_of(chunk, me)[...] = ctx_buf[:, me - FIRST]

                @pl.when(chunk == N_CHUNKS - 1)
                def _():
                    send_ctx(chunk)

                    @pl.when(is_first)
                    def _():
                        pass_on(0)

                @pl.when(is_first)
                def _():
                    for kind in range(3):
                        get_own_near(chunk, kind).wait()
                        get_other_near(chunk, kind).wait()

                    @pl.loop(0, nb)
                    def _(b):
                        for d in range(dests):
                            for h in range(heads):
                                q, k, v = (both[t, b, d, h].reshape(Q_TILE, head_dim) for t in range(3))

                                def write(i, out):
                                    col = (d * heads + h) * head_dim
                                    near_buf[b, :, :, col : col + head_dim] = out.reshape(
                                        FIRST, seq_dev, head_dim
                                    )

                                causal_head(q, k, v, write)

                    bounce_near(chunk).start()
                    rows_of(chunk, me * dests, dests)[...] = near_buf[:, me]

        get_w_out().wait()

        @pl.loop(0, N_CHUNKS)
        def _(turn):
            chunk = jnp.where(turn == 2, RELAYED, jnp.where((turn > 2) & (turn <= RELAYED), turn - 1, turn))

            g = pl.ds(pl.multiple_of(chunk * rows, rows), rows)
            pl.when(is_first)(lambda: put_ctx_near(chunk).wait_recv())
            for part in range(n // FIRST):
                home = me // FIRST
                source = jnp.where(part == 0, home, jnp.where(part <= home, part - 1, part))

                @pl.when(later_on)
                def _():
                    count = FIRST - (part == 0)
                    drain(rows_of(chunk, 0, count), ctx_recv_sem.at[chunk, source])

                span = pl.ds(pl.multiple_of(source * FIRST * cols, FIRST * cols), FIRST * cols)
                left = ctx_rows[pl.ds(chunk * nb, nb), :, span].reshape(rows, FIRST * cols)
                for c in range(0, width, 1024):
                    cs = slice(c, c + 1024)
                    total = acc[g, cs] + jnp.dot(left, w_buf[span, cs], preferred_element_type=F32)
                    if part < n // FIRST - 1:
                        acc[g, cs] = total
                    else:
                        h_mlp[g, cs] = total.astype(BF16)

    pl.run_scoped(
        rest,
        pltpu.VMEM((2, width, UP_TILE), BF16),
        pltpu.VMEM((2, UP_TILE, width), BF16),
        pltpu.VMEM((width, width), BF16),
        pltpu.VMEM((3, nb, heads, n, seq_dev, head_dim), BF16),
        pltpu.VMEM((nb, n - FIRST, seq_dev, cols), BF16),
        pltpu.VMEM((3, nb, dests, heads, FIRST, seq_dev, head_dim), BF16),
        pltpu.VMEM((nb, FIRST, seq_dev, dests * cols), BF16),
    )

    @pl.loop(0, N_CHUNKS)
    def _(chunk):
        bs = pl.ds(chunk * nb, nb)

        @pl.when(is_first)
        def _():
            drain(send.at[pl.ds(1, 2), bs, pl.ds(0, n - 1)], send_sem.at[chunk])
            drain(near.at[:, bs], near_send_sem.at[chunk])
            drain(ctx_send.at[bs, pl.ds(0, n - FIRST)], ctx_send_sem.at[chunk])
            drain(ctx_near.at[bs, 0], ctx_near_send_sem.at[chunk])
            pl.when(chunk < RELAYED)(lambda: drain(relay.at[bs], relay_send_sem.at[chunk]))

        @pl.when(later_on)
        def _():
            drain(send.at[:, bs, pl.ds(0, n - 1)], send_sem.at[chunk])
            drain(ctx_send.at[bs, pl.ds(0, n - FIRST - 1)], ctx_send_sem.at[chunk])


def store_kernel(y_ref, kv_hbm, y_hbm, k_hbm, v_hbm, buf, in_sem, out_sem, y_sem):
    n_batch = k_hbm.shape[0]
    y_out = pltpu.make_async_copy(y_ref, y_hbm, y_sem)
    pieces = [(t, b) for t in range(2) for b in range(n_batch)]
    get = [
        pltpu.make_async_copy(kv_hbm.at[1 + t, b], buf.at[t, b], in_sem.at[t, b]) for t, b in pieces
    ]
    put = [
        pltpu.make_async_copy(buf.at[t, b], (k_hbm, v_hbm)[t].at[b], out_sem.at[t, b]) for t, b in pieces
    ]
    for copy in get:
        copy.start()
    y_out.start()
    for got, going in zip(get, put):
        got.wait()
        going.start()
    for copy in put:
        copy.wait()
    y_out.wait()


def solution(mesh):
    n = mesh.shape["sp"]

    def local_layer(x_blk, ln_attn_w, ln_attn_b, ln_mlp_w, ln_mlp_b, w_qkv, w_out, w_up, w_down):
        n_batch, seq_dev, width = x_blk.shape
        groups, head_dim = w_qkv.shape[1], w_qkv.shape[3]
        heads = groups // n
        nb = n_batch // N_CHUNKS
        rows = n_batch * seq_dev
        dests = QKV_HEADS // heads
        ffn = w_up.shape[1]
        cos_t, sin_t = rope_tables(n * seq_dev, head_dim)
        row = lambda p: p.reshape(1, width)
        anywhere = pl.BlockSpec(memory_space=pl.ANY)
        flops = 2 * rows * width * (3 * width + 2 * ffn) + 2 * rows * n * seq_dev * width * 2
        y_out, recv, *_ = pl.pallas_call(
            functools.partial(layer_kernel, n),
            out_shape=[
                pltpu.VMEM((rows, width), BF16),
                jax.ShapeDtypeStruct((3, n_batch, heads, n, seq_dev, head_dim), BF16),
                jax.ShapeDtypeStruct((3, n_batch, n, heads, seq_dev, head_dim), BF16),
                jax.ShapeDtypeStruct((n_batch, n, seq_dev, heads * head_dim), BF16),
                jax.ShapeDtypeStruct((3, n_batch, dests, heads, seq_dev, head_dim), BF16),
                jax.ShapeDtypeStruct((n_batch, FIRST, seq_dev, dests * heads * head_dim), BF16),
                jax.ShapeDtypeStruct((n_batch, FIRST, seq_dev, heads * head_dim), BF16),
            ],
            in_specs=[anywhere] * 11,
            out_specs=[pl.BlockSpec(memory_space=pltpu.VMEM)] + [anywhere] * 6,
            scratch_shapes=[
                pltpu.VMEM((rows, width), F32),
                pltpu.VMEM((n_batch, seq_dev, width), BF16),
                pltpu.VMEM((4, 1, width), F32),
                pltpu.SemaphoreType.DMA,
                pltpu.SemaphoreType.DMA((4,)),
                pltpu.SemaphoreType.DMA((2,)),
                pltpu.SemaphoreType.DMA((2,)),
                pltpu.SemaphoreType.DMA((5,)),
                pltpu.SemaphoreType.DMA((2,)),
                pltpu.SemaphoreType.DMA((2,)),
                pltpu.SemaphoreType.DMA((3,)),
                pltpu.SemaphoreType.DMA((3, 2)),
                pltpu.SemaphoreType.DMA((N_CHUNKS,)),
                pltpu.SemaphoreType.DMA((N_CHUNKS, 3)),
                pltpu.SemaphoreType.DMA((N_CHUNKS,)),
                pltpu.SemaphoreType.DMA((N_CHUNKS, n // FIRST)),
                pltpu.SemaphoreType.DMA((N_CHUNKS,)),
                pltpu.SemaphoreType.DMA((N_CHUNKS,)),
                pltpu.SemaphoreType.DMA((N_CHUNKS,)),
                pltpu.SemaphoreType.DMA((N_CHUNKS,)),
                pltpu.SemaphoreType.DMA((N_CHUNKS,)),
                pltpu.SemaphoreType.DMA((N_CHUNKS,)),
            ],
            compiler_params=pltpu.CompilerParams(
                collective_id=0, has_side_effects=True, vmem_limit_bytes=57 * 2**20
            ),
            cost_estimate=pl.CostEstimate(flops=flops, bytes_accessed=3 * 10**8, transcendentals=10**7),
            name="layer",
        )(
            x_blk.reshape(rows, width),
            cos_t,
            sin_t,
            row(ln_attn_w),
            row(ln_attn_b),
            row(ln_mlp_w),
            row(ln_mlp_b),
            w_qkv.transpose(0, 2, 1, 3),
            w_out,
            w_up,
            w_down,
        )
        cache = jax.ShapeDtypeStruct((n_batch, heads, n, seq_dev, head_dim), BF16)
        y_out, k_cache, v_cache = pl.pallas_call(
            store_kernel,
            out_shape=[jax.ShapeDtypeStruct((rows, width), BF16), cache, cache],
            in_specs=[anywhere] * 2,
            out_specs=[pl.BlockSpec(memory_space=pltpu.HBM)] * 3,
            scratch_shapes=[
                pltpu.VMEM((2, n_batch, heads, n, seq_dev, head_dim), BF16),
                pltpu.SemaphoreType.DMA((2, n_batch)),
                pltpu.SemaphoreType.DMA((2, n_batch)),
                pltpu.SemaphoreType.DMA,
            ],
            compiler_params=pltpu.CompilerParams(vmem_limit_bytes=44 * 2**20),
            cost_estimate=pl.CostEstimate(flops=10**6, bytes_accessed=3 * 10**7, transcendentals=0),
            name="store",
        )(y_out, recv)
        shape = (n_batch, heads, n * seq_dev, head_dim)
        return y_out.reshape(x_blk.shape), k_cache.reshape(shape), v_cache.reshape(shape)

    act_spec, cache_spec = P("dp", "sp", None), P("dp", "sp", None, None)
    return jax.shard_map(
        local_layer,
        mesh=mesh,
        in_specs=(act_spec,) + (P(),) * 8,
        out_specs=(act_spec, cache_spec, cache_spec),
        check_vma=False,
    )
```

```python
import functools

import jax
import jax.numpy as jnp
import numpy as np
from jax import lax
from jax.experimental import pallas as pl
from jax.experimental.pallas import tpu as pltpu
from jax.sharding import PartitionSpec as P

LN_EPS = 1e-5
ROPE_BASE = 10000.0
LOG2E = 1.4426950408889634
N_CHUNKS = 6
UP_TILE = 512
QKV_HEADS = 8
Q_TILE = 256
FIRST = 2
LATE_STEPS = 2
RELAYED = 4
F32 = jnp.float32
BF16 = jnp.bfloat16


def rope_tables(positions, head_dim):
    half_dim = head_dim // 2
    inv_freq = np.float32(ROPE_BASE) ** (np.float32(-2.0) * np.arange(half_dim, dtype=np.float32) / np.float32(head_dim))
    angles = np.arange(positions, dtype=np.float32)[:, None] * inv_freq[None, :]
    cos_t, sin_t = np.cos(angles.astype(np.float64)), np.sin(angles.astype(np.float64))
    wide = lambda a, b: jnp.asarray(np.concatenate([a, b], -1).astype(np.float32))
    return wide(cos_t, cos_t), wide(-sin_t, sin_t)


def causal_head(q, k, v, write):
    seq, head_dim = k.shape
    scale = LOG2E * head_dim**-0.5
    keys = lax.broadcasted_iota(jnp.int32, (Q_TILE, Q_TILE), 0)
    queries = lax.broadcasted_iota(jnp.int32, (Q_TILE, Q_TILE), 1)
    for i in range(q.shape[0] // Q_TILE):
        lo = seq - q.shape[0] + i * Q_TILE
        hi = lo + Q_TILE
        q_i = q[i * Q_TILE : (i + 1) * Q_TILE]
        scores = lax.dot_general(k[:hi], q_i, (((1,), (1,)), ((), ())), preferred_element_type=F32)
        diag = jnp.where(keys <= queries, scores[lo:], -1e30)
        scores = jnp.concatenate([scores[:lo], diag], axis=0) if lo else diag
        prob = jnp.exp2((scores - jnp.max(scores, axis=0, keepdims=True)) * scale)
        prob = (prob * (1.0 / jnp.sum(prob, axis=0, keepdims=True))).astype(BF16)
        out = lax.dot_general(prob, v[:hi], (((0,), (0,)), ((), ())), preferred_element_type=F32)
        write(i, out.astype(BF16))


def layer_kernel(
    n,
    x_hbm,
    cos_hbm,
    sin_hbm,
    ln_aw_hbm,
    ln_ab_hbm,
    ln_mw_hbm,
    ln_mb_hbm,
    w_qkv,
    w_out,
    w_up,
    w_down,
    h_mlp,
    recv,
    send,
    ctx_send,
    near,
    ctx_near,
    relay,
    acc,
    ctx_rows,
    ln_buf,
    x_sem,
    ln_sem,
    w_sem,
    bounce_sem,
    own_sem,
    up_sem,
    down_sem,
    qkv_sem,
    near_sem,
    send_sem,
    recv_sem,
    ctx_send_sem,
    ctx_recv_sem,
    near_send_sem,
    near_recv_sem,
    ctx_near_send_sem,
    ctx_near_recv_sem,
    relay_recv_sem,
    relay_send_sem,
):
    me = lax.axis_index("sp")
    n_batch, _, heads, seq_dev, head_dim = send.shape[1:]
    cols = heads * head_dim
    width = x_hbm.shape[1]
    nb = n_batch // N_CHUNKS
    rows = nb * seq_dev
    ffn = w_up.shape[1]
    dests = QKV_HEADS // heads
    parts = n // dests
    blocks = 3 * parts

    def peer(step):
        return lax.bitwise_xor(me, step)

    def rows_of(chunk, first, count=1):
        return ctx_rows.at[pl.ds(chunk * nb, nb), :, pl.ds(pl.multiple_of(first * cols, cols), count * cols)]

    def put(chunk, kind, to, frm):
        bs = pl.ds(chunk * nb, nb)
        return pltpu.make_async_remote_copy(
            src_ref=send.at[kind, bs, to],
            dst_ref=recv.at[kind, bs, :, frm],
            send_sem=send_sem.at[chunk],
            recv_sem=recv_sem.at[chunk, kind],
            device_id={"sp": to},
            device_id_type=pl.DeviceIdType.MESH,
        )

    def put_ctx(chunk, to, frm):
        bs = pl.ds(chunk * nb, nb)
        return pltpu.make_async_remote_copy(
            src_ref=ctx_send.at[bs, to],
            dst_ref=rows_of(chunk, frm),
            send_sem=ctx_send_sem.at[chunk],
            recv_sem=ctx_recv_sem.at[chunk, frm // FIRST],
            device_id={"sp": to},
            device_id_type=pl.DeviceIdType.MESH,
        )

    def put_relay(chunk, to, slot):
        bs = pl.ds(chunk * nb, nb)
        return pltpu.make_async_remote_copy(
            src_ref=ctx_send.at[bs, to],
            dst_ref=relay.at[bs, slot],
            send_sem=ctx_send_sem.at[chunk],
            recv_sem=relay_recv_sem.at[chunk],
            device_id={"sp": to - FIRST},
            device_id_type=pl.DeviceIdType.MESH,
        )

    def forward(chunk, slot):
        bs = pl.ds(chunk * nb, nb)
        return pltpu.make_async_remote_copy(
            src_ref=relay.at[bs, slot],
            dst_ref=rows_of(chunk, 2 * FIRST + slot),
            send_sem=relay_send_sem.at[chunk],
            recv_sem=ctx_recv_sem.at[chunk, 2],
            device_id={"sp": me + FIRST},
            device_id_type=pl.DeviceIdType.MESH,
        )

    def put_near(chunk, kind):
        bs = pl.ds(chunk * nb, nb)
        return pltpu.make_async_remote_copy(
            src_ref=send.at[kind, bs, pl.ds((1 - me) * dests, dests)],
            dst_ref=near.at[kind, bs],
            send_sem=near_send_sem.at[chunk],
            recv_sem=near_recv_sem.at[chunk],
            device_id={"sp": 1 - me},
            device_id_type=pl.DeviceIdType.MESH,
        )

    def put_ctx_near(chunk):
        bs = pl.ds(chunk * nb, nb)
        return pltpu.make_async_remote_copy(
            src_ref=ctx_near.at[bs, 1 - me],
            dst_ref=rows_of(chunk, me * dests, dests),
            send_sem=ctx_near_send_sem.at[chunk],
            recv_sem=ctx_near_recv_sem.at[chunk],
            device_id={"sp": 1 - me},
            device_id_type=pl.DeviceIdType.MESH,
        )

    def drain(ref, sem):
        pltpu.make_async_copy(ref, ref, sem).wait()

    is_first = me < FIRST
    later_on = jnp.logical_not(is_first)

    def each_peer(do, lowest=0):
        for other in range(lowest, n):
            pl.when(other != me)(functools.partial(do, other))

    def qkv_phase(x_buf, h_attn, w_nat, w_cols, out_buf, own, cos_ref, sin_ref):
        mine = pl.ds(pl.multiple_of(me * seq_dev, seq_dev), seq_dev)
        get_cos = pltpu.make_async_copy(cos_hbm.at[mine], cos_ref, own_sem.at[3])
        get_sin = pltpu.make_async_copy(sin_hbm.at[mine], sin_ref, own_sem.at[4])

        def get_x(chunk):
            return pltpu.make_async_copy(x_hbm.at[pl.ds(chunk * rows, rows)], x_buf, x_sem)

        def get_w(half):
            block, slot = half // 2, lax.rem(half, 2)
            src = w_qkv.at[
                pl.ds(slot * (width // 2), width // 2),
                block // parts,
                pl.ds(lax.rem(block, parts) * QKV_HEADS, QKV_HEADS),
            ]
            return pltpu.make_async_copy(src, w_nat.at[slot], w_sem.at[slot])

        def bounce(step):
            slot, block = lax.rem(step, 2), lax.rem(step, blocks)
            dst = send.at[
                block // parts, pl.ds(step // blocks * nb, nb), pl.ds(lax.rem(block, parts) * dests, dests)
            ]
            return pltpu.make_async_copy(out_buf.at[slot], dst, bounce_sem.at[slot])

        def put_own(chunk, kind):
            dst = recv.at[kind, pl.ds(chunk * nb, nb), :, me]
            return pltpu.make_async_copy(own.at[kind], dst, own_sem.at[kind])

        def send_block(step):
            bounce(step).wait()
            block = lax.rem(step, blocks)
            for d in range(dests):
                to = lax.rem(block, parts) * dests + lax.rem(me + d, dests)

                @pl.when((to != me) & jnp.logical_not(is_first & (block < parts)))
                def _():
                    put(step // blocks, block // parts, to, me).start()

            @pl.when(is_first & (lax.rem(block, parts) == 1 - me))
            def _():
                put_near(step // blocks, block // parts).start()

        ln_hbm = (ln_aw_hbm, ln_ab_hbm, ln_mw_hbm, ln_mb_hbm)
        get_ln = [pltpu.make_async_copy(p, ln_buf.at[i], ln_sem.at[i]) for i, p in enumerate(ln_hbm)]
        ln_aw, ln_ab, ln_mw, ln_mb = (ln_buf.at[i] for i in range(4))
        get_x(0).start()
        for copy in get_ln:
            copy.start()
        get_w(0).start()
        get_w(1).start()
        get_cos.start()
        get_sin.start()
        barrier = pltpu.get_barrier_semaphore()
        for step in range(1, n):
            pl.semaphore_signal(
                barrier, inc=1, device_id={"sp": peer(step)}, device_id_type=pl.DeviceIdType.MESH
            )

        @pl.loop(0, N_CHUNKS * blocks)
        def _(step):
            chunk, block = step // blocks, lax.rem(step, blocks)
            kind, part = block // parts, lax.rem(block, parts)
            slot = lax.rem(step, 2)

            @pl.when(block == 0)
            def _():
                get_x(chunk).wait()

                @pl.when(chunk == 0)
                def _():
                    for copy in get_ln:
                        copy.wait()

                @pl.loop(0, nb)
                def _(i):
                    r = pl.ds(pl.multiple_of(i * seq_dev, seq_dev), seq_dev)
                    g = pl.ds(pl.multiple_of(chunk * rows + i * seq_dev, seq_dev), seq_dev)
                    xf = x_buf[r, :].astype(F32)
                    mean = jnp.sum(xf, axis=-1, keepdims=True) * (1.0 / width)
                    dev = xf - mean
                    var = jnp.sum(dev * dev, axis=-1, keepdims=True) * (1.0 / width)
                    unit = dev * lax.rsqrt(var + LN_EPS)
                    h_attn[r, :] = (unit * ln_aw[...] + ln_ab[...]).astype(BF16)
                    h_mlp[g, :] = (unit * ln_mw[...] + ln_mb[...]).astype(BF16)
                    acc[g, :] = xf

                @pl.when(chunk + 1 < N_CHUNKS)
                def _():
                    get_x(chunk + 1).start()

            @pl.when(chunk == 0)
            def _():
                @pl.when(block == 0)
                def _():
                    get_cos.wait()
                    get_sin.wait()

                @pl.loop(2 * block, 2 * block + 2)
                def _(half):
                    get_w(half).wait()

                    @pl.loop(0, width // 2 // 128)
                    def _(i):
                        r = pl.ds(pl.multiple_of(i * 128, 128), 128)
                        top = lax.rem(half, 2) * (width // 2)
                        to = pl.ds(pl.multiple_of(top + i * 128, 128), 128)
                        by_head = jnp.swapaxes(w_nat[lax.rem(half, 2), r].astype(F32), 0, 1)
                        for h in range(QKV_HEADS):
                            w_cols[block, to, h * head_dim : (h + 1) * head_dim] = by_head[h].astype(BF16)

                    @pl.when(half + 2 < 2 * blocks)
                    def _():
                        get_w(half + 2).start()

            for d in range(dests):
                cs = slice(d * heads * head_dim, (d + 1) * heads * head_dim)
                cols = jnp.dot(h_attn[...], w_cols[block, :, cs], preferred_element_type=F32)
                for h in range(heads):
                    for b in range(nb):
                        u = cols[b * seq_dev : (b + 1) * seq_dev, h * head_dim : (h + 1) * head_dim]
                        u = u.astype(BF16).astype(F32)
                        turned = u * cos_ref[...] + pltpu.roll(u, head_dim // 2, 1) * sin_ref[...]
                        out_buf[slot, b, d, h] = jnp.where(kind < 2, turned, u).astype(BF16)

            bounce(step).start()

            @pl.when(me // dests == part)
            def _():
                @pl.when(chunk > 0)
                def _():
                    put_own(chunk - 1, kind).wait()

                own[kind] = out_buf[slot, :, lax.rem(me, dests)]
                put_own(chunk, kind).start()

            @pl.when(step == 0)
            def _():
                pl.semaphore_wait(barrier, n - 1)

            @pl.when(chunk == 0)
            def _():
                send_block(step)

            @pl.when(step > blocks)
            def _():
                send_block(step - 1)

        send_block(N_CHUNKS * blocks - 1)
        for kind in range(3):
            put_own(N_CHUNKS - 1, kind).wait()

    pl.run_scoped(
        qkv_phase,
        pltpu.VMEM((rows, width), BF16),
        pltpu.VMEM((rows, width), BF16),
        pltpu.VMEM((2, width // 2, QKV_HEADS, head_dim), BF16),
        pltpu.VMEM((blocks, width, QKV_HEADS * head_dim), BF16),
        pltpu.VMEM((2, nb, dests, heads, seq_dev, head_dim), BF16),
        pltpu.VMEM((3, nb, heads, seq_dev, head_dim), BF16),
        pltpu.VMEM((seq_dev, head_dim), F32),
        pltpu.VMEM((seq_dev, head_dim), F32),
    )

    def rest(up_buf, down_buf, w_buf, qkv_buf, ctx_buf, both, near_buf):
        later = n - FIRST
        steps = ffn // UP_TILE

        def get_up(f):
            cols = pl.ds(pl.multiple_of(f * UP_TILE, UP_TILE), UP_TILE)
            slot = lax.rem(f, 2)
            return pltpu.make_async_copy(w_up.at[:, cols], up_buf.at[slot], up_sem.at[slot])

        def get_down(f):
            cols = pl.ds(pl.multiple_of(f * UP_TILE, UP_TILE), UP_TILE)
            slot = lax.rem(f, 2)
            return pltpu.make_async_copy(w_down.at[cols], down_buf.at[slot], down_sem.at[slot])

        def get_w_out():
            return pltpu.make_async_copy(w_out, w_buf, w_sem.at[0])

        def get_qkv(chunk, kind):
            return pltpu.make_async_copy(recv.at[kind, pl.ds(chunk * nb, nb)], qkv_buf.at[kind], qkv_sem.at[kind])

        def get_own_near(chunk, kind):
            src = send.at[kind, pl.ds(chunk * nb, nb), pl.ds(me * dests, dests)]
            return pltpu.make_async_copy(src, both.at[kind, :, :, :, me], near_sem.at[kind, 0])

        def get_other_near(chunk, kind):
            src = near.at[kind, pl.ds(chunk * nb, nb)]
            return pltpu.make_async_copy(src, both.at[kind, :, :, :, 1 - me], near_sem.at[kind, 1])

        def bounce_ctx(chunk):
            dst = ctx_send.at[pl.ds(chunk * nb, nb), pl.ds(FIRST, later)]
            return pltpu.make_async_copy(ctx_buf, dst, bounce_sem.at[0])

        def bounce_near(chunk):
            return pltpu.make_async_copy(near_buf, ctx_near.at[pl.ds(chunk * nb, nb)], bounce_sem.at[1])

        def send_ctx(chunk):
            bounce_ctx(chunk).wait()
            relays = (me // FIRST == 2) & (chunk < RELAYED)

            def one(other):
                if other // FIRST == 1:

                    @pl.when(relays)
                    def _():
                        put_relay(chunk, other, me - 2 * FIRST).start()

                    @pl.when(jnp.logical_not(relays))
                    def _():
                        put_ctx(chunk, other, me).start()

                else:
                    put_ctx(chunk, other, me).start()

            each_peer(one, FIRST)

        def send_near(chunk):
            bounce_near(chunk).wait()
            put_ctx_near(chunk).start()

        def pass_on(chunk):
            drain(relay.at[pl.ds(chunk * nb, nb)], relay_recv_sem.at[chunk])
            for slot in range(FIRST):
                forward(chunk, slot).start()

        def load_qkv(chunk):
            for kind in range(3):
                got = lambda count: recv.at[kind, pl.ds(chunk * nb, nb), :, pl.ds(0, count)]
                if kind:
                    drain(got(n - 1), recv_sem.at[chunk, kind])
                else:
                    pl.when(is_first)(lambda: drain(got(n - FIRST), recv_sem.at[chunk, kind]))
                    pl.when(later_on)(lambda: drain(got(n - FIRST - 1), recv_sem.at[chunk, kind]))
                get_qkv(chunk, kind).start()

            @pl.when(is_first)
            def _():
                drain(near.at[:, pl.ds(chunk * nb, nb)], near_recv_sem.at[chunk])
                for kind in range(3):
                    get_own_near(chunk, kind).start()
                    get_other_near(chunk, kind).start()

        get_up(0).start()
        get_down(0).start()
        get_w_out().start()

        @pl.loop(0, N_CHUNKS + 1)
        def _(chunk):
            early = steps - LATE_STEPS
            first = chunk * early // N_CHUNKS
            last = jnp.where(chunk < N_CHUNKS, (chunk + 1) * early // N_CHUNKS, steps)

            @pl.loop(first, last)
            def _(f):
                slot = lax.rem(f, 2)

                @pl.when(f + 1 < steps)
                def _():
                    get_up(f + 1).start()
                    get_down(f + 1).start()

                @pl.when((f == last - 1) & (chunk < N_CHUNKS - 1))
                def _():
                    load_qkv(chunk)

                get_up(f).wait()
                get_down(f).wait()
                for r in range(n_batch * seq_dev // 512):
                    rs = pl.ds(r * 512, 512)
                    up = jnp.dot(h_mlp[rs, :], up_buf[slot], preferred_element_type=F32)
                    hid = (0.5 * up * (1.0 + lax.erf(up * 0.5**0.5))).astype(BF16)
                    acc[rs, :] += jnp.dot(hid, down_buf[slot], preferred_element_type=F32)

                @pl.when((f == first) & (chunk > 0))
                def _():
                    @pl.when(chunk < N_CHUNKS)
                    def _():
                        send_ctx(chunk - 1)

                    @pl.when(is_first)
                    def _():
                        send_near(chunk - 1)

                @pl.when(is_first & (chunk == N_CHUNKS))
                def _():
                    first_relay = 1 + (f - first) * 2

                    @pl.loop(first_relay, jnp.minimum(jnp.where(f == steps - 1, RELAYED, first_relay + 2), RELAYED))
                    def _(c):
                        pass_on(c)

            @pl.when(chunk < N_CHUNKS)
            def _():
                @pl.when(chunk == N_CHUNKS - 1)
                def _():
                    load_qkv(chunk)

                for kind in range(3):
                    get_qkv(chunk, kind).wait()
                for b in range(nb):
                    for h in range(heads):
                        q = qkv_buf[0, b, h, FIRST:].reshape(later * seq_dev, head_dim)
                        k, v = (qkv_buf[t, b, h].reshape(n * seq_dev, head_dim) for t in (1, 2))
                        per = Q_TILE // seq_dev

                        def write(i, out):
                            ctx_buf[b, i * per : (i + 1) * per, :, h * head_dim : (h + 1) * head_dim] = out.reshape(
                                per, seq_dev, head_dim
                            )

                        causal_head(q, k, v, write)
                bounce_ctx(chunk).start()

                @pl.when(later_on)
                def _():
                    rows_of(chunk, me)[...] = ctx_buf[:, me - FIRST]

                @pl.when(chunk == N_CHUNKS - 1)
                def _():
                    send_ctx(chunk)

                    @pl.when(is_first)
                    def _():
                        pass_on(0)

                @pl.when(is_first)
                def _():
                    for kind in range(3):
                        get_own_near(chunk, kind).wait()
                        get_other_near(chunk, kind).wait()

                    @pl.loop(0, nb)
                    def _(b):
                        for d in range(dests):
                            for h in range(heads):
                                q, k, v = (both[t, b, d, h].reshape(Q_TILE, head_dim) for t in range(3))

                                def write(i, out):
                                    col = (d * heads + h) * head_dim
                                    near_buf[b, :, :, col : col + head_dim] = out.reshape(
                                        FIRST, seq_dev, head_dim
                                    )

                                causal_head(q, k, v, write)

                    bounce_near(chunk).start()
                    rows_of(chunk, me * dests, dests)[...] = near_buf[:, me]

        get_w_out().wait()

        @pl.loop(0, N_CHUNKS)
        def _(chunk):
            bs = pl.ds(chunk * nb, nb)

            @pl.when(is_first)
            def _():
                drain(send.at[pl.ds(1, 2), bs, pl.ds(0, n - 1)], send_sem.at[chunk])
                drain(near.at[:, bs], near_send_sem.at[chunk])

            @pl.when(later_on)
            def _():
                drain(send.at[:, bs, pl.ds(0, n - 1)], send_sem.at[chunk])

        def drain_ctx(chunk):
            bs = pl.ds(chunk * nb, nb)

            @pl.when(is_first)
            def _():
                drain(ctx_send.at[bs, pl.ds(0, n - FIRST)], ctx_send_sem.at[chunk])
                drain(ctx_near.at[bs, 0], ctx_near_send_sem.at[chunk])

            pl.when(later_on)(lambda: drain(ctx_send.at[bs, pl.ds(0, n - FIRST - 1)], ctx_send_sem.at[chunk]))

        @pl.loop(0, N_CHUNKS)
        def _(turn):
            pl.when(turn > 1)(lambda: drain_ctx(turn - 2))
            chunk = jnp.where(turn == 2, RELAYED, jnp.where((turn > 2) & (turn <= RELAYED), turn - 1, turn))

            g = pl.ds(pl.multiple_of(chunk * rows, rows), rows)
            pl.when(is_first)(lambda: put_ctx_near(chunk).wait_recv())
            for part in range(n // FIRST):
                home = me // FIRST
                source = jnp.where(part == 0, home, jnp.where(part <= home, part - 1, part))

                @pl.when(later_on)
                def _():
                    count = FIRST - (part == 0)
                    drain(rows_of(chunk, 0, count), ctx_recv_sem.at[chunk, source])

                span = pl.ds(pl.multiple_of(source * FIRST * cols, FIRST * cols), FIRST * cols)
                left = ctx_rows[pl.ds(chunk * nb, nb), :, span].reshape(rows, FIRST * cols)
                for c in range(0, width, 1024):
                    cs = slice(c, c + 1024)
                    total = acc[g, cs] + jnp.dot(left, w_buf[span, cs], preferred_element_type=F32)
                    if part < n // FIRST - 1:
                        acc[g, cs] = total
                    else:
                        h_mlp[g, cs] = total.astype(BF16)

        for chunk in (N_CHUNKS - 2, N_CHUNKS - 1):
            drain_ctx(chunk)

        @pl.when(is_first)
        def _():
            for chunk in range(RELAYED):
                drain(relay.at[pl.ds(chunk * nb, nb)], relay_send_sem.at[chunk])

    pl.run_scoped(
        rest,
        pltpu.VMEM((2, width, UP_TILE), BF16),
        pltpu.VMEM((2, UP_TILE, width), BF16),
        pltpu.VMEM((width, width), BF16),
        pltpu.VMEM((3, nb, heads, n, seq_dev, head_dim), BF16),
        pltpu.VMEM((nb, n - FIRST, seq_dev, cols), BF16),
        pltpu.VMEM((3, nb, dests, heads, FIRST, seq_dev, head_dim), BF16),
        pltpu.VMEM((nb, FIRST, seq_dev, dests * cols), BF16),
    )


def store_kernel(y_ref, kv_hbm, y_hbm, k_hbm, v_hbm, buf, in_sem, out_sem, y_sem):
    n_batch = k_hbm.shape[0]
    y_out = pltpu.make_async_copy(y_ref, y_hbm, y_sem)
    pieces = [(t, b) for t in range(2) for b in range(n_batch)]
    get = [
        pltpu.make_async_copy(kv_hbm.at[1 + t, b], buf.at[t, b], in_sem.at[t, b]) for t, b in pieces
    ]
    put = [
        pltpu.make_async_copy(buf.at[t, b], (k_hbm, v_hbm)[t].at[b], out_sem.at[t, b]) for t, b in pieces
    ]
    for copy in get:
        copy.start()
    for copy in get:
        copy.wait()
    y_out.start()
    for copy in put:
        copy.start()
    for copy in put:
        copy.wait()
    y_out.wait()


def solution(mesh):
    n = mesh.shape["sp"]

    def local_layer(x_blk, ln_attn_w, ln_attn_b, ln_mlp_w, ln_mlp_b, w_qkv, w_out, w_up, w_down):
        n_batch, seq_dev, width = x_blk.shape
        groups, head_dim = w_qkv.shape[1], w_qkv.shape[3]
        heads = groups // n
        nb = n_batch // N_CHUNKS
        rows = n_batch * seq_dev
        dests = QKV_HEADS // heads
        ffn = w_up.shape[1]
        cos_t, sin_t = rope_tables(n * seq_dev, head_dim)
        row = lambda p: p.reshape(1, width)
        anywhere = pl.BlockSpec(memory_space=pl.ANY)
        flops = 2 * rows * width * (3 * width + 2 * ffn) + 2 * rows * n * seq_dev * width * 2
        y_out, recv, *_ = pl.pallas_call(
            functools.partial(layer_kernel, n),
            out_shape=[
                pltpu.VMEM((rows, width), BF16),
                jax.ShapeDtypeStruct((3, n_batch, heads, n, seq_dev, head_dim), BF16),
                jax.ShapeDtypeStruct((3, n_batch, n, heads, seq_dev, head_dim), BF16),
                jax.ShapeDtypeStruct((n_batch, n, seq_dev, heads * head_dim), BF16),
                jax.ShapeDtypeStruct((3, n_batch, dests, heads, seq_dev, head_dim), BF16),
                jax.ShapeDtypeStruct((n_batch, FIRST, seq_dev, dests * heads * head_dim), BF16),
                jax.ShapeDtypeStruct((n_batch, FIRST, seq_dev, heads * head_dim), BF16),
            ],
            in_specs=[anywhere] * 11,
            out_specs=[pl.BlockSpec(memory_space=pltpu.VMEM)] + [anywhere] * 6,
            scratch_shapes=[
                pltpu.VMEM((rows, width), F32),
                pltpu.VMEM((n_batch, seq_dev, width), BF16),
                pltpu.VMEM((4, 1, width), F32),
                pltpu.SemaphoreType.DMA,
                pltpu.SemaphoreType.DMA((4,)),
                pltpu.SemaphoreType.DMA((2,)),
                pltpu.SemaphoreType.DMA((2,)),
                pltpu.SemaphoreType.DMA((5,)),
                pltpu.SemaphoreType.DMA((2,)),
                pltpu.SemaphoreType.DMA((2,)),
                pltpu.SemaphoreType.DMA((3,)),
                pltpu.SemaphoreType.DMA((3, 2)),
                pltpu.SemaphoreType.DMA((N_CHUNKS,)),
                pltpu.SemaphoreType.DMA((N_CHUNKS, 3)),
                pltpu.SemaphoreType.DMA((N_CHUNKS,)),
                pltpu.SemaphoreType.DMA((N_CHUNKS, n // FIRST)),
                pltpu.SemaphoreType.DMA((N_CHUNKS,)),
                pltpu.SemaphoreType.DMA((N_CHUNKS,)),
                pltpu.SemaphoreType.DMA((N_CHUNKS,)),
                pltpu.SemaphoreType.DMA((N_CHUNKS,)),
                pltpu.SemaphoreType.DMA((N_CHUNKS,)),
                pltpu.SemaphoreType.DMA((N_CHUNKS,)),
            ],
            compiler_params=pltpu.CompilerParams(
                collective_id=0, has_side_effects=True, vmem_limit_bytes=57 * 2**20
            ),
            cost_estimate=pl.CostEstimate(flops=flops, bytes_accessed=3 * 10**8, transcendentals=10**7),
            name="layer",
        )(
            x_blk.reshape(rows, width),
            cos_t,
            sin_t,
            row(ln_attn_w),
            row(ln_attn_b),
            row(ln_mlp_w),
            row(ln_mlp_b),
            w_qkv.transpose(0, 2, 1, 3),
            w_out,
            w_up,
            w_down,
        )
        cache = jax.ShapeDtypeStruct((n_batch, heads, n, seq_dev, head_dim), BF16)
        y_out, k_cache, v_cache = pl.pallas_call(
            store_kernel,
            out_shape=[jax.ShapeDtypeStruct((rows, width), BF16), cache, cache],
            in_specs=[anywhere] * 2,
            out_specs=[pl.BlockSpec(memory_space=pltpu.HBM)] * 3,
            scratch_shapes=[
                pltpu.VMEM((2, n_batch, heads, n, seq_dev, head_dim), BF16),
                pltpu.SemaphoreType.DMA((2, n_batch)),
                pltpu.SemaphoreType.DMA((2, n_batch)),
                pltpu.SemaphoreType.DMA,
            ],
            compiler_params=pltpu.CompilerParams(vmem_limit_bytes=44 * 2**20),
            cost_estimate=pl.CostEstimate(flops=10**6, bytes_accessed=3 * 10**7, transcendentals=0),
            name="store",
        )(y_out, recv)
        shape = (n_batch, heads, n * seq_dev, head_dim)
        return y_out.reshape(x_blk.shape), k_cache.reshape(shape), v_cache.reshape(shape)

    act_spec, cache_spec = P("dp", "sp", None), P("dp", "sp", None, None)
    return jax.shard_map(
        local_layer,
        mesh=mesh,
        in_specs=(act_spec,) + (P(),) * 8,
        out_specs=(act_spec, cache_spec, cache_spec),
        check_vma=False,
    )
```

```python
import functools

import jax
import jax.numpy as jnp
import numpy as np
from jax import lax
from jax.experimental import pallas as pl
from jax.experimental.pallas import tpu as pltpu
from jax.sharding import PartitionSpec as P

LN_EPS = 1e-5
ROPE_BASE = 10000.0
LOG2E = 1.4426950408889634
N_CHUNKS = 6
UNITS = N_CHUNKS + 1
UP_TILE = 512
QKV_HEADS = 8
Q_TILE = 256
FIRST = 2
LATE_STEPS = 2
RELAYED = 5
F32 = jnp.float32
BF16 = jnp.bfloat16


def rope_tables(positions, head_dim):
    half_dim = head_dim // 2
    inv_freq = np.float32(ROPE_BASE) ** (np.float32(-2.0) * np.arange(half_dim, dtype=np.float32) / np.float32(head_dim))
    angles = np.arange(positions, dtype=np.float32)[:, None] * inv_freq[None, :]
    cos_t, sin_t = np.cos(angles.astype(np.float64)), np.sin(angles.astype(np.float64))
    wide = lambda a, b: jnp.asarray(np.concatenate([a, b], -1).astype(np.float32))
    return wide(cos_t, cos_t), wide(-sin_t, sin_t)


def causal_head(q, k, v, write):
    seq, head_dim = k.shape
    scale = LOG2E * head_dim**-0.5
    keys = lax.broadcasted_iota(jnp.int32, (Q_TILE, Q_TILE), 0)
    queries = lax.broadcasted_iota(jnp.int32, (Q_TILE, Q_TILE), 1)
    for i in range(q.shape[0] // Q_TILE):
        lo = seq - q.shape[0] + i * Q_TILE
        hi = lo + Q_TILE
        q_i = q[i * Q_TILE : (i + 1) * Q_TILE]
        scores = lax.dot_general(k[:hi], q_i, (((1,), (1,)), ((), ())), preferred_element_type=F32)
        diag = jnp.where(keys <= queries, scores[lo:], -1e30)
        scores = jnp.concatenate([scores[:lo], diag], axis=0) if lo else diag
        prob = jnp.exp2((scores - jnp.max(scores, axis=0, keepdims=True)) * scale)
        prob = (prob * (1.0 / jnp.sum(prob, axis=0, keepdims=True))).astype(BF16)
        out = lax.dot_general(prob, v[:hi], (((0,), (0,)), ((), ())), preferred_element_type=F32)
        write(i, out.astype(BF16))


def layer_kernel(
    n,
    x_hbm,
    cos_hbm,
    sin_hbm,
    ln_aw_hbm,
    ln_ab_hbm,
    ln_mw_hbm,
    ln_mb_hbm,
    w_qkv,
    w_out,
    w_up,
    w_down,
    h_mlp,
    recv,
    send,
    ctx_send,
    near,
    ctx_near,
    relay,
    acc,
    ctx_rows,
    ln_buf,
    x_sem,
    ln_sem,
    w_sem,
    bounce_sem,
    own_sem,
    up_sem,
    down_sem,
    qkv_sem,
    near_sem,
    send_sem,
    recv_sem,
    ctx_send_sem,
    ctx_recv_sem,
    near_send_sem,
    near_recv_sem,
    ctx_near_send_sem,
    ctx_near_recv_sem,
    relay_recv_sem,
    relay_send_sem,
):
    me = lax.axis_index("sp")
    n_batch, _, heads, seq_dev, head_dim = send.shape[1:]
    cols = heads * head_dim
    width = x_hbm.shape[1]
    nb = n_batch // N_CHUNKS
    rows = nb * seq_dev
    ffn = w_up.shape[1]
    dests = QKV_HEADS // heads
    parts = n // dests
    blocks = 3 * parts

    def peer(step):
        return lax.bitwise_xor(me, step)

    def rows_of(bs, first, count=1):
        return ctx_rows.at[bs, :, pl.ds(pl.multiple_of(first * cols, cols), count * cols)]

    half = nb // 2

    def span(unit, small):
        return pl.ds(n_batch - nb + (unit - (N_CHUNKS - 1)) * half, half) if small else pl.ds(unit * nb, nb)

    def put(unit, kind, to, frm, small=False):
        bs = span(unit, small)
        return pltpu.make_async_remote_copy(
            src_ref=send.at[kind, bs, to],
            dst_ref=recv.at[kind, bs, :, frm],
            send_sem=send_sem.at[unit],
            recv_sem=recv_sem.at[unit, kind],
            device_id={"sp": to},
            device_id_type=pl.DeviceIdType.MESH,
        )

    def put_ctx(unit, to, frm, small=False):
        bs = span(unit, small)
        return pltpu.make_async_remote_copy(
            src_ref=ctx_send.at[bs, to],
            dst_ref=rows_of(bs, frm),
            send_sem=ctx_send_sem.at[unit],
            recv_sem=ctx_recv_sem.at[unit, frm // FIRST],
            device_id={"sp": to},
            device_id_type=pl.DeviceIdType.MESH,
        )

    def put_relay(chunk, to, slot):
        bs = pl.ds(chunk * nb, nb)
        return pltpu.make_async_remote_copy(
            src_ref=ctx_send.at[bs, to],
            dst_ref=relay.at[bs, slot],
            send_sem=ctx_send_sem.at[chunk],
            recv_sem=relay_recv_sem.at[chunk],
            device_id={"sp": to - FIRST},
            device_id_type=pl.DeviceIdType.MESH,
        )

    def forward(chunk, slot):
        bs = pl.ds(chunk * nb, nb)
        return pltpu.make_async_remote_copy(
            src_ref=relay.at[bs, slot],
            dst_ref=rows_of(bs, 2 * FIRST + slot),
            send_sem=relay_send_sem.at[chunk],
            recv_sem=ctx_recv_sem.at[chunk, 2],
            device_id={"sp": me + FIRST},
            device_id_type=pl.DeviceIdType.MESH,
        )

    def put_near(chunk, kind):
        bs = pl.ds(chunk * nb, nb)
        return pltpu.make_async_remote_copy(
            src_ref=send.at[kind, bs, pl.ds((1 - me) * dests, dests)],
            dst_ref=near.at[kind, bs],
            send_sem=near_send_sem.at[chunk],
            recv_sem=near_recv_sem.at[chunk],
            device_id={"sp": 1 - me},
            device_id_type=pl.DeviceIdType.MESH,
        )

    def put_ctx_near(chunk):
        bs = pl.ds(chunk * nb, nb)
        return pltpu.make_async_remote_copy(
            src_ref=ctx_near.at[bs, 1 - me],
            dst_ref=rows_of(bs, me * dests, dests),
            send_sem=ctx_near_send_sem.at[chunk],
            recv_sem=ctx_near_recv_sem.at[chunk],
            device_id={"sp": 1 - me},
            device_id_type=pl.DeviceIdType.MESH,
        )

    def drain(ref, sem):
        pltpu.make_async_copy(ref, ref, sem).wait()

    is_first = me < FIRST
    later_on = jnp.logical_not(is_first)

    def each_peer(do, lowest=0):
        for other in range(lowest, n):
            pl.when(other != me)(functools.partial(do, other))

    def qkv_phase(x_buf, h_attn, w_nat, w_cols, out_buf, own, cos_ref, sin_ref):
        mine = pl.ds(pl.multiple_of(me * seq_dev, seq_dev), seq_dev)
        get_cos = pltpu.make_async_copy(cos_hbm.at[mine], cos_ref, own_sem.at[3])
        get_sin = pltpu.make_async_copy(sin_hbm.at[mine], sin_ref, own_sem.at[4])

        def get_x(chunk):
            return pltpu.make_async_copy(x_hbm.at[pl.ds(chunk * rows, rows)], x_buf, x_sem)

        def get_w(half):
            block, slot = half // 2, lax.rem(half, 2)
            src = w_qkv.at[
                pl.ds(slot * (width // 2), width // 2),
                block // parts,
                pl.ds(lax.rem(block, parts) * QKV_HEADS, QKV_HEADS),
            ]
            return pltpu.make_async_copy(src, w_nat.at[slot], w_sem.at[slot])

        def bounce(step):
            slot, block = lax.rem(step, 2), lax.rem(step, blocks)
            dst = send.at[
                block // parts, pl.ds(step // blocks * nb, nb), pl.ds(lax.rem(block, parts) * dests, dests)
            ]
            return pltpu.make_async_copy(out_buf.at[slot], dst, bounce_sem.at[slot])

        def put_own(chunk, kind):
            dst = recv.at[kind, pl.ds(chunk * nb, nb), :, me]
            return pltpu.make_async_copy(own.at[kind], dst, own_sem.at[kind])

        def send_unit(unit, block, small):
            for d in range(dests):
                to = lax.rem(block, parts) * dests + lax.rem(me + d, dests)

                @pl.when((to != me) & jnp.logical_not(is_first & (block < parts)))
                def _():
                    put(unit, block // parts, to, me, small).start()

        def send_block(step):
            bounce(step).wait()
            block = lax.rem(step, blocks)
            is_last = step // blocks == N_CHUNKS - 1
            pl.when(jnp.logical_not(is_last))(lambda: send_unit(step // blocks, block, False))
            pl.when(is_last)(lambda: send_unit(N_CHUNKS - 1, block, True))

            @pl.when(is_first & (lax.rem(block, parts) == 1 - me))
            def _():
                put_near(step // blocks, block // parts).start()

        ln_hbm = (ln_aw_hbm, ln_ab_hbm, ln_mw_hbm, ln_mb_hbm)
        get_ln = [pltpu.make_async_copy(p, ln_buf.at[i], ln_sem.at[i]) for i, p in enumerate(ln_hbm)]
        ln_aw, ln_ab, ln_mw, ln_mb = (ln_buf.at[i] for i in range(4))
        get_x(0).start()
        for copy in get_ln:
            copy.start()
        get_w(0).start()
        get_w(1).start()
        get_cos.start()
        get_sin.start()
        barrier = pltpu.get_barrier_semaphore()
        for step in range(1, n):
            pl.semaphore_signal(
                barrier, inc=1, device_id={"sp": peer(step)}, device_id_type=pl.DeviceIdType.MESH
            )

        @pl.loop(0, N_CHUNKS * blocks)
        def _(step):
            chunk, block = step // blocks, lax.rem(step, blocks)
            kind, part = block // parts, lax.rem(block, parts)
            slot = lax.rem(step, 2)

            @pl.when(block == 0)
            def _():
                get_x(chunk).wait()

                @pl.when(chunk == 0)
                def _():
                    for copy in get_ln:
                        copy.wait()

                @pl.loop(0, nb)
                def _(i):
                    r = pl.ds(pl.multiple_of(i * seq_dev, seq_dev), seq_dev)
                    g = pl.ds(pl.multiple_of(chunk * rows + i * seq_dev, seq_dev), seq_dev)
                    xf = x_buf[r, :].astype(F32)
                    mean = jnp.sum(xf, axis=-1, keepdims=True) * (1.0 / width)
                    dev = xf - mean
                    var = jnp.sum(dev * dev, axis=-1, keepdims=True) * (1.0 / width)
                    unit = dev * lax.rsqrt(var + LN_EPS)
                    h_attn[r, :] = (unit * ln_aw[...] + ln_ab[...]).astype(BF16)
                    h_mlp[g, :] = (unit * ln_mw[...] + ln_mb[...]).astype(BF16)
                    acc[g, :] = xf

                @pl.when(chunk + 1 < N_CHUNKS)
                def _():
                    get_x(chunk + 1).start()

            @pl.when(chunk == 0)
            def _():
                @pl.when(block == 0)
                def _():
                    get_cos.wait()
                    get_sin.wait()

                @pl.loop(2 * block, 2 * block + 2)
                def _(half):
                    get_w(half).wait()

                    @pl.loop(0, width // 2 // 128)
                    def _(i):
                        r = pl.ds(pl.multiple_of(i * 128, 128), 128)
                        top = lax.rem(half, 2) * (width // 2)
                        to = pl.ds(pl.multiple_of(top + i * 128, 128), 128)
                        by_head = jnp.swapaxes(w_nat[lax.rem(half, 2), r].astype(F32), 0, 1)
                        for h in range(QKV_HEADS):
                            w_cols[block, to, h * head_dim : (h + 1) * head_dim] = by_head[h].astype(BF16)

                    @pl.when(half + 2 < 2 * blocks)
                    def _():
                        get_w(half + 2).start()

            for d in range(dests):
                cs = slice(d * heads * head_dim, (d + 1) * heads * head_dim)
                cols = jnp.dot(h_attn[...], w_cols[block, :, cs], preferred_element_type=F32)
                for h in range(heads):
                    for b in range(nb):
                        u = cols[b * seq_dev : (b + 1) * seq_dev, h * head_dim : (h + 1) * head_dim]
                        u = u.astype(BF16).astype(F32)
                        turned = u * cos_ref[...] + pltpu.roll(u, head_dim // 2, 1) * sin_ref[...]
                        out_buf[slot, b, d, h] = jnp.where(kind < 2, turned, u).astype(BF16)

            bounce(step).start()

            @pl.when(me // dests == part)
            def _():
                @pl.when(chunk > 0)
                def _():
                    put_own(chunk - 1, kind).wait()

                own[kind] = out_buf[slot, :, lax.rem(me, dests)]
                put_own(chunk, kind).start()

            @pl.when(step == 0)
            def _():
                pl.semaphore_wait(barrier, n - 1)

            @pl.when(chunk == 0)
            def _():
                send_block(step)

            @pl.when(step > blocks)
            def _():
                send_block(step - 1)

        send_block(N_CHUNKS * blocks - 1)
        pl.loop(0, blocks)(lambda block: send_unit(UNITS - 1, block, True))
        for kind in range(3):
            put_own(N_CHUNKS - 1, kind).wait()

    pl.run_scoped(
        qkv_phase,
        pltpu.VMEM((rows, width), BF16),
        pltpu.VMEM((rows, width), BF16),
        pltpu.VMEM((2, width // 2, QKV_HEADS, head_dim), BF16),
        pltpu.VMEM((blocks, width, QKV_HEADS * head_dim), BF16),
        pltpu.VMEM((2, nb, dests, heads, seq_dev, head_dim), BF16),
        pltpu.VMEM((3, nb, heads, seq_dev, head_dim), BF16),
        pltpu.VMEM((seq_dev, head_dim), F32),
        pltpu.VMEM((seq_dev, head_dim), F32),
    )

    def rest(up_buf, down_buf, w_buf, qkv_buf, ctx_buf, both, near_buf):
        later = n - FIRST
        steps = ffn // UP_TILE

        def get_up(f):
            cols = pl.ds(pl.multiple_of(f * UP_TILE, UP_TILE), UP_TILE)
            slot = lax.rem(f, 2)
            return pltpu.make_async_copy(w_up.at[:, cols], up_buf.at[slot], up_sem.at[slot])

        def get_down(f):
            cols = pl.ds(pl.multiple_of(f * UP_TILE, UP_TILE), UP_TILE)
            slot = lax.rem(f, 2)
            return pltpu.make_async_copy(w_down.at[cols], down_buf.at[slot], down_sem.at[slot])

        def get_w_out():
            return pltpu.make_async_copy(w_out, w_buf, w_sem.at[0])

        def get_qkv(unit, kind, small):
            count = half if small else nb
            to = qkv_buf.at[kind, pl.ds(0, count)]
            return pltpu.make_async_copy(recv.at[kind, span(unit, small)], to, qkv_sem.at[kind])

        def get_own_near(chunk, kind):
            src = send.at[kind, pl.ds(chunk * nb, nb), pl.ds(me * dests, dests)]
            return pltpu.make_async_copy(src, both.at[kind, :, :, :, me], near_sem.at[kind, 0])

        def get_other_near(chunk, kind):
            src = near.at[kind, pl.ds(chunk * nb, nb)]
            return pltpu.make_async_copy(src, both.at[kind, :, :, :, 1 - me], near_sem.at[kind, 1])

        def bounce_ctx(unit, small):
            dst = ctx_send.at[span(unit, small), pl.ds(FIRST, later)]
            return pltpu.make_async_copy(ctx_buf.at[pl.ds(0, half if small else nb)], dst, bounce_sem.at[0])

        def bounce_near(chunk):
            return pltpu.make_async_copy(near_buf, ctx_near.at[pl.ds(chunk * nb, nb)], bounce_sem.at[1])

        def send_ctx(unit, small=False):
            bounce_ctx(unit, small).wait()
            relays = (me // FIRST == 2) & (unit < RELAYED)

            def one(other):
                if other // FIRST == 1 and not small:
                    pl.when(relays)(lambda: put_relay(unit, other, me - 2 * FIRST).start())
                    pl.when(jnp.logical_not(relays))(lambda: put_ctx(unit, other, me).start())
                else:
                    put_ctx(unit, other, me, small).start()

            each_peer(one, FIRST)

        def send_near(chunk):
            bounce_near(chunk).wait()
            put_ctx_near(chunk).start()

        def pass_on(chunk):
            drain(relay.at[pl.ds(chunk * nb, nb)], relay_recv_sem.at[chunk])
            for slot in range(FIRST):
                forward(chunk, slot).start()

        def load_qkv(unit, small=False):
            bs = span(unit, small)
            for kind in range(3):
                got = lambda count: recv.at[kind, bs, :, pl.ds(0, count)]
                if kind:
                    drain(got(n - 1), recv_sem.at[unit, kind])
                else:
                    pl.when(is_first)(lambda: drain(got(n - FIRST), recv_sem.at[unit, kind]))
                    pl.when(later_on)(lambda: drain(got(n - FIRST - 1), recv_sem.at[unit, kind]))
                get_qkv(unit, kind, small).start()

        def load_near(chunk):
            drain(near.at[:, pl.ds(chunk * nb, nb)], near_recv_sem.at[chunk])
            for kind in range(3):
                get_own_near(chunk, kind).start()
                get_other_near(chunk, kind).start()

        def attend(unit, small=False):
            for kind in range(3):
                get_qkv(unit, kind, small).wait()
            count = half if small else nb
            for b in range(count):
                for h in range(heads):
                    q = qkv_buf[0, b, h, FIRST:].reshape(later * seq_dev, head_dim)
                    k, v = (qkv_buf[t, b, h].reshape(n * seq_dev, head_dim) for t in (1, 2))
                    per = Q_TILE // seq_dev

                    def write(i, out):
                        ctx_buf[b, i * per : (i + 1) * per, :, h * head_dim : (h + 1) * head_dim] = out.reshape(
                            per, seq_dev, head_dim
                        )

                    causal_head(q, k, v, write)
            bounce_ctx(unit, small).start()

            @pl.when(later_on)
            def _():
                rows_of(span(unit, small), me)[...] = ctx_buf[:count, me - FIRST]

        get_up(0).start()
        get_down(0).start()
        get_w_out().start()

        early = steps - LATE_STEPS

        def mlp_end(turn):
            whole = (turn + 1) * early // N_CHUNKS
            return jnp.where(turn < N_CHUNKS - 1, whole, jnp.where(turn < UNITS, early - UNITS + 1 + turn, steps))

        @pl.loop(0, UNITS + 1)
        def _(unit):
            first, last = jnp.where(unit > 0, mlp_end(unit - 1), 0), mlp_end(unit)
            is_small = (unit == UNITS - 1) | (unit == UNITS - 2)

            @pl.loop(first, last)
            def _(f):
                slot = lax.rem(f, 2)

                @pl.when(f + 1 < steps)
                def _():
                    get_up(f + 1).start()
                    get_down(f + 1).start()

                @pl.when((f == last - 1) & (unit < N_CHUNKS - 1))
                def _():
                    load_qkv(unit)
                    pl.when(is_first)(lambda: load_near(unit))

                @pl.when((f == last - 1) & (unit == UNITS - 2))
                def _():
                    load_qkv(unit, True)

                get_up(f).wait()
                get_down(f).wait()
                for r in range(n_batch * seq_dev // 512):
                    rs = pl.ds(r * 512, 512)
                    up = jnp.dot(h_mlp[rs, :], up_buf[slot], preferred_element_type=F32)
                    hid = (0.5 * up * (1.0 + lax.erf(up * 0.5**0.5))).astype(BF16)
                    acc[rs, :] += jnp.dot(hid, down_buf[slot], preferred_element_type=F32)

                @pl.when((f == first) & (unit > 0) & (unit < N_CHUNKS))
                def _():
                    send_ctx(unit - 1)
                    pl.when(is_first)(lambda: send_near(unit - 1))

                @pl.when(is_first & (unit == UNITS))
                def _():
                    pl.when(f == first)(lambda: send_near(N_CHUNKS - 1))
                    pass_on(1 + 2 * (f - first))
                    pl.when(f == first)(lambda: pass_on(2))

            pl.when(unit < N_CHUNKS - 1)(lambda: attend(unit))
            pl.when(unit == UNITS - 1)(lambda: load_qkv(unit, True))

            @pl.when(is_small)
            def _():
                attend(unit, True)
                send_ctx(unit, True)

            @pl.when(is_first & (unit != UNITS - 2) & (unit < UNITS))
            def _():
                chunk = jnp.minimum(unit, N_CHUNKS - 1)

                @pl.when(unit == UNITS - 1)
                def _():
                    pass_on(0)
                    load_near(chunk)

                if chunk is not None:
                    for kind in range(3):
                        get_own_near(chunk, kind).wait()
                        get_other_near(chunk, kind).wait()

                    @pl.loop(0, nb)
                    def _(b):
                        for d in range(dests):
                            for h in range(heads):
                                q, k, v = (both[t, b, d, h].reshape(Q_TILE, head_dim) for t in range(3))

                                def write(i, out):
                                    col = (d * heads + h) * head_dim
                                    near_buf[b, :, :, col : col + head_dim] = out.reshape(
                                        FIRST, seq_dev, head_dim
                                    )

                                causal_head(q, k, v, write)

                    bounce_near(chunk).start()
                    rows_of(pl.ds(chunk * nb, nb), me * dests, dests)[...] = near_buf[:, me]

        get_w_out().wait()

        def drain_qkv(unit, small=False):
            bs = span(unit, small)
            pl.when(is_first)(lambda: drain(send.at[pl.ds(1, 2), bs, pl.ds(0, n - 1)], send_sem.at[unit]))
            pl.when(later_on)(lambda: drain(send.at[:, bs, pl.ds(0, n - 1)], send_sem.at[unit]))

        def drain_ctx(unit, small=False):
            bs = span(unit, small)
            pl.when(is_first)(lambda: drain(ctx_send.at[bs, pl.ds(0, n - FIRST)], ctx_send_sem.at[unit]))
            pl.when(later_on)(lambda: drain(ctx_send.at[bs, pl.ds(0, n - FIRST - 1)], ctx_send_sem.at[unit]))

        pl.loop(0, N_CHUNKS - 1)(drain_qkv)
        pl.loop(N_CHUNKS - 1, UNITS)(lambda unit: drain_qkv(unit, True))

        @pl.loop(0, N_CHUNKS)
        def _(turn):
            pl.when(turn > 1)(lambda: drain_ctx(turn - 2))
            pl.when(is_first & (turn == 2))(lambda: pass_on(RELAYED - 1))
            chunk = turn
            g = pl.ds(pl.multiple_of(chunk * rows, rows), rows)
            pl.when(is_first)(lambda: put_ctx_near(chunk).wait_recv())
            for part in range(n // FIRST):
                home = me // FIRST
                source = jnp.where(part == 0, home, jnp.where(part <= home, part - 1, part))

                count = FIRST - (part == 0)

                @pl.when(later_on & (chunk < N_CHUNKS - 1))
                def _():
                    drain(rows_of(span(chunk, False), 0, count), ctx_recv_sem.at[chunk, source])

                @pl.when(later_on & (chunk == N_CHUNKS - 1))
                def _():
                    for unit in (N_CHUNKS - 1, N_CHUNKS):
                        drain(rows_of(span(unit, True), 0, count), ctx_recv_sem.at[unit, source])

                those = pl.ds(pl.multiple_of(source * FIRST * cols, FIRST * cols), FIRST * cols)
                left = ctx_rows[pl.ds(chunk * nb, nb), :, those].reshape(rows, FIRST * cols)
                for c in range(0, width, 1024):
                    cs = slice(c, c + 1024)
                    total = acc[g, cs] + jnp.dot(left, w_buf[those, cs], preferred_element_type=F32)
                    if part < n // FIRST - 1:
                        acc[g, cs] = total
                    else:
                        h_mlp[g, cs] = total.astype(BF16)

        drain_ctx(N_CHUNKS - 2)
        pl.loop(N_CHUNKS - 1, UNITS)(lambda unit: drain_ctx(unit, True))

        @pl.when(is_first)
        def _():
            for chunk in range(N_CHUNKS):
                bs = pl.ds(chunk * nb, nb)
                drain(near.at[:, bs], near_send_sem.at[chunk])
                drain(ctx_near.at[bs, 0], ctx_near_send_sem.at[chunk])
            for chunk in range(RELAYED):
                drain(relay.at[pl.ds(chunk * nb, nb)], relay_send_sem.at[chunk])

    pl.run_scoped(
        rest,
        pltpu.VMEM((2, width, UP_TILE), BF16),
        pltpu.VMEM((2, UP_TILE, width), BF16),
        pltpu.VMEM((width, width), BF16),
        pltpu.VMEM((3, nb, heads, n, seq_dev, head_dim), BF16),
        pltpu.VMEM((nb, n - FIRST, seq_dev, cols), BF16),
        pltpu.VMEM((3, nb, dests, heads, FIRST, seq_dev, head_dim), BF16),
        pltpu.VMEM((nb, FIRST, seq_dev, dests * cols), BF16),
    )


def store_kernel(y_ref, kv_hbm, y_hbm, k_hbm, v_hbm, buf, in_sem, out_sem, y_sem):
    n_batch = k_hbm.shape[0]
    y_out = pltpu.make_async_copy(y_ref, y_hbm, y_sem)
    pieces = [(t, b) for t in range(2) for b in range(n_batch)]
    get = [
        pltpu.make_async_copy(kv_hbm.at[1 + t, b], buf.at[t, b], in_sem.at[t, b]) for t, b in pieces
    ]
    put = [
        pltpu.make_async_copy(buf.at[t, b], (k_hbm, v_hbm)[t].at[b], out_sem.at[t, b]) for t, b in pieces
    ]
    for copy in get:
        copy.start()
    for copy in get:
        copy.wait()
    y_out.start()
    for copy in put:
        copy.start()
    for copy in put:
        copy.wait()
    y_out.wait()


def solution(mesh):
    n = mesh.shape["sp"]

    def local_layer(x_blk, ln_attn_w, ln_attn_b, ln_mlp_w, ln_mlp_b, w_qkv, w_out, w_up, w_down):
        n_batch, seq_dev, width = x_blk.shape
        groups, head_dim = w_qkv.shape[1], w_qkv.shape[3]
        heads = groups // n
        nb = n_batch // N_CHUNKS
        rows = n_batch * seq_dev
        dests = QKV_HEADS // heads
        ffn = w_up.shape[1]
        cos_t, sin_t = rope_tables(n * seq_dev, head_dim)
        row = lambda p: p.reshape(1, width)
        anywhere = pl.BlockSpec(memory_space=pl.ANY)
        flops = 2 * rows * width * (3 * width + 2 * ffn) + 2 * rows * n * seq_dev * width * 2
        y_out, recv, *_ = pl.pallas_call(
            functools.partial(layer_kernel, n),
            out_shape=[
                pltpu.VMEM((rows, width), BF16),
                jax.ShapeDtypeStruct((3, n_batch, heads, n, seq_dev, head_dim), BF16),
                jax.ShapeDtypeStruct((3, n_batch, n, heads, seq_dev, head_dim), BF16),
                jax.ShapeDtypeStruct((n_batch, n, seq_dev, heads * head_dim), BF16),
                jax.ShapeDtypeStruct((3, n_batch, dests, heads, seq_dev, head_dim), BF16),
                jax.ShapeDtypeStruct((n_batch, FIRST, seq_dev, dests * heads * head_dim), BF16),
                jax.ShapeDtypeStruct((n_batch, FIRST, seq_dev, heads * head_dim), BF16),
            ],
            in_specs=[anywhere] * 11,
            out_specs=[pl.BlockSpec(memory_space=pltpu.VMEM)] + [anywhere] * 6,
            scratch_shapes=[
                pltpu.VMEM((rows, width), F32),
                pltpu.VMEM((n_batch, seq_dev, width), BF16),
                pltpu.VMEM((4, 1, width), F32),
                pltpu.SemaphoreType.DMA,
                pltpu.SemaphoreType.DMA((4,)),
                pltpu.SemaphoreType.DMA((2,)),
                pltpu.SemaphoreType.DMA((2,)),
                pltpu.SemaphoreType.DMA((5,)),
                pltpu.SemaphoreType.DMA((2,)),
                pltpu.SemaphoreType.DMA((2,)),
                pltpu.SemaphoreType.DMA((3,)),
                pltpu.SemaphoreType.DMA((3, 2)),
                pltpu.SemaphoreType.DMA((UNITS,)),
                pltpu.SemaphoreType.DMA((UNITS, 3)),
                pltpu.SemaphoreType.DMA((UNITS,)),
                pltpu.SemaphoreType.DMA((UNITS, n // FIRST)),
                pltpu.SemaphoreType.DMA((N_CHUNKS,)),
                pltpu.SemaphoreType.DMA((N_CHUNKS,)),
                pltpu.SemaphoreType.DMA((N_CHUNKS,)),
                pltpu.SemaphoreType.DMA((N_CHUNKS,)),
                pltpu.SemaphoreType.DMA((N_CHUNKS,)),
                pltpu.SemaphoreType.DMA((N_CHUNKS,)),
            ],
            compiler_params=pltpu.CompilerParams(
                collective_id=0, has_side_effects=True, vmem_limit_bytes=57 * 2**20
            ),
            cost_estimate=pl.CostEstimate(flops=flops, bytes_accessed=3 * 10**8, transcendentals=10**7),
            name="layer",
        )(
            x_blk.reshape(rows, width),
            cos_t,
            sin_t,
            row(ln_attn_w),
            row(ln_attn_b),
            row(ln_mlp_w),
            row(ln_mlp_b),
            w_qkv.transpose(0, 2, 1, 3),
            w_out,
            w_up,
            w_down,
        )
        cache = jax.ShapeDtypeStruct((n_batch, heads, n, seq_dev, head_dim), BF16)
        y_out, k_cache, v_cache = pl.pallas_call(
            store_kernel,
            out_shape=[jax.ShapeDtypeStruct((rows, width), BF16), cache, cache],
            in_specs=[anywhere] * 2,
            out_specs=[pl.BlockSpec(memory_space=pltpu.HBM)] * 3,
            scratch_shapes=[
                pltpu.VMEM((2, n_batch, heads, n, seq_dev, head_dim), BF16),
                pltpu.SemaphoreType.DMA((2, n_batch)),
                pltpu.SemaphoreType.DMA((2, n_batch)),
                pltpu.SemaphoreType.DMA,
            ],
            compiler_params=pltpu.CompilerParams(vmem_limit_bytes=44 * 2**20),
            cost_estimate=pl.CostEstimate(flops=10**6, bytes_accessed=3 * 10**7, transcendentals=0),
            name="store",
        )(y_out, recv)
        shape = (n_batch, heads, n * seq_dev, head_dim)
        return y_out.reshape(x_blk.shape), k_cache.reshape(shape), v_cache.reshape(shape)

    act_spec, cache_spec = P("dp", "sp", None), P("dp", "sp", None, None)
    return jax.shard_map(
        local_layer,
        mesh=mesh,
        in_specs=(act_spec,) + (P(),) * 8,
        out_specs=(act_spec, cache_spec, cache_spec),
        check_vma=False,
    )
```

```python
import functools

import jax
import jax.numpy as jnp
import numpy as np
from jax import lax
from jax.experimental import pallas as pl
from jax.experimental.pallas import tpu as pltpu
from jax.sharding import PartitionSpec as P

LN_EPS = 1e-5
ROPE_BASE = 10000.0
LOG2E = 1.4426950408889634
N_CHUNKS = 6
UNITS = N_CHUNKS + 1
UP_TILE = 512
QKV_HEADS = 8
Q_TILE = 256
FIRST = 2
LATE_STEPS = 2
RELAYED = 5
F32 = jnp.float32
BF16 = jnp.bfloat16


def rope_tables(positions, head_dim):
    half_dim = head_dim // 2
    inv_freq = np.float32(ROPE_BASE) ** (np.float32(-2.0) * np.arange(half_dim, dtype=np.float32) / np.float32(head_dim))
    angles = np.arange(positions, dtype=np.float32)[:, None] * inv_freq[None, :]
    cos_t, sin_t = np.cos(angles.astype(np.float64)), np.sin(angles.astype(np.float64))
    wide = lambda a, b: jnp.asarray(np.concatenate([a, b], -1).astype(np.float32))
    return wide(cos_t, cos_t), wide(-sin_t, sin_t)


def causal_head(q, k, v, write):
    seq, head_dim = k.shape
    scale = LOG2E * head_dim**-0.5
    keys = lax.broadcasted_iota(jnp.int32, (Q_TILE, Q_TILE), 0)
    queries = lax.broadcasted_iota(jnp.int32, (Q_TILE, Q_TILE), 1)
    for i in range(q.shape[0] // Q_TILE):
        lo = seq - q.shape[0] + i * Q_TILE
        hi = lo + Q_TILE
        q_i = q[i * Q_TILE : (i + 1) * Q_TILE]
        scores = lax.dot_general(k[:hi], q_i, (((1,), (1,)), ((), ())), preferred_element_type=F32)
        diag = jnp.where(keys <= queries, scores[lo:], -1e30)
        scores = jnp.concatenate([scores[:lo], diag], axis=0) if lo else diag
        prob = jnp.exp2((scores - jnp.max(scores, axis=0, keepdims=True)) * scale)
        prob = (prob * (1.0 / jnp.sum(prob, axis=0, keepdims=True))).astype(BF16)
        out = lax.dot_general(prob, v[:hi], (((0,), (0,)), ((), ())), preferred_element_type=F32)
        write(i, out.astype(BF16))


def layer_kernel(
    n,
    x_hbm,
    cos_hbm,
    sin_hbm,
    ln_aw_hbm,
    ln_ab_hbm,
    ln_mw_hbm,
    ln_mb_hbm,
    w_qkv,
    w_out,
    w_up,
    w_down,
    h_mlp,
    recv,
    send,
    ctx_send,
    near,
    ctx_near,
    relay,
    acc,
    ctx_rows,
    ln_buf,
    x_sem,
    ln_sem,
    w_sem,
    bounce_sem,
    own_sem,
    up_sem,
    down_sem,
    qkv_sem,
    near_sem,
    send_sem,
    recv_sem,
    ctx_send_sem,
    ctx_recv_sem,
    near_send_sem,
    near_recv_sem,
    ctx_near_send_sem,
    ctx_near_recv_sem,
    relay_recv_sem,
    relay_send_sem,
):
    me = lax.axis_index("sp")
    n_batch, _, heads, seq_dev, head_dim = send.shape[1:]
    cols = heads * head_dim
    width = x_hbm.shape[1]
    nb = n_batch // N_CHUNKS
    rows = nb * seq_dev
    ffn = w_up.shape[1]
    dests = QKV_HEADS // heads
    parts = n // dests
    blocks = 3 * parts

    def peer(step):
        return lax.bitwise_xor(me, step)

    def rows_of(bs, first, count=1):
        return ctx_rows.at[bs, :, pl.ds(pl.multiple_of(first * cols, cols), count * cols)]

    half = nb // 2

    def span(unit, small):
        return pl.ds(n_batch - nb + (unit - (N_CHUNKS - 1)) * half, half) if small else pl.ds(unit * nb, nb)

    def put(unit, kind, to, frm, small=False):
        bs = span(unit, small)
        return pltpu.make_async_remote_copy(
            src_ref=send.at[kind, bs, to],
            dst_ref=recv.at[kind, bs, :, frm],
            send_sem=send_sem.at[unit],
            recv_sem=recv_sem.at[unit, kind],
            device_id={"sp": to},
            device_id_type=pl.DeviceIdType.MESH,
        )

    def put_ctx(unit, to, frm, small=False):
        bs = span(unit, small)
        return pltpu.make_async_remote_copy(
            src_ref=ctx_send.at[bs, to],
            dst_ref=rows_of(bs, frm),
            send_sem=ctx_send_sem.at[unit],
            recv_sem=ctx_recv_sem.at[unit, frm // FIRST],
            device_id={"sp": to},
            device_id_type=pl.DeviceIdType.MESH,
        )

    def put_relay(chunk, to, slot):
        bs = pl.ds(chunk * nb, nb)
        return pltpu.make_async_remote_copy(
            src_ref=ctx_send.at[bs, to],
            dst_ref=relay.at[bs, slot],
            send_sem=ctx_send_sem.at[chunk],
            recv_sem=relay_recv_sem.at[chunk],
            device_id={"sp": to - FIRST},
            device_id_type=pl.DeviceIdType.MESH,
        )

    def forward(chunk, slot):
        bs = pl.ds(chunk * nb, nb)
        return pltpu.make_async_remote_copy(
            src_ref=relay.at[bs, slot],
            dst_ref=rows_of(bs, 2 * FIRST + slot),
            send_sem=relay_send_sem.at[chunk],
            recv_sem=ctx_recv_sem.at[chunk, 2],
            device_id={"sp": me + FIRST},
            device_id_type=pl.DeviceIdType.MESH,
        )

    def put_near(chunk, kind):
        bs = pl.ds(chunk * nb, nb)
        return pltpu.make_async_remote_copy(
            src_ref=send.at[kind, bs, pl.ds((1 - me) * dests, dests)],
            dst_ref=near.at[kind, bs],
            send_sem=near_send_sem.at[chunk],
            recv_sem=near_recv_sem.at[chunk],
            device_id={"sp": 1 - me},
            device_id_type=pl.DeviceIdType.MESH,
        )

    def put_ctx_near(chunk):
        bs = pl.ds(chunk * nb, nb)
        return pltpu.make_async_remote_copy(
            src_ref=ctx_near.at[bs, 1 - me],
            dst_ref=rows_of(bs, me * dests, dests),
            send_sem=ctx_near_send_sem.at[chunk],
            recv_sem=ctx_near_recv_sem.at[chunk],
            device_id={"sp": 1 - me},
            device_id_type=pl.DeviceIdType.MESH,
        )

    def drain(ref, sem):
        pltpu.make_async_copy(ref, ref, sem).wait()

    is_first = me < FIRST
    later_on = jnp.logical_not(is_first)

    def each_peer(do, lowest=0):
        for other in range(lowest, n):
            pl.when(other != me)(functools.partial(do, other))

    def qkv_phase(x_buf, h_attn, w_nat, w_cols, out_buf, own, cos_ref, sin_ref):
        mine = pl.ds(pl.multiple_of(me * seq_dev, seq_dev), seq_dev)
        get_cos = pltpu.make_async_copy(cos_hbm.at[mine], cos_ref, own_sem.at[3])
        get_sin = pltpu.make_async_copy(sin_hbm.at[mine], sin_ref, own_sem.at[4])

        def get_x(chunk):
            return pltpu.make_async_copy(x_hbm.at[pl.ds(chunk * rows, rows)], x_buf, x_sem)

        def get_w(half):
            block, slot = half // 2, lax.rem(half, 2)
            src = w_qkv.at[
                pl.ds(slot * (width // 2), width // 2),
                block // parts,
                pl.ds(lax.rem(block, parts) * QKV_HEADS, QKV_HEADS),
            ]
            return pltpu.make_async_copy(src, w_nat.at[slot], w_sem.at[slot])

        def bounce(step):
            slot, block = lax.rem(step, 2), lax.rem(step, blocks)
            dst = send.at[
                block // parts, pl.ds(step // blocks * nb, nb), pl.ds(lax.rem(block, parts) * dests, dests)
            ]
            return pltpu.make_async_copy(out_buf.at[slot], dst, bounce_sem.at[slot])

        def put_own(chunk, kind):
            dst = recv.at[kind, pl.ds(chunk * nb, nb), :, me]
            return pltpu.make_async_copy(own.at[kind], dst, own_sem.at[kind])

        def send_unit(unit, block, small):
            for d in range(dests):
                to = lax.rem(block, parts) * dests + lax.rem(me + d, dests)

                @pl.when((to != me) & jnp.logical_not(is_first & (block < parts)))
                def _():
                    put(unit, block // parts, to, me, small).start()

        def send_block(step):
            bounce(step).wait()
            block = lax.rem(step, blocks)
            is_last = step // blocks == N_CHUNKS - 1
            pl.when(jnp.logical_not(is_last))(lambda: send_unit(step // blocks, block, False))
            pl.when(is_last)(lambda: send_unit(N_CHUNKS - 1, block, True))

            @pl.when(is_first & (lax.rem(block, parts) == 1 - me))
            def _():
                put_near(step // blocks, block // parts).start()

        ln_hbm = (ln_aw_hbm, ln_ab_hbm, ln_mw_hbm, ln_mb_hbm)
        get_ln = [pltpu.make_async_copy(p, ln_buf.at[i], ln_sem.at[i]) for i, p in enumerate(ln_hbm)]
        ln_aw, ln_ab, ln_mw, ln_mb = (ln_buf.at[i] for i in range(4))
        get_x(0).start()
        for copy in get_ln:
            copy.start()
        get_w(0).start()
        get_w(1).start()
        get_cos.start()
        get_sin.start()
        barrier = pltpu.get_barrier_semaphore()
        for step in range(1, n):
            pl.semaphore_signal(
                barrier, inc=1, device_id={"sp": peer(step)}, device_id_type=pl.DeviceIdType.MESH
            )

        @pl.loop(0, N_CHUNKS * blocks)
        def _(step):
            chunk, block = step // blocks, lax.rem(step, blocks)
            kind, part = block // parts, lax.rem(block, parts)
            slot = lax.rem(step, 2)

            @pl.when(block == 0)
            def _():
                get_x(chunk).wait()

                @pl.when(chunk == 0)
                def _():
                    for copy in get_ln:
                        copy.wait()

                @pl.loop(0, nb)
                def _(i):
                    r = pl.ds(pl.multiple_of(i * seq_dev, seq_dev), seq_dev)
                    g = pl.ds(pl.multiple_of(chunk * rows + i * seq_dev, seq_dev), seq_dev)
                    xf = x_buf[r, :].astype(F32)
                    mean = jnp.sum(xf, axis=-1, keepdims=True) * (1.0 / width)
                    dev = xf - mean
                    var = jnp.sum(dev * dev, axis=-1, keepdims=True) * (1.0 / width)
                    unit = dev * lax.rsqrt(var + LN_EPS)
                    h_attn[r, :] = (unit * ln_aw[...] + ln_ab[...]).astype(BF16)
                    h_mlp[g, :] = (unit * ln_mw[...] + ln_mb[...]).astype(BF16)
                    acc[g, :] = xf

                @pl.when(chunk + 1 < N_CHUNKS)
                def _():
                    get_x(chunk + 1).start()

            @pl.when(chunk == 0)
            def _():
                @pl.when(block == 0)
                def _():
                    get_cos.wait()
                    get_sin.wait()

                @pl.loop(2 * block, 2 * block + 2)
                def _(half):
                    get_w(half).wait()

                    @pl.loop(0, width // 2 // 128)
                    def _(i):
                        r = pl.ds(pl.multiple_of(i * 128, 128), 128)
                        top = lax.rem(half, 2) * (width // 2)
                        to = pl.ds(pl.multiple_of(top + i * 128, 128), 128)
                        by_head = jnp.swapaxes(w_nat[lax.rem(half, 2), r].astype(F32), 0, 1)
                        for h in range(QKV_HEADS):
                            w_cols[block, to, h * head_dim : (h + 1) * head_dim] = by_head[h].astype(BF16)

                    @pl.when(half + 2 < 2 * blocks)
                    def _():
                        get_w(half + 2).start()

            for d in range(dests):
                cs = slice(d * heads * head_dim, (d + 1) * heads * head_dim)
                cols = jnp.dot(h_attn[...], w_cols[block, :, cs], preferred_element_type=F32)
                for h in range(heads):
                    for b in range(nb):
                        u = cols[b * seq_dev : (b + 1) * seq_dev, h * head_dim : (h + 1) * head_dim]
                        u = u.astype(BF16).astype(F32)
                        turned = u * cos_ref[...] + pltpu.roll(u, head_dim // 2, 1) * sin_ref[...]
                        out_buf[slot, b, d, h] = jnp.where(kind < 2, turned, u).astype(BF16)

            bounce(step).start()

            @pl.when(me // dests == part)
            def _():
                @pl.when(chunk > 0)
                def _():
                    put_own(chunk - 1, kind).wait()

                own[kind] = out_buf[slot, :, lax.rem(me, dests)]
                put_own(chunk, kind).start()

            @pl.when(step == 0)
            def _():
                pl.semaphore_wait(barrier, n - 1)

            @pl.when(chunk == 0)
            def _():
                send_block(step)

            @pl.when(step > blocks)
            def _():
                send_block(step - 1)

        send_block(N_CHUNKS * blocks - 1)
        pl.loop(0, blocks)(lambda block: send_unit(UNITS - 1, block, True))
        for kind in range(3):
            put_own(N_CHUNKS - 1, kind).wait()

    pl.run_scoped(
        qkv_phase,
        pltpu.VMEM((rows, width), BF16),
        pltpu.VMEM((rows, width), BF16),
        pltpu.VMEM((2, width // 2, QKV_HEADS, head_dim), BF16),
        pltpu.VMEM((blocks, width, QKV_HEADS * head_dim), BF16),
        pltpu.VMEM((2, nb, dests, heads, seq_dev, head_dim), BF16),
        pltpu.VMEM((3, nb, heads, seq_dev, head_dim), BF16),
        pltpu.VMEM((seq_dev, head_dim), F32),
        pltpu.VMEM((seq_dev, head_dim), F32),
    )

    def rest(up_buf, down_buf, w_buf, qkv_buf, ctx_buf, both, near_buf):
        later = n - FIRST
        steps = ffn // UP_TILE

        def get_up(f):
            cols = pl.ds(pl.multiple_of(f * UP_TILE, UP_TILE), UP_TILE)
            slot = lax.rem(f, 2)
            return pltpu.make_async_copy(w_up.at[:, cols], up_buf.at[slot], up_sem.at[slot])

        def get_down(f):
            cols = pl.ds(pl.multiple_of(f * UP_TILE, UP_TILE), UP_TILE)
            slot = lax.rem(f, 2)
            return pltpu.make_async_copy(w_down.at[cols], down_buf.at[slot], down_sem.at[slot])

        def get_w_out():
            return pltpu.make_async_copy(w_out, w_buf, w_sem.at[0])

        def get_qkv(unit, kind, small):
            count = half if small else nb
            to = qkv_buf.at[kind, pl.ds(0, count)]
            return pltpu.make_async_copy(recv.at[kind, span(unit, small)], to, qkv_sem.at[kind])

        def get_own_near(chunk, kind):
            src = send.at[kind, pl.ds(chunk * nb, nb), pl.ds(me * dests, dests)]
            return pltpu.make_async_copy(src, both.at[kind, :, :, :, me], near_sem.at[kind, 0])

        def get_other_near(chunk, kind):
            src = near.at[kind, pl.ds(chunk * nb, nb)]
            return pltpu.make_async_copy(src, both.at[kind, :, :, :, 1 - me], near_sem.at[kind, 1])

        def bounce_ctx(unit, small):
            dst = ctx_send.at[span(unit, small), pl.ds(FIRST, later)]
            return pltpu.make_async_copy(ctx_buf.at[pl.ds(0, half if small else nb)], dst, bounce_sem.at[0])

        def bounce_near(chunk):
            return pltpu.make_async_copy(near_buf, ctx_near.at[pl.ds(chunk * nb, nb)], bounce_sem.at[1])

        def send_ctx(unit, small=False):
            bounce_ctx(unit, small).wait()
            relays = (me // FIRST == 2) & (unit < RELAYED)

            def one(other):
                if other // FIRST == 1 and not small:
                    pl.when(relays)(lambda: put_relay(unit, other, me - 2 * FIRST).start())
                    pl.when(jnp.logical_not(relays))(lambda: put_ctx(unit, other, me).start())
                else:
                    put_ctx(unit, other, me, small).start()

            each_peer(one, FIRST)

        def send_near(chunk):
            bounce_near(chunk).wait()
            put_ctx_near(chunk).start()

        def pass_on(chunk):
            drain(relay.at[pl.ds(chunk * nb, nb)], relay_recv_sem.at[chunk])
            for slot in range(FIRST):
                forward(chunk, slot).start()

        def load_qkv(unit, small=False):
            bs = span(unit, small)
            for kind in range(3):
                got = lambda count: recv.at[kind, bs, :, pl.ds(0, count)]
                if kind:
                    drain(got(n - 1), recv_sem.at[unit, kind])
                else:
                    pl.when(is_first)(lambda: drain(got(n - FIRST), recv_sem.at[unit, kind]))
                    pl.when(later_on)(lambda: drain(got(n - FIRST - 1), recv_sem.at[unit, kind]))
                get_qkv(unit, kind, small).start()

        def load_near(chunk):
            drain(near.at[:, pl.ds(chunk * nb, nb)], near_recv_sem.at[chunk])
            for kind in range(3):
                get_own_near(chunk, kind).start()
                get_other_near(chunk, kind).start()

        def attend(unit, small=False):
            for kind in range(3):
                get_qkv(unit, kind, small).wait()
            count = half if small else nb
            for b in range(count):
                for h in range(heads):
                    q = qkv_buf[0, b, h, FIRST:].reshape(later * seq_dev, head_dim)
                    k, v = (qkv_buf[t, b, h].reshape(n * seq_dev, head_dim) for t in (1, 2))
                    per = Q_TILE // seq_dev

                    def write(i, out):
                        ctx_buf[b, i * per : (i + 1) * per, :, h * head_dim : (h + 1) * head_dim] = out.reshape(
                            per, seq_dev, head_dim
                        )

                    causal_head(q, k, v, write)
            bounce_ctx(unit, small).start()

            @pl.when(later_on)
            def _():
                rows_of(span(unit, small), me)[...] = ctx_buf[:count, me - FIRST]

        get_up(0).start()
        get_down(0).start()
        get_w_out().start()

        early = steps - LATE_STEPS

        def mlp_end(turn):
            whole = (turn + 1) * early // N_CHUNKS
            return jnp.where(turn < N_CHUNKS - 1, whole, jnp.where(turn < UNITS, early - UNITS + 1 + turn, steps))

        @pl.loop(0, UNITS + 1)
        def _(unit):
            first, last = jnp.where(unit > 0, mlp_end(unit - 1), 0), mlp_end(unit)
            is_small = (unit == UNITS - 1) | (unit == UNITS - 2)

            @pl.loop(first, last)
            def _(f):
                slot = lax.rem(f, 2)

                @pl.when(f + 1 < steps)
                def _():
                    get_up(f + 1).start()
                    get_down(f + 1).start()

                @pl.when((f == last - 1) & (unit < N_CHUNKS - 1))
                def _():
                    load_qkv(unit)
                    pl.when(is_first)(lambda: load_near(unit))

                @pl.when((f == last - 1) & (unit == UNITS - 2))
                def _():
                    load_qkv(unit, True)

                get_up(f).wait()
                get_down(f).wait()
                for r in range(n_batch * seq_dev // 512):
                    rs = pl.ds(r * 512, 512)
                    up = jnp.dot(h_mlp[rs, :], up_buf[slot], preferred_element_type=F32)
                    hid = (0.5 * up * (1.0 + lax.erf(up * 0.5**0.5))).astype(BF16)
                    acc[rs, :] += jnp.dot(hid, down_buf[slot], preferred_element_type=F32)

                @pl.when((f == first) & (unit > 0) & (unit < N_CHUNKS))
                def _():
                    send_ctx(unit - 1)
                    pl.when(is_first)(lambda: send_near(unit - 1))

                @pl.when(is_first & (unit == UNITS))
                def _():
                    pl.when(f == first)(lambda: send_near(N_CHUNKS - 1))
                    pass_on(2 + f - first)

            pl.when(unit < N_CHUNKS - 1)(lambda: attend(unit))
            pl.when(unit == UNITS - 1)(lambda: load_qkv(unit, True))

            @pl.when(is_small)
            def _():
                attend(unit, True)
                send_ctx(unit, True)

            @pl.when(is_first & (unit != UNITS - 2) & (unit < UNITS))
            def _():
                chunk = jnp.minimum(unit, N_CHUNKS - 1)

                @pl.when(unit == UNITS - 1)
                def _():
                    pass_on(0)
                    load_near(chunk)

                for kind in range(3):
                    get_own_near(chunk, kind).wait()
                    get_other_near(chunk, kind).wait()

                @pl.loop(0, nb)
                def _(b):
                    for d in range(dests):
                        for h in range(heads):
                            q, k, v = (both[t, b, d, h].reshape(Q_TILE, head_dim) for t in range(3))

                            def write(i, out):
                                col = (d * heads + h) * head_dim
                                near_buf[b, :, :, col : col + head_dim] = out.reshape(
                                    FIRST, seq_dev, head_dim
                                )

                            causal_head(q, k, v, write)

                bounce_near(chunk).start()
                rows_of(pl.ds(chunk * nb, nb), me * dests, dests)[...] = near_buf[:, me]
                pl.when(unit == UNITS - 1)(lambda: pass_on(1))

        get_w_out().wait()

        def drain_qkv(unit, small=False):
            bs = span(unit, small)
            pl.when(is_first)(lambda: drain(send.at[pl.ds(1, 2), bs, pl.ds(0, n - 1)], send_sem.at[unit]))
            pl.when(later_on)(lambda: drain(send.at[:, bs, pl.ds(0, n - 1)], send_sem.at[unit]))

        def drain_ctx(unit, small=False):
            bs = span(unit, small)
            pl.when(is_first)(lambda: drain(ctx_send.at[bs, pl.ds(0, n - FIRST)], ctx_send_sem.at[unit]))
            pl.when(later_on)(lambda: drain(ctx_send.at[bs, pl.ds(0, n - FIRST - 1)], ctx_send_sem.at[unit]))

        pl.loop(0, N_CHUNKS - 1)(drain_qkv)
        pl.loop(N_CHUNKS - 1, UNITS)(lambda unit: drain_qkv(unit, True))

        @pl.loop(0, N_CHUNKS)
        def _(turn):
            pl.when(turn > 1)(lambda: drain_ctx(turn - 2))
            pl.when(is_first & (turn == 2))(lambda: pass_on(RELAYED - 1))
            chunk = turn
            g = pl.ds(pl.multiple_of(chunk * rows, rows), rows)
            pl.when(is_first)(lambda: put_ctx_near(chunk).wait_recv())
            for part in range(n // FIRST):
                home = me // FIRST
                source = jnp.where(part == 0, home, jnp.where(part <= home, part - 1, part))

                count = FIRST - (part == 0)

                @pl.when(later_on & (chunk < N_CHUNKS - 1))
                def _():
                    drain(rows_of(span(chunk, False), 0, count), ctx_recv_sem.at[chunk, source])

                @pl.when(later_on & (chunk == N_CHUNKS - 1))
                def _():
                    for unit in (N_CHUNKS - 1, N_CHUNKS):
                        drain(rows_of(span(unit, True), 0, count), ctx_recv_sem.at[unit, source])

                those = pl.ds(pl.multiple_of(source * FIRST * cols, FIRST * cols), FIRST * cols)
                left = ctx_rows[pl.ds(chunk * nb, nb), :, those].reshape(rows, FIRST * cols)
                for c in range(0, width, 1024):
                    cs = slice(c, c + 1024)
                    total = acc[g, cs] + jnp.dot(left, w_buf[those, cs], preferred_element_type=F32)
                    if part < n // FIRST - 1:
                        acc[g, cs] = total
                    else:
                        h_mlp[g, cs] = total.astype(BF16)

        drain_ctx(N_CHUNKS - 2)
        pl.loop(N_CHUNKS - 1, UNITS)(lambda unit: drain_ctx(unit, True))

        @pl.when(is_first)
        def _():
            for chunk in range(N_CHUNKS):
                bs = pl.ds(chunk * nb, nb)
                drain(near.at[:, bs], near_send_sem.at[chunk])
                drain(ctx_near.at[bs, 0], ctx_near_send_sem.at[chunk])
            for chunk in range(RELAYED):
                drain(relay.at[pl.ds(chunk * nb, nb)], relay_send_sem.at[chunk])

    pl.run_scoped(
        rest,
        pltpu.VMEM((2, width, UP_TILE), BF16),
        pltpu.VMEM((2, UP_TILE, width), BF16),
        pltpu.VMEM((width, width), BF16),
        pltpu.VMEM((3, nb, heads, n, seq_dev, head_dim), BF16),
        pltpu.VMEM((nb, n - FIRST, seq_dev, cols), BF16),
        pltpu.VMEM((3, nb, dests, heads, FIRST, seq_dev, head_dim), BF16),
        pltpu.VMEM((nb, FIRST, seq_dev, dests * cols), BF16),
    )


def store_kernel(y_ref, kv_hbm, y_hbm, k_hbm, v_hbm, buf, in_sem, out_sem, y_sem):
    n_batch = k_hbm.shape[0]
    y_out = pltpu.make_async_copy(y_ref, y_hbm, y_sem)
    pieces = [(t, b) for t in range(2) for b in range(n_batch)]
    get = [
        pltpu.make_async_copy(kv_hbm.at[1 + t, b], buf.at[t, b], in_sem.at[t, b]) for t, b in pieces
    ]
    put = [
        pltpu.make_async_copy(buf.at[t, b], (k_hbm, v_hbm)[t].at[b], out_sem.at[t, b]) for t, b in pieces
    ]
    for copy in get:
        copy.start()
    for copy in get:
        copy.wait()
    y_out.start()
    for copy in put:
        copy.start()
    for copy in put:
        copy.wait()
    y_out.wait()


def solution(mesh):
    n = mesh.shape["sp"]

    def local_layer(x_blk, ln_attn_w, ln_attn_b, ln_mlp_w, ln_mlp_b, w_qkv, w_out, w_up, w_down):
        n_batch, seq_dev, width = x_blk.shape
        groups, head_dim = w_qkv.shape[1], w_qkv.shape[3]
        heads = groups // n
        nb = n_batch // N_CHUNKS
        rows = n_batch * seq_dev
        dests = QKV_HEADS // heads
        ffn = w_up.shape[1]
        cos_t, sin_t = rope_tables(n * seq_dev, head_dim)
        row = lambda p: p.reshape(1, width)
        anywhere = pl.BlockSpec(memory_space=pl.ANY)
        flops = 2 * rows * width * (3 * width + 2 * ffn) + 2 * rows * n * seq_dev * width * 2
        y_out, recv, *_ = pl.pallas_call(
            functools.partial(layer_kernel, n),
            out_shape=[
                pltpu.VMEM((rows, width), BF16),
                jax.ShapeDtypeStruct((3, n_batch, heads, n, seq_dev, head_dim), BF16),
                jax.ShapeDtypeStruct((3, n_batch, n, heads, seq_dev, head_dim), BF16),
                jax.ShapeDtypeStruct((n_batch, n, seq_dev, heads * head_dim), BF16),
                jax.ShapeDtypeStruct((3, n_batch, dests, heads, seq_dev, head_dim), BF16),
                jax.ShapeDtypeStruct((n_batch, FIRST, seq_dev, dests * heads * head_dim), BF16),
                jax.ShapeDtypeStruct((n_batch, FIRST, seq_dev, heads * head_dim), BF16),
            ],
            in_specs=[anywhere] * 11,
            out_specs=[pl.BlockSpec(memory_space=pltpu.VMEM)] + [anywhere] * 6,
            scratch_shapes=[
                pltpu.VMEM((rows, width), F32),
                pltpu.VMEM((n_batch, seq_dev, width), BF16),
                pltpu.VMEM((4, 1, width), F32),
                pltpu.SemaphoreType.DMA,
                pltpu.SemaphoreType.DMA((4,)),
                pltpu.SemaphoreType.DMA((2,)),
                pltpu.SemaphoreType.DMA((2,)),
                pltpu.SemaphoreType.DMA((5,)),
                pltpu.SemaphoreType.DMA((2,)),
                pltpu.SemaphoreType.DMA((2,)),
                pltpu.SemaphoreType.DMA((3,)),
                pltpu.SemaphoreType.DMA((3, 2)),
                pltpu.SemaphoreType.DMA((UNITS,)),
                pltpu.SemaphoreType.DMA((UNITS, 3)),
                pltpu.SemaphoreType.DMA((UNITS,)),
                pltpu.SemaphoreType.DMA((UNITS, n // FIRST)),
                pltpu.SemaphoreType.DMA((N_CHUNKS,)),
                pltpu.SemaphoreType.DMA((N_CHUNKS,)),
                pltpu.SemaphoreType.DMA((N_CHUNKS,)),
                pltpu.SemaphoreType.DMA((N_CHUNKS,)),
                pltpu.SemaphoreType.DMA((N_CHUNKS,)),
                pltpu.SemaphoreType.DMA((N_CHUNKS,)),
            ],
            compiler_params=pltpu.CompilerParams(
                collective_id=0, has_side_effects=True, vmem_limit_bytes=57 * 2**20
            ),
            cost_estimate=pl.CostEstimate(flops=flops, bytes_accessed=3 * 10**8, transcendentals=10**7),
            name="layer",
        )(
            x_blk.reshape(rows, width),
            cos_t,
            sin_t,
            row(ln_attn_w),
            row(ln_attn_b),
            row(ln_mlp_w),
            row(ln_mlp_b),
            w_qkv.transpose(0, 2, 1, 3),
            w_out,
            w_up,
            w_down,
        )
        cache = jax.ShapeDtypeStruct((n_batch, heads, n, seq_dev, head_dim), BF16)
        y_out, k_cache, v_cache = pl.pallas_call(
            store_kernel,
            out_shape=[jax.ShapeDtypeStruct((rows, width), BF16), cache, cache],
            in_specs=[anywhere] * 2,
            out_specs=[pl.BlockSpec(memory_space=pltpu.HBM)] * 3,
            scratch_shapes=[
                pltpu.VMEM((2, n_batch, heads, n, seq_dev, head_dim), BF16),
                pltpu.SemaphoreType.DMA((2, n_batch)),
                pltpu.SemaphoreType.DMA((2, n_batch)),
                pltpu.SemaphoreType.DMA,
            ],
            compiler_params=pltpu.CompilerParams(vmem_limit_bytes=44 * 2**20),
            cost_estimate=pl.CostEstimate(flops=10**6, bytes_accessed=3 * 10**7, transcendentals=0),
            name="store",
        )(y_out, recv)
        shape = (n_batch, heads, n * seq_dev, head_dim)
        return y_out.reshape(x_blk.shape), k_cache.reshape(shape), v_cache.reshape(shape)

    act_spec, cache_spec = P("dp", "sp", None), P("dp", "sp", None, None)
    return jax.shard_map(
        local_layer,
        mesh=mesh,
        in_specs=(act_spec,) + (P(),) * 8,
        out_specs=(act_spec, cache_spec, cache_spec),
        check_vma=False,
    )
```
